128 devices in a mesh: dp: 1, ep2: 2 (over core), ep: 64 (over z, y, x).
Axes of the slice: x: 4, y: 4, z: 4, core: 2. Of those that a mesh axis runs over, the one named last changes fastest.
Arguments:
- x_tok: bfloat16 [32768, 2048], P(('dp', 'ep2', 'ep'))
- expert_ids: int32 [32768, 8], P(('dp', 'ep2', 'ep'))
- gate_w: float32 [32768, 8], P(('dp', 'ep2', 'ep'))
- w_in: bfloat16 [256, 2048, 512], P(('ep2', 'ep'))
- w_out: bfloat16 [256, 512, 2048], P(('ep2', 'ep'))
Outputs:
- output: bfloat16 [32768, 2048], P(('dp', 'ep2', 'ep'))
All inputs are finite; a program needn't handle non-finite values.
Results may differ from the reference program's by a relative error of at most 0.00101.
Values are sent between devices in bfloat16 or wider.
A program may use at most 1 GiB of HBM per device.

```python
import math
import jax
import jax.numpy as jnp
from jax import lax

TOKENS = 256
GROUP = 128
D_MODEL = 2048
FF = 512
EXPERTS = 256
TOP = 8
CAP = 1280


def draw_routing(route_key):
    k_perm, k_shift, k_tok, k_roll = jax.random.split(route_key, 4)
    avg_count = TOKENS * TOP // EXPERTS
    spread = avg_count - 1
    rank_of = jax.random.permutation(k_perm, EXPERTS)
    shifts = jax.random.randint(k_shift, (GROUP, 1), 0, EXPERTS // 16 + 2)
    prof_pos = (rank_of[None, :] + shifts) % EXPERTS
    near_end = jnp.minimum(prof_pos, EXPERTS - 1 - prof_pos)
    step_mag = (spread * (EXPERTS - 1 - 2 * near_end)) // (EXPERTS - 1)
    dev_counts = avg_count + jnp.where(prof_pos < EXPERTS - 1 - prof_pos, step_mag, -step_mag)
    run_end = jnp.cumsum(dev_counts, axis=1)
    list_pos = jnp.arange(TOKENS * TOP)
    sorted_ids = jax.vmap(lambda end_row: jnp.searchsorted(end_row, list_pos, side='right'))(run_end)
    id_grid = jnp.swapaxes(sorted_ids.reshape(GROUP, TOP, TOKENS), 1, 2)
    tok_keys = jax.random.split(k_tok, GROUP)
    tok_perm = jax.vmap(lambda tok_key: jax.random.permutation(tok_key, TOKENS))(tok_keys)
    id_grid = jnp.take_along_axis(id_grid, jnp.broadcast_to(tok_perm[:, :, None], (GROUP, TOKENS, TOP)), axis=1)
    roll_by = jax.random.randint(k_roll, (GROUP, TOKENS, 1), 0, TOP)
    col_ids = (jnp.arange(TOP)[None, None, :] + roll_by) % TOP
    id_grid = jnp.take_along_axis(id_grid, col_ids, axis=2)
    return id_grid.reshape(GROUP * TOKENS, TOP).astype(jnp.int32)


def setup_inputs(seed: int = 0, part: int = 0) -> dict:
    key_part = jax.random.fold_in(jax.random.key(seed), part)
    k_x, k_gate, k_route = jax.random.split(key_part, 3)
    k_in, k_out = jax.random.split(jax.random.key(seed + 1), 2)
    x_tok = jax.random.normal(k_x, (GROUP * TOKENS, D_MODEL), jnp.float32).astype(jnp.bfloat16)
    gate_w = jax.random.uniform(k_gate, (GROUP * TOKENS, TOP), jnp.float32, 0.5, 1.5) * (2.0 / math.sqrt(TOP))
    w_in = (jax.random.normal(k_in, (EXPERTS, D_MODEL, FF), jnp.float32) * (D_MODEL ** -0.5)).astype(jnp.bfloat16)
    w_out = (jax.random.normal(k_out, (EXPERTS, FF, D_MODEL), jnp.float32) * (FF ** -0.5)).astype(jnp.bfloat16)
    return {'x_tok': x_tok, 'expert_ids': draw_routing(k_route), 'gate_w': gate_w, 'w_in': w_in, 'w_out': w_out}


def reference(x_tok, expert_ids, gate_w, w_in, w_out):
    flat_e = expert_ids.reshape(-1)
    n_pair = flat_e.shape[0]
    pair_order = jnp.argsort(flat_e, stable=True)
    counts = jnp.bincount(flat_e, length=EXPERTS)
    starts = jnp.cumsum(counts) - counts
    slot_ids = jnp.arange(CAP)
    flat_gate = gate_w.reshape(-1)

    def one_expert(acc_y, inputs):
        start_at, n_count, w_a, w_b = inputs
        pair_ids = pair_order[jnp.minimum(start_at + slot_ids, n_pair - 1)]
        is_kept = slot_ids < jnp.minimum(n_count, CAP)
        tok_ids = pair_ids // TOP
        tok_rows = jnp.where(is_kept[:, None], x_tok[tok_ids], jnp.zeros((), x_tok.dtype))
        hidden = jax.nn.gelu(jnp.dot(tok_rows, w_a, preferred_element_type=jnp.float32), approximate=True).astype(jnp.bfloat16)
        out_rows = jnp.dot(hidden, w_b, preferred_element_type=jnp.float32).astype(jnp.bfloat16)
        weight = jnp.where(is_kept, flat_gate[pair_ids], 0.0)
        acc_y = acc_y.at[tok_ids].add(weight[:, None] * out_rows.astype(jnp.float32))
        return acc_y, None

    acc_y, _ = lax.scan(one_expert, x_tok.astype(jnp.float32), (starts, counts, w_in, w_out))
    return acc_y.astype(jnp.bfloat16)
```

```python
import functools

import jax
import jax.numpy as jnp
from jax import lax
from jax.experimental import pallas as pl
from jax.experimental.pallas import tpu as pltpu
from jax.sharding import PartitionSpec as P

LANES = 16


def onehot_sum(keys, values, width, base=0):
    n_tok, n_top = keys.shape
    cols = lax.broadcasted_iota(jnp.int32, (n_tok, width), 1) + base
    total = jnp.zeros((n_tok, width), jnp.float32)
    for j in range(n_top):
        total = jnp.where(cols == keys[:, j:j + 1], values[j], total)
    return total


def route_kernel(ids_ref, slot_ref, count_ref):
    ids = ids_ref[...]
    n_tok, n_top = ids.shape
    experts = count_ref.shape[1]
    member = onehot_sum(ids, [1.0] * n_top, experts)
    row = lax.broadcasted_iota(jnp.int32, (n_tok, n_tok), 0)
    col = lax.broadcasted_iota(jnp.int32, (n_tok, n_tok), 1)
    earlier = jnp.where(col < row, 1.0, 0.0).astype(jnp.bfloat16)
    before = jnp.dot(earlier, member.astype(jnp.bfloat16), preferred_element_type=jnp.float32)
    count_ref[...] = jnp.sum(member, axis=0, keepdims=True).astype(jnp.int32)
    cols = lax.broadcasted_iota(jnp.int32, (n_tok, experts), 1)
    for j in range(n_top):
        rank = jnp.sum(jnp.where(cols == ids[:, j:j + 1], before, 0.0), axis=1, keepdims=True)
        slot_ref[:, j:j + 1] = ids[:, j:j + 1] * LANES + rank.astype(jnp.int32)


def route(ids, experts):
    return pl.pallas_call(
        route_kernel,
        out_shape=(jax.ShapeDtypeStruct(ids.shape, jnp.int32), jax.ShapeDtypeStruct((1, experts), jnp.int32)),
        name='route',
    )(ids)


def pack_kernel(slot_ref, x_ref, out_ref):
    rows = out_ref.shape[0]
    pick = onehot_sum(slot_ref[...], [1.0] * slot_ref.shape[1], rows, pl.program_id(0) * rows).astype(jnp.bfloat16)
    out_ref[...] = lax.dot_general(pick, x_ref[...], (((0,), (0,)), ((), ())), preferred_element_type=jnp.float32).astype(out_ref.dtype)


def pack(slot, x, n_slot, rows=512):
    n_tok, d_model = x.shape
    return pl.pallas_call(
        pack_kernel,
        grid=(n_slot // rows,),
        in_specs=[pl.BlockSpec(slot.shape, lambda i: (0, 0)), pl.BlockSpec(x.shape, lambda i: (0, 0))],
        out_specs=pl.BlockSpec((rows, d_model), lambda i: (i, 0)),
        out_shape=jax.ShapeDtypeStruct((n_slot, d_model), x.dtype),
        cost_estimate=pl.CostEstimate(flops=2 * n_slot * n_tok * d_model, bytes_accessed=2 * n_slot * d_model, transcendentals=0),
        name='pack',
    )(slot, x)


def expert_kernel(rows_ref, w_in_ref, w_out_ref, out_ref):
    shape = rows_ref.shape
    rows = rows_ref[...].reshape(shape[0] * shape[2], shape[3])
    hidden = jax.nn.gelu(jnp.dot(rows, w_in_ref[0], preferred_element_type=jnp.float32), approximate=True).astype(jnp.bfloat16)
    out_ref[...] = jnp.dot(hidden, w_out_ref[0], preferred_element_type=jnp.float32).astype(out_ref.dtype).reshape(shape)


def expert(rows, w_in, w_out, group=32):
    n_src, e_loc, lanes, d_model = rows.shape
    ff = w_in.shape[2]
    row_spec = pl.BlockSpec((group, 1, lanes, d_model), lambda e, i: (i, e, 0, 0))
    return pl.pallas_call(
        expert_kernel,
        grid=(e_loc, n_src // group),
        in_specs=[row_spec, pl.BlockSpec((1, d_model, ff), lambda e, i: (e, 0, 0)), pl.BlockSpec((1, ff, d_model), lambda e, i: (e, 0, 0))],
        out_specs=row_spec,
        out_shape=jax.ShapeDtypeStruct(rows.shape, rows.dtype),
        compiler_params=pltpu.CompilerParams(vmem_limit_bytes=48 * 2**20),
        cost_estimate=pl.CostEstimate(flops=4 * n_src * e_loc * lanes * d_model * ff, bytes_accessed=4 * rows.size, transcendentals=0),
        name='expert',
    )(rows, w_in, w_out)


def combine_kernel(capacity, slot_ref, ids_ref, gate_ref, off_ref, x_ref, back_ref, out_ref, acc_ref, weight_ref):
    step = pl.program_id(0)
    n_tok, n_top = ids_ref.shape
    experts = off_ref.shape[1]
    rows = back_ref.shape[0]

    @pl.when(step == 0)
    def _():
        ids = ids_ref[...]
        off = off_ref[...].astype(jnp.float32)
        cols = lax.broadcasted_iota(jnp.int32, (n_tok, experts), 1)
        for j in range(n_top):
            first = jnp.sum(jnp.where(cols == ids[:, j:j + 1], off, 0.0), axis=1, keepdims=True).astype(jnp.int32)
            rank = first + slot_ref[:, j:j + 1] - ids[:, j:j + 1] * LANES
            weight_ref[:, j:j + 1] = jnp.where(rank < capacity, gate_ref[:, j:j + 1], 0.0)
        acc_ref[...] = x_ref[...].astype(jnp.float32)

    weight = weight_ref[...]
    gates = onehot_sum(slot_ref[...], [weight[:, j:j + 1] for j in range(n_top)], rows, step * rows)
    high = gates.astype(jnp.bfloat16)
    rest = gates - high.astype(jnp.float32)
    mid = rest.astype(jnp.bfloat16)
    low = (rest - mid.astype(jnp.float32)).astype(jnp.bfloat16)
    parts = jnp.concatenate([high, mid, low], axis=0)
    mix = jnp.dot(parts, back_ref[...], preferred_element_type=jnp.float32)
    acc_ref[...] += mix[:n_tok] + mix[n_tok:2 * n_tok] + mix[2 * n_tok:]

    @pl.when(step == pl.num_programs(0) - 1)
    def _():
        out_ref[...] = acc_ref[...].astype(out_ref.dtype)


def combine(slot, ids, gate, off, x, back, capacity, rows=512):
    n_tok, d_model = x.shape
    whole = lambda a: pl.BlockSpec(a.shape, lambda i: (0, 0))
    return pl.pallas_call(
        functools.partial(combine_kernel, capacity),
        grid=(back.shape[0] // rows,),
        in_specs=[whole(slot), whole(ids), whole(gate), whole(off), whole(x), pl.BlockSpec((rows, d_model), lambda i: (i, 0))],
        out_specs=whole(x),
        out_shape=jax.ShapeDtypeStruct(x.shape, x.dtype),
        scratch_shapes=[pltpu.VMEM(x.shape, jnp.float32), pltpu.VMEM(ids.shape, jnp.float32)],
        compiler_params=pltpu.CompilerParams(vmem_limit_bytes=48 * 2**20),
        name='combine',
    )(slot, ids, gate, off, x, back)


def solution(mesh):
    dev_axes = ('ep2', 'ep')
    group_size = mesh.shape['ep2'] * mesh.shape['ep']

    def local_step(x_loc, ids_loc, gate_loc, w_a, w_b):
        n_tok, d_model = x_loc.shape
        n_top = ids_loc.shape[1]
        e_loc = w_a.shape[0]
        experts = e_loc * group_size
        capacity = 8 * ((5 * group_size * n_tok * n_top) // (32 * experts))
        slot, counts = route(ids_loc, experts)
        send = pack(slot, x_loc, experts * LANES)
        recv = lax.all_to_all(send.reshape(group_size, e_loc * LANES, d_model), dev_axes, 0, 0, tiled=True)
        all_counts = lax.all_gather(counts[0], dev_axes)
        earlier = jnp.arange(group_size)[:, None] < lax.axis_index(dev_axes)
        off = jnp.sum(jnp.where(earlier, all_counts, 0), axis=0, keepdims=True)
        out = expert(recv.reshape(group_size, e_loc, LANES, d_model), w_a, w_b)
        back = lax.all_to_all(out.reshape(group_size, e_loc * LANES, d_model), dev_axes, 0, 0, tiled=True)
        return combine(slot, ids_loc, gate_loc, off, x_loc, back.reshape(experts * LANES, d_model), capacity)

    tok_spec = P(('dp', 'ep2', 'ep'), None)
    w_spec = P(dev_axes, None, None)
    return jax.shard_map(local_step, mesh=mesh, in_specs=(tok_spec, tok_spec, tok_spec, w_spec, w_spec), out_specs=tok_spec, check_vma=False)
```

```python
import functools

import jax
import jax.numpy as jnp
from jax import lax
from jax.experimental import pallas as pl
from jax.experimental.pallas import tpu as pltpu
from jax.sharding import PartitionSpec as P

MESH = pl.DeviceIdType.MESH
LANES = 16
RING = 4
STRIDE = {'x': 1, 'y': RING, 'z': RING * RING}
ORDERS = ('xyz', 'yzx', 'zxy')
WIDTHS = (640, 640, 768)
STARTS = (0, 640, 1280)
PARTS = range(3)


def place():
    chip = lax.axis_index('ep')
    coord = {axis: lax.rem(chip // stride, RING) for axis, stride in STRIDE.items()}
    return lax.axis_index('ep2'), chip, coord


class Item:
    def __init__(self, axis, source, target, half, dtype, switch=False):
        self.axis, self.source, self.target, self.half, self.dtype, self.switch = axis, source, target, half, dtype, switch


def exchange_kernel(items, partner, n_in, n_out, *refs):
    refs, scratch = refs[:n_in + n_out], refs[n_in + n_out:]
    relays, (send, recv, local) = scratch[:len(items)], scratch[len(items):]
    core, chip, coord = place()
    other = 1 - core
    axes = sorted({item.axis for item in items})
    switch = any(item.switch for item in items)

    def at(axis, step):
        pos = lax.rem(coord[axis] + step + RING, RING)
        return pos, chip + (pos - coord[axis]) * STRIDE[axis]

    barrier = pltpu.get_barrier_semaphore()
    peers = 0
    for axis in axes:
        for step in (1, -1):
            for c in ((core, other) if switch else (core,)):
                pl.semaphore_signal(barrier, inc=1, device_id=(0, c, at(axis, step)[1]), device_id_type=MESH)
                peers += 1
    if switch or partner:
        pl.semaphore_signal(barrier, inc=1, device_id=(0, other, chip), device_id_type=MESH)
        peers += 1
    pl.semaphore_wait(barrier, peers)

    def remote(i, src, dst, s, r, c, to):
        return pltpu.make_async_remote_copy(src_ref=src, dst_ref=dst, send_sem=send.at[i, s], recv_sem=recv.at[i, r], device_id=(0, c, to), device_id_type=MESH)

    sent, landed, kept = [], [], []
    for i, item in enumerate(items):
        far = at(item.axis, 2)[0]
        for h, step in ((0, 1), (1, -1)):
            copy = remote(i, item.source(refs, far, h), relays[i].at[h], h, h, core, at(item.axis, step)[1])
            copy.start()
            sent.append(copy)
    for i, item in enumerate(items):
        me = coord[item.axis]
        for d, step in ((0, 1), (1, -1)):
            pos, to = at(item.axis, step)
            for h in (0, 1):
                k, c = (core, h) if item.switch else (h, core)
                copy = remote(i, item.source(refs, pos, h), item.target(refs, me, k), 2 + 2 * d + h, 2 + 2 * d + k, c, to)
                copy.start()
                sent.append(copy)
    for i, item in enumerate(items):
        me = coord[item.axis]
        if item.switch:
            copy = remote(i, item.source(refs, me, other), item.target(refs, me, core), 8, 8, other, chip)
            copy.start()
            sent.append(copy)
            own = [(item.source(refs, me, core), item.target(refs, me, core))]
        else:
            own = [(item.source(refs, me, h), item.target(refs, me, h)) for h in (0, 1)]
        for h, (src, dst) in enumerate(own):
            copy = pltpu.make_async_copy(src, dst, local.at[i, h])
            copy.start()
            kept.append(copy)
    if partner:
        n = len(items)
        copy = remote(n, refs[partner[0]], refs[partner[1]], 0, 0, other, chip)
        copy.start()
        sent.append(copy)
    for i, item in enumerate(items):
        me = coord[item.axis]
        for h, step in ((0, 1), (1, -1)):
            remote(i, relays[i].at[h], relays[i].at[h], h, h, core, chip).wait_recv()
            to = at(item.axis, step)[1]
            k, c, r = (core, h, 6 + core) if item.switch else (h, core, 6 + h)
            copy = remote(i, relays[i].at[h], item.target(refs, at(item.axis, -step)[0], k), 6 + h, r, c, to)
            copy.start()
            sent.append(copy)
    for i, item in enumerate(items):
        me = coord[item.axis]
        for d, step in ((0, -1), (1, 1)):
            for k in (0, 1):
                dst = item.target(refs, at(item.axis, step)[0], k)
                remote(i, dst, dst, 2 + 2 * d + k, 2 + 2 * d + k, core, chip).wait_recv()
        for k in (0, 1):
            dst = item.target(refs, at(item.axis, 2)[0], k)
            remote(i, dst, dst, 6 + k, 6 + k, core, chip).wait_recv()
        if item.switch:
            dst = item.target(refs, me, other)
            remote(i, dst, dst, 8, 8, core, chip).wait_recv()
    if partner:
        dst = refs[partner[1]]
        remote(len(items), dst, dst, 0, 0, core, chip).wait_recv()
    for copy in kept:
        copy.wait()
    for copy in sent:
        copy.wait_send()


def exchange(name, collective_id, items, inputs, outputs, partner=None):
    anywhere = pl.BlockSpec(memory_space=pl.ANY)
    n = len(items)
    return pl.pallas_call(
        functools.partial(exchange_kernel, items, partner, len(inputs), len(outputs)),
        in_specs=[anywhere] * len(inputs),
        out_specs=[anywhere] * len(outputs),
        out_shape=[jax.ShapeDtypeStruct(shape, dtype) for shape, dtype in outputs],
        scratch_shapes=[pltpu.VMEM((2,) + item.half, item.dtype) for item in items]
        + [pltpu.SemaphoreType.DMA((n + 1, 9)), pltpu.SemaphoreType.DMA((n + 1, 9)), pltpu.SemaphoreType.DMA((n, 2))],
        compiler_params=pltpu.CompilerParams(collective_id=collective_id, has_side_effects=True),
        name=name,
    )(*inputs)


def route_kernel(ids_ref, slot_ref, count_ref):
    ids = ids_ref[...]
    n_top, n_tok = ids.shape
    experts = 2 * count_ref.shape[2]
    expert_of = lax.broadcasted_iota(jnp.int32, (experts, n_tok), 0)
    member = jnp.zeros((experts, n_tok), jnp.float32)
    for j in range(n_top):
        member = jnp.where(expert_of == ids[j:j + 1], 1.0, member)
    row = lax.broadcasted_iota(jnp.int32, (n_tok, n_tok), 0)
    col = lax.broadcasted_iota(jnp.int32, (n_tok, n_tok), 1)
    earlier = jnp.where(row < col, 1.0, 0.0).astype(jnp.bfloat16)
    member_lp = member.astype(jnp.bfloat16)
    before = jnp.dot(member_lp, earlier, preferred_element_type=jnp.float32)
    ones = jnp.ones((n_top, n_tok), jnp.bfloat16)
    counts = lax.dot_general(ones, member_lp, (((1,), (1,)), ((), ())), preferred_element_type=jnp.float32).astype(jnp.int32)
    half = n_tok // 2
    for h in (0, 1):
        count_ref[h] = counts[:, h * half:(h + 1) * half]
    for j in range(n_top):
        rank = jnp.sum(jnp.where(expert_of == ids[j:j + 1], before, 0.0), axis=0, keepdims=True)
        slot = ids[j:j + 1] * LANES + rank.astype(jnp.int32)
        for h in (0, 1):
            slot_ref[h, j:j + 1, :] = slot[:, h * half:(h + 1) * half]


def plane_slots(shape, order, coord):
    row = lax.broadcasted_iota(jnp.int32, shape, 0)
    per_dev = 2 * LANES
    third = (row >> 5) & (RING - 1)
    core = (row >> 7) & 1
    second = row >> 8
    first, stride = coord[order[0]], [STRIDE[axis] for axis in order]
    dev = core * RING**3 + second * stride[1] + third * stride[2] + first * stride[0]
    return dev * per_dev + (row & (per_dev - 1))


def pack_kernel(*refs):
    slots, tokens, outs = refs[:3], refs[3:6], refs[6:]
    _, _, coord = place()
    for r in PARTS:
        n_tok = tokens[r].shape[1]
        rows = 2 * RING * RING * 2 * LANES
        wanted = plane_slots((rows, n_tok // 2), ORDERS[r], coord)
        picks = []
        for h in (0, 1):
            pick = jnp.zeros((rows, n_tok // 2), jnp.float32)
            for j in range(slots[r].shape[2]):
                pick = jnp.where(wanted == slots[r][0, h, j:j + 1], 1.0, pick)
            picks.append(pick.astype(jnp.bfloat16))
        got = jnp.dot(jnp.concatenate(picks, axis=1), tokens[r][0], preferred_element_type=jnp.float32).astype(jnp.bfloat16)
        outs[r][...] = got.reshape(outs[r].shape)


def pack(slots, tokens):
    lead = (RING, 2, RING)
    return pl.pallas_call(
        pack_kernel,
        grid=(RING,),
        in_specs=[pl.BlockSpec((1,) + s.shape[1:], lambda a: (a, 0, 0, 0)) for s in slots]
        + [pl.BlockSpec((1,) + t.shape[1:], lambda a: (a, 0, 0)) for t in tokens],
        out_specs=[pl.BlockSpec(lead + (1, 2 * LANES, w), lambda a: (0, 0, 0, a, 0, 0)) for w in WIDTHS],
        out_shape=[jax.ShapeDtypeStruct(lead + (RING, 2 * LANES, w), jnp.bfloat16) for w in WIDTHS],
        compiler_params=pltpu.CompilerParams(vmem_limit_bytes=48 * 2**20),
        name='pack',
    )(*slots, *tokens)


def expert_kernel(*refs):
    ins, (w_in_ref, w_out_ref), outs = refs[:3], refs[3:5], refs[5:]
    total = None
    for r in PARTS:
        shape = ins[r].shape
        rows = ins[r][...].reshape(shape[0] * shape[2], shape[3])
        term = jnp.dot(rows, w_in_ref[0, STARTS[r]:STARTS[r] + WIDTHS[r]], preferred_element_type=jnp.float32)
        total = term if total is None else total + term
    hidden = jax.nn.gelu(total, approximate=True).astype(jnp.bfloat16)
    for r in PARTS:
        out = jnp.dot(hidden, w_out_ref[0, :, STARTS[r]:STARTS[r] + WIDTHS[r]], preferred_element_type=jnp.float32)
        outs[r][...] = out.astype(jnp.bfloat16).reshape(outs[r].shape)


def expert(parts, w_in, w_out, group=32):
    e_loc, d_model, ff = w_in.shape
    shape = (2 * RING**3, e_loc, LANES)
    specs = [pl.BlockSpec((group, 1, LANES, w), lambda e, i: (i, e, 0, 0)) for w in WIDTHS]
    return pl.pallas_call(
        expert_kernel,
        grid=(e_loc, shape[0] // group),
        in_specs=specs + [pl.BlockSpec((1, d_model, ff), lambda e, i: (e, 0, 0)), pl.BlockSpec((1, ff, d_model), lambda e, i: (e, 0, 0))],
        out_specs=specs,
        out_shape=[jax.ShapeDtypeStruct(shape + (w,), jnp.bfloat16) for w in WIDTHS],
        compiler_params=pltpu.CompilerParams(vmem_limit_bytes=48 * 2**20),
        name='expert',
    )(*[p.reshape(shape + (w,)) for p, w in zip(parts, WIDTHS)], w_in, w_out)


def weight_kernel(capacity, ids_ref, slot_ref, gate_ref, mine_ref, partner_ref, out_ref):
    core, chip, _ = place()
    ids, gate = ids_ref[...], gate_ref[...]
    n_top, n_tok = ids.shape
    mine = mine_ref[...]
    ahead = lax.broadcasted_iota(jnp.int32, mine.shape, 0) < chip
    off = jnp.sum(jnp.where(ahead, mine, 0), axis=0) + jnp.where(core == 1, jnp.sum(partner_ref[...], axis=0), 0)
    off = jnp.concatenate([off[0], off[1]], axis=1)
    high = (off >> 7).astype(jnp.bfloat16)
    low = (off & 127).astype(jnp.bfloat16)
    expert_of = lax.broadcasted_iota(jnp.int32, (off.shape[1], n_tok), 0)
    half = n_tok // 2
    for j in range(n_top):
        choice = jnp.where(expert_of == ids[j:j + 1], 1.0, 0.0).astype(jnp.bfloat16)
        first = 128 * jnp.dot(high, choice, preferred_element_type=jnp.float32) + jnp.dot(low, choice, preferred_element_type=jnp.float32)
        first = first[0:1].astype(jnp.int32)
        for h in (0, 1):
            cut = slice(h * half, (h + 1) * half)
            rank = first[:, cut] + slot_ref[h, j:j + 1] - ids[j:j + 1, cut] * LANES
            out_ref[h, j:j + 1] = jnp.where(rank < capacity, gate[j:j + 1, cut], 0.0)


def combine_kernel(*refs):
    slots, gates, backs, outs = refs[:3], refs[3:6], refs[6:9], refs[9:]
    _, _, coord = place()
    for r in PARTS:
        n_tok = outs[r].shape[1]
        rows = 2 * RING * RING * 2 * LANES
        wanted = plane_slots((rows, n_tok // 2), ORDERS[r], coord)
        back = backs[r][...].reshape(rows, WIDTHS[r])
        for h in (0, 1):
            gate = jnp.zeros((rows, n_tok // 2), jnp.float32)
            for j in range(slots[r].shape[2]):
                gate = jnp.where(wanted == slots[r][0, h, j:j + 1], gates[r][0, h, j:j + 1], gate)
            high = gate.astype(jnp.bfloat16)
            rest = gate - high.astype(jnp.float32)
            mid = rest.astype(jnp.bfloat16)
            low = (rest - mid.astype(jnp.float32)).astype(jnp.bfloat16)
            gate3 = jnp.concatenate([high, mid, low], axis=1)
            mix = lax.dot_general(gate3, back, (((0,), (0,)), ((), ())), preferred_element_type=jnp.float32)
            n = n_tok // 2
            outs[r][0, h * n:(h + 1) * n] = mix[:n] + mix[n:2 * n] + mix[2 * n:]


def combine(slots, gates, backs, n_tok):
    lead = (RING, 2, RING)
    small = [pl.BlockSpec((1,) + s.shape[1:], lambda a: (a, 0, 0, 0)) for s in slots]
    return pl.pallas_call(
        combine_kernel,
        grid=(RING,),
        in_specs=small + small + [pl.BlockSpec(lead + (1, 2 * LANES, w), lambda a: (0, 0, 0, a, 0, 0)) for w in WIDTHS],
        out_specs=[pl.BlockSpec((1, n_tok, w), lambda a: (a, 0, 0)) for w in WIDTHS],
        out_shape=[jax.ShapeDtypeStruct((RING, n_tok, w), jnp.float32) for w in WIDTHS],
        compiler_params=pltpu.CompilerParams(vmem_limit_bytes=48 * 2**20),
        name='combine',
    )(*slots, *gates, *backs)


def final_kernel(x_ref, *refs):
    parts, out_ref = refs[:3], refs[3]
    for r in PARTS:
        cut = slice(STARTS[r], STARTS[r] + WIDTHS[r])
        total = x_ref[:, cut].astype(jnp.float32)
        for a in range(RING):
            total += parts[r][a]
        out_ref[:, cut] = total.astype(out_ref.dtype)


def final(x, parts, rows=64):
    n_tok, d_model = x.shape
    return pl.pallas_call(
        final_kernel,
        grid=(n_tok // rows,),
        in_specs=[pl.BlockSpec((rows, d_model), lambda i: (i, 0))] + [pl.BlockSpec((RING, rows, w), lambda i: (0, i, 0)) for w in WIDTHS],
        out_specs=pl.BlockSpec((rows, d_model), lambda i: (i, 0)),
        out_shape=jax.ShapeDtypeStruct(x.shape, x.dtype),
        name='final',
    )(x, *parts)


def spot(axis, order, index):
    return (slice(None),) * [a for a in 'zyx' if a in order].index(axis) + (index,)


def solution(mesh):
    dev_axes = ('ep2', 'ep')
    bf16, f32, i32 = jnp.bfloat16, jnp.float32, jnp.int32
    group_size = mesh.shape['ep2'] * mesh.shape['ep']

    def local_step(x, ids, gate, w_a, w_b):
        n_tok, d_model = x.shape
        n_top = ids.shape[1]
        experts = w_a.shape[0] * group_size
        capacity = 8 * ((5 * group_size * n_tok * n_top) // (32 * experts))
        small = (2, n_top, n_tok // 2)
        ids_t, gate_t = ids.T, gate.T
        slot, counts = pl.pallas_call(route_kernel, out_shape=(jax.ShapeDtypeStruct(small, i32), jax.ShapeDtypeStruct((2, n_top, experts // 2), i32)), name='route')(ids_t)
        tile = (n_top, n_tok // 2)
        half_tok = n_tok // 2
        block = (RING, RING, 2 * LANES)
        first = [o[0] for o in ORDERS]
        second = [o[1] for o in ORDERS]
        third = [o[2] for o in ORDERS]

        items = [Item(first[r], lambda f, p, h, r=r: f[0].at[pl.ds(h * half_tok, half_tok), pl.ds(STARTS[r], WIDTHS[r])],
                      lambda f, o, k, r=r: f[3 + r].at[o, pl.ds(k * half_tok, half_tok)], (half_tok, WIDTHS[r]), bf16) for r in PARTS]
        items += [Item(first[r], lambda f, p, h: f[1].at[h], lambda f, o, k, r=r: f[6 + r].at[o, k], tile, i32) for r in PARTS]
        items += [Item('x', lambda f, p, h: f[2].at[h], lambda f, o, k: f[9].at[o, k], tile, i32)]
        outs = exchange('stage_a', 0, items, [x, slot, counts],
                        [((RING, n_tok, w), bf16) for w in WIDTHS] + [((RING,) + small, i32)] * 4)
        tokens, slots, count_x = outs[:3], outs[3:6], outs[6]
        sends = pack(slots, tokens)

        items = [Item(second[r], lambda f, p, h, r=r: f[r].at[p, h],
                      lambda f, o, k, r=r: f[4 + r].at[(slice(None), k) + spot(second[r], ORDERS[r][:2], o)], block + (WIDTHS[r],), bf16, True) for r in PARTS]
        items += [Item('y', lambda f, p, h: f[3].at[:, h], lambda f, o, k: f[7].at[o, :, k], (RING,) + tile, i32)]
        mids = exchange('stage_b', 1, items, [*sends, count_x],
                        [((RING, 2) + block + (w,), bf16) for w in WIDTHS] + [((RING, RING) + small, i32)])

        items = [Item(third[r], lambda f, p, h, r=r: f[r].at[p, h],
                      lambda f, o, k, r=r: f[4 + r].at[(k,) + spot(third[r], 'zyx', o)], block + (WIDTHS[r],), bf16) for r in PARTS]
        items += [Item('z', lambda f, p, h: f[3].at[:, :, h], lambda f, o, k: f[7].at[o, :, :, k], (RING, RING) + tile, i32)]
        outs = exchange('stage_c', 2, items, list(mids),
                        [((2, RING) + block + (w,), bf16) for w in WIDTHS] + [((RING, RING, RING) + small, i32)])
        count_z = outs[3]
        results = expert(outs[:3], w_a, w_b)
        results = [o.reshape((2, RING) + block + (w,)) for o, w in zip(results, WIDTHS)]

        items = [Item(third[r], lambda f, p, h, r=r: f[r].at[(h,) + spot(third[r], 'zyx', p)],
                      lambda f, o, k, r=r: f[4 + r].at[o, k], block + (WIDTHS[r],), bf16) for r in PARTS]
        outs = exchange('stage_c_back', 3, items, [*results, count_z],
                        [((RING, 2) + block + (w,), bf16) for w in WIDTHS] + [(count_z.shape, i32)], partner=(3, 7))
        mids, count_other = outs[:3], outs[3]
        chips = (RING**3,) + small
        gates = pl.pallas_call(functools.partial(weight_kernel, capacity), out_shape=jax.ShapeDtypeStruct(small, f32), name='weight')(
            ids_t, slot, gate_t, count_z.reshape(chips), count_other.reshape(chips))
        items = [Item(second[r], lambda f, p, h, r=r: f[r].at[(slice(None), h) + spot(second[r], ORDERS[r][:2], p)],
                      lambda f, o, k, r=r: f[4 + r].at[o, k], block + (WIDTHS[r],), bf16, True) for r in PARTS]
        items += [Item(first[r], lambda f, p, h: f[3].at[h], lambda f, o, k, r=r: f[7 + r].at[o, k], tile, f32) for r in PARTS]
        outs = exchange('stage_b_back', 4, items, [*mids, gates],
                        [((RING, 2) + block + (w,), bf16) for w in WIDTHS] + [((RING,) + small, f32)] * 3)
        partial = combine(slots, outs[3:], outs[:3], n_tok)

        items = [Item(first[r], lambda f, p, h, r=r: f[r].at[p, pl.ds(h * half_tok, half_tok)],
                      lambda f, o, k, r=r: f[3 + r].at[o, pl.ds(k * half_tok, half_tok)], (half_tok, WIDTHS[r]), f32) for r in PARTS]
        parts = exchange('stage_a_back', 5, items, list(partial), [((RING, n_tok, w), f32) for w in WIDTHS])
        return final(x, parts)

    tok_spec = P(('dp', 'ep2', 'ep'), None)
    w_spec = P(dev_axes, None, None)
    return jax.shard_map(local_step, mesh=mesh, in_specs=(tok_spec, tok_spec, tok_spec, w_spec, w_spec), out_specs=tok_spec, check_vma=False)
```

```python
import functools

import jax
import jax.numpy as jnp
from jax import lax
from jax.experimental import pallas as pl
from jax.experimental.pallas import tpu as pltpu
from jax.sharding import PartitionSpec as P

MESH = pl.DeviceIdType.MESH
LANES = 16
RING = 4
STRIDE = {'x': 1, 'y': RING, 'z': RING * RING}
ORDERS = ('xyz', 'yzx', 'zxy')
WIDTHS = (640, 640, 768)
STARTS = (0, 640, 1280)
PARTS = range(3)


def place():
    chip = lax.axis_index('ep')
    coord = {axis: lax.rem(chip // stride, RING) for axis, stride in STRIDE.items()}
    return lax.axis_index('ep2'), chip, coord


class Item:
    def __init__(self, axis, source, target, half, dtype, switch=False):
        self.axis, self.source, self.target, self.half, self.dtype, self.switch = axis, source, target, half, dtype, switch


def exchange_kernel(items, partner, n_in, n_out, *refs):
    refs, scratch = refs[:n_in + n_out], refs[n_in + n_out:]
    relays, bounces, (send, recv, local) = scratch[:len(items)], scratch[len(items):2 * len(items)], scratch[2 * len(items):]
    core, chip, coord = place()
    other = 1 - core
    loads = []
    for i, item in enumerate(items):
        me = coord[item.axis]
        own = [(core, core)] if item.switch else [(0, 0), (1, 1)]
        for n, (h, k) in enumerate(own):
            copy = pltpu.make_async_copy(item.source(refs, me, h), bounces[i].at[n], local.at[i, n])
            copy.start()
            loads.append((copy, bounces[i].at[n], item.target(refs, me, k), local.at[i, 2 + n]))
    axes = sorted({item.axis for item in items})
    switch = any(item.switch for item in items)

    def at(axis, step):
        pos = lax.rem(coord[axis] + step + RING, RING)
        return pos, chip + (pos - coord[axis]) * STRIDE[axis]

    barrier = pltpu.get_barrier_semaphore()
    peers = 0
    for axis in axes:
        for step in (1, -1):
            for c in ((core, other) if switch else (core,)):
                pl.semaphore_signal(barrier, inc=1, device_id=(0, c, at(axis, step)[1]), device_id_type=MESH)
                peers += 1
    if switch or partner:
        pl.semaphore_signal(barrier, inc=1, device_id=(0, other, chip), device_id_type=MESH)
        peers += 1
    pl.semaphore_wait(barrier, peers)

    def remote(i, src, dst, s, r, c, to):
        return pltpu.make_async_remote_copy(src_ref=src, dst_ref=dst, send_sem=send.at[i, s], recv_sem=recv.at[i, r], device_id=(0, c, to), device_id_type=MESH)

    sent, landed, kept = [], [], []
    for i, item in enumerate(items):
        far = at(item.axis, 2)[0]
        for h, step in ((0, 1), (1, -1)):
            copy = remote(i, item.source(refs, far, h), relays[i].at[h], h, h, core, at(item.axis, step)[1])
            copy.start()
            sent.append(copy)
    for i, item in enumerate(items):
        me = coord[item.axis]
        for d, step in ((0, 1), (1, -1)):
            pos, to = at(item.axis, step)
            for h in (0, 1):
                k, c = (core, h) if item.switch else (h, core)
                copy = remote(i, item.source(refs, pos, h), item.target(refs, me, k), 2 + 2 * d + h, 2 + 2 * d + k, c, to)
                copy.start()
                sent.append(copy)
    for i, item in enumerate(items):
        me = coord[item.axis]
        if item.switch:
            copy = remote(i, item.source(refs, me, other), item.target(refs, me, core), 8, 8, other, chip)
            copy.start()
            sent.append(copy)
    if partner:
        n = len(items)
        copy = remote(n, refs[partner[0]], refs[partner[1]], 0, 0, other, chip)
        copy.start()
        sent.append(copy)
    for load, src, dst, sem in loads:
        load.wait()
        copy = pltpu.make_async_copy(src, dst, sem)
        copy.start()
        kept.append(copy)
    for i, item in enumerate(items):
        for h, step in ((0, 1), (1, -1)):
            remote(i, relays[i].at[h], relays[i].at[h], h, h, core, chip).wait_recv()
            to = at(item.axis, step)[1]
            k, c, r = (core, h, 6 + core) if item.switch else (h, core, 6 + h)
            copy = remote(i, relays[i].at[h], item.target(refs, at(item.axis, -step)[0], k), 6 + h, r, c, to)
            copy.start()
            sent.append(copy)
    for i, item in enumerate(items):
        me = coord[item.axis]
        for d, step in ((0, -1), (1, 1)):
            for k in (0, 1):
                dst = item.target(refs, at(item.axis, step)[0], k)
                remote(i, dst, dst, 2 + 2 * d + k, 2 + 2 * d + k, core, chip).wait_recv()
        for k in (0, 1):
            dst = item.target(refs, at(item.axis, 2)[0], k)
            remote(i, dst, dst, 6 + k, 6 + k, core, chip).wait_recv()
        if item.switch:
            dst = item.target(refs, me, other)
            remote(i, dst, dst, 8, 8, core, chip).wait_recv()
    if partner:
        dst = refs[partner[1]]
        remote(len(items), dst, dst, 0, 0, core, chip).wait_recv()
    for copy in kept:
        copy.wait()
    for copy in sent:
        copy.wait_send()


def exchange(name, collective_id, items, inputs, outputs, partner=None):
    anywhere = pl.BlockSpec(memory_space=pl.ANY)
    n = len(items)
    return pl.pallas_call(
        functools.partial(exchange_kernel, items, partner, len(inputs), len(outputs)),
        in_specs=[anywhere] * len(inputs),
        out_specs=[anywhere] * len(outputs),
        out_shape=[jax.ShapeDtypeStruct(shape, dtype) for shape, dtype in outputs],
        scratch_shapes=[pltpu.VMEM((2,) + item.half, item.dtype) for item in items]
        + [pltpu.VMEM((1 if item.switch else 2,) + item.half, item.dtype) for item in items]
        + [pltpu.SemaphoreType.DMA((n + 1, 9)), pltpu.SemaphoreType.DMA((n + 1, 9)), pltpu.SemaphoreType.DMA((n, 4))],
        compiler_params=pltpu.CompilerParams(collective_id=collective_id, has_side_effects=True),
        name=name,
    )(*inputs)


def route_kernel(ids_ref, slot_ref, count_ref):
    ids = ids_ref[...]
    n_top, n_tok = ids.shape
    experts = 2 * count_ref.shape[2]
    expert_of = lax.broadcasted_iota(jnp.int32, (experts, n_tok), 0)
    member = jnp.zeros((experts, n_tok), jnp.float32)
    for j in range(n_top):
        member = jnp.where(expert_of == ids[j:j + 1], 1.0, member)
    row = lax.broadcasted_iota(jnp.int32, (n_tok, n_tok), 0)
    col = lax.broadcasted_iota(jnp.int32, (n_tok, n_tok), 1)
    earlier = jnp.where(row < col, 1.0, 0.0).astype(jnp.bfloat16)
    member_lp = member.astype(jnp.bfloat16)
    before = jnp.dot(member_lp, earlier, preferred_element_type=jnp.float32)
    ones = jnp.ones((n_top, n_tok), jnp.bfloat16)
    counts = lax.dot_general(ones, member_lp, (((1,), (1,)), ((), ())), preferred_element_type=jnp.float32).astype(jnp.int32)
    half = n_tok // 2
    for h in (0, 1):
        count_ref[h] = counts[:, h * half:(h + 1) * half]
    for j in range(n_top):
        rank = jnp.sum(jnp.where(expert_of == ids[j:j + 1], before, 0.0), axis=0, keepdims=True)
        slot = ids[j:j + 1] * LANES + rank.astype(jnp.int32)
        for h in (0, 1):
            slot_ref[h, j:j + 1, :] = slot[:, h * half:(h + 1) * half]


def plane_slots(shape, order, coord):
    row = lax.broadcasted_iota(jnp.int32, shape, 0)
    per_dev = 2 * LANES
    third = (row >> 5) & (RING - 1)
    core = (row >> 7) & 1
    second = row >> 8
    first, stride = coord[order[0]], [STRIDE[axis] for axis in order]
    dev = core * RING**3 + second * stride[1] + third * stride[2] + first * stride[0]
    return dev * per_dev + (row & (per_dev - 1))


def pack_kernel(*refs):
    slots, tokens, outs = refs[:3], refs[3:6], refs[6:]
    _, _, coord = place()
    for r in PARTS:
        n_tok = tokens[r].shape[1]
        rows = 2 * RING * RING * 2 * LANES
        wanted = plane_slots((rows, n_tok // 2), ORDERS[r], coord)
        picks = []
        for h in (0, 1):
            pick = jnp.zeros((rows, n_tok // 2), jnp.float32)
            for j in range(slots[r].shape[2]):
                pick = jnp.where(wanted == slots[r][0, h, j:j + 1], 1.0, pick)
            picks.append(pick.astype(jnp.bfloat16))
        got = jnp.dot(jnp.concatenate(picks, axis=1), tokens[r][0], preferred_element_type=jnp.float32).astype(jnp.bfloat16)
        outs[r][...] = got.reshape(outs[r].shape)


def pack(slots, tokens):
    lead = (RING, 2, RING)
    return pl.pallas_call(
        pack_kernel,
        grid=(RING,),
        in_specs=[pl.BlockSpec((1,) + s.shape[1:], lambda a: (a, 0, 0, 0)) for s in slots]
        + [pl.BlockSpec((1,) + t.shape[1:], lambda a: (a, 0, 0)) for t in tokens],
        out_specs=[pl.BlockSpec(lead + (1, 2 * LANES, w), lambda a: (0, 0, 0, a, 0, 0)) for w in WIDTHS],
        out_shape=[jax.ShapeDtypeStruct(lead + (RING, 2 * LANES, w), jnp.bfloat16) for w in WIDTHS],
        compiler_params=pltpu.CompilerParams(vmem_limit_bytes=48 * 2**20),
        name='pack',
    )(*slots, *tokens)


def expert_kernel(*refs):
    ins, (w_in_ref, w_out_ref), outs = refs[:3], refs[3:5], refs[5:]
    total = None
    for r in PARTS:
        shape = ins[r].shape
        rows = ins[r][...].reshape(shape[0] * shape[2], shape[3])
        term = jnp.dot(rows, w_in_ref[0, STARTS[r]:STARTS[r] + WIDTHS[r]], preferred_element_type=jnp.float32)
        total = term if total is None else total + term
    hidden = jax.nn.gelu(total, approximate=True).astype(jnp.bfloat16)
    for r in PARTS:
        out = jnp.dot(hidden, w_out_ref[0, :, STARTS[r]:STARTS[r] + WIDTHS[r]], preferred_element_type=jnp.float32)
        outs[r][...] = out.astype(jnp.bfloat16).reshape(outs[r].shape)


def expert(parts, w_in, w_out, group=32):
    e_loc, d_model, ff = w_in.shape
    shape = (2 * RING**3, e_loc, LANES)
    specs = [pl.BlockSpec((group, 1, LANES, w), lambda e, i: (i, e, 0, 0)) for w in WIDTHS]
    return pl.pallas_call(
        expert_kernel,
        grid=(e_loc, shape[0] // group),
        in_specs=specs + [pl.BlockSpec((1, d_model, ff), lambda e, i: (e, 0, 0)), pl.BlockSpec((1, ff, d_model), lambda e, i: (e, 0, 0))],
        out_specs=specs,
        out_shape=[jax.ShapeDtypeStruct(shape + (w,), jnp.bfloat16) for w in WIDTHS],
        compiler_params=pltpu.CompilerParams(vmem_limit_bytes=48 * 2**20),
        name='expert',
    )(*[p.reshape(shape + (w,)) for p, w in zip(parts, WIDTHS)], w_in, w_out)


def weight_kernel(capacity, ids_ref, slot_ref, gate_ref, mine_ref, partner_ref, out_ref):
    core, chip, _ = place()
    ids, gate = ids_ref[...], gate_ref[...]
    n_top, n_tok = ids.shape
    mine = mine_ref[...]
    ahead = lax.broadcasted_iota(jnp.int32, mine.shape, 0) < chip
    off = jnp.sum(jnp.where(ahead, mine, 0), axis=0) + jnp.where(core == 1, jnp.sum(partner_ref[...], axis=0), 0)
    off = jnp.concatenate([off[0], off[1]], axis=1)
    high = (off >> 7).astype(jnp.bfloat16)
    low = (off & 127).astype(jnp.bfloat16)
    expert_of = lax.broadcasted_iota(jnp.int32, (off.shape[1], n_tok), 0)
    half = n_tok // 2
    for j in range(n_top):
        choice = jnp.where(expert_of == ids[j:j + 1], 1.0, 0.0).astype(jnp.bfloat16)
        first = 128 * jnp.dot(high, choice, preferred_element_type=jnp.float32) + jnp.dot(low, choice, preferred_element_type=jnp.float32)
        first = first[0:1].astype(jnp.int32)
        for h in (0, 1):
            cut = slice(h * half, (h + 1) * half)
            rank = first[:, cut] + slot_ref[h, j:j + 1] - ids[j:j + 1, cut] * LANES
            out_ref[h, j:j + 1] = jnp.where(rank < capacity, gate[j:j + 1, cut], 0.0)


def combine_kernel(*refs):
    slots, gates, backs, outs = refs[:3], refs[3:6], refs[6:9], refs[9:]
    _, _, coord = place()
    for r in PARTS:
        n_tok = outs[r].shape[1]
        rows = 2 * RING * RING * 2 * LANES
        wanted = plane_slots((rows, n_tok // 2), ORDERS[r], coord)
        back = backs[r][...].reshape(rows, WIDTHS[r])
        for h in (0, 1):
            gate = jnp.zeros((rows, n_tok // 2), jnp.float32)
            for j in range(slots[r].shape[2]):
                gate = jnp.where(wanted == slots[r][0, h, j:j + 1], gates[r][0, h, j:j + 1], gate)
            high = gate.astype(jnp.bfloat16)
            rest = gate - high.astype(jnp.float32)
            mid = rest.astype(jnp.bfloat16)
            low = (rest - mid.astype(jnp.float32)).astype(jnp.bfloat16)
            gate3 = jnp.concatenate([high, mid, low], axis=1)
            mix = lax.dot_general(gate3, back, (((0,), (0,)), ((), ())), preferred_element_type=jnp.float32)
            n = n_tok // 2
            outs[r][0, h * n:(h + 1) * n] = mix[:n] + mix[n:2 * n] + mix[2 * n:]


def combine(slots, gates, backs, n_tok):
    lead = (RING, 2, RING)
    small = [pl.BlockSpec((1,) + s.shape[1:], lambda a: (a, 0, 0, 0)) for s in slots]
    return pl.pallas_call(
        combine_kernel,
        grid=(RING,),
        in_specs=small + small + [pl.BlockSpec(lead + (1, 2 * LANES, w), lambda a: (0, 0, 0, a, 0, 0)) for w in WIDTHS],
        out_specs=[pl.BlockSpec((1, n_tok, w), lambda a: (a, 0, 0)) for w in WIDTHS],
        out_shape=[jax.ShapeDtypeStruct((RING, n_tok, w), jnp.float32) for w in WIDTHS],
        compiler_params=pltpu.CompilerParams(vmem_limit_bytes=48 * 2**20),
        name='combine',
    )(*slots, *gates, *backs)


def final_kernel(x_ref, *refs):
    parts, out_ref = refs[:3], refs[3]
    for r in PARTS:
        cut = slice(STARTS[r], STARTS[r] + WIDTHS[r])
        total = x_ref[:, cut].astype(jnp.float32)
        for a in range(RING):
            total += parts[r][a]
        out_ref[:, cut] = total.astype(out_ref.dtype)


def final(x, parts, rows=64):
    n_tok, d_model = x.shape
    return pl.pallas_call(
        final_kernel,
        grid=(n_tok // rows,),
        in_specs=[pl.BlockSpec((rows, d_model), lambda i: (i, 0))] + [pl.BlockSpec((RING, rows, w), lambda i: (0, i, 0)) for w in WIDTHS],
        out_specs=pl.BlockSpec((rows, d_model), lambda i: (i, 0)),
        out_shape=jax.ShapeDtypeStruct(x.shape, x.dtype),
        name='final',
    )(x, *parts)


def spot(axis, order, index):
    return (slice(None),) * [a for a in 'zyx' if a in order].index(axis) + (index,)


def solution(mesh):
    dev_axes = ('ep2', 'ep')
    bf16, f32, i32 = jnp.bfloat16, jnp.float32, jnp.int32
    group_size = mesh.shape['ep2'] * mesh.shape['ep']

    def local_step(x, ids, gate, w_a, w_b):
        n_tok, d_model = x.shape
        n_top = ids.shape[1]
        experts = w_a.shape[0] * group_size
        capacity = 8 * ((5 * group_size * n_tok * n_top) // (32 * experts))
        small = (2, n_top, n_tok // 2)
        ids_t, gate_t = ids.T, gate.T
        slot, counts = pl.pallas_call(route_kernel, out_shape=(jax.ShapeDtypeStruct(small, i32), jax.ShapeDtypeStruct((2, n_top, experts // 2), i32)), name='route')(ids_t)
        tile = (n_top, n_tok // 2)
        half_tok = n_tok // 2
        block = (RING, RING, 2 * LANES)
        first = [o[0] for o in ORDERS]
        second = [o[1] for o in ORDERS]
        third = [o[2] for o in ORDERS]

        items = [Item(first[r], lambda f, p, h, r=r: f[0].at[pl.ds(h * half_tok, half_tok), pl.ds(STARTS[r], WIDTHS[r])],
                      lambda f, o, k, r=r: f[3 + r].at[o, pl.ds(k * half_tok, half_tok)], (half_tok, WIDTHS[r]), bf16) for r in PARTS]
        items += [Item(first[r], lambda f, p, h: f[1].at[h], lambda f, o, k, r=r: f[6 + r].at[o, k], tile, i32) for r in PARTS]
        items += [Item('x', lambda f, p, h: f[2].at[h], lambda f, o, k: f[9].at[o, k], tile, i32)]
        outs = exchange('stage_a', 0, items, [x, slot, counts],
                        [((RING, n_tok, w), bf16) for w in WIDTHS] + [((RING,) + small, i32)] * 4)
        tokens, slots, count_x = outs[:3], outs[3:6], outs[6]
        sends = pack(slots, tokens)

        items = [Item(second[r], lambda f, p, h, r=r: f[r].at[p, h],
                      lambda f, o, k, r=r: f[4 + r].at[(slice(None), k) + spot(second[r], ORDERS[r][:2], o)], block + (WIDTHS[r],), bf16, True) for r in PARTS]
        items += [Item('y', lambda f, p, h: f[3].at[:, h], lambda f, o, k: f[7].at[o, :, k], (RING,) + tile, i32)]
        mids = exchange('stage_b', 1, items, [*sends, count_x],
                        [((RING, 2) + block + (w,), bf16) for w in WIDTHS] + [((RING, RING) + small, i32)])

        items = [Item(third[r], lambda f, p, h, r=r: f[r].at[p, h],
                      lambda f, o, k, r=r: f[4 + r].at[(k,) + spot(third[r], 'zyx', o)], block + (WIDTHS[r],), bf16) for r in PARTS]
        items += [Item('z', lambda f, p, h: f[3].at[:, :, h], lambda f, o, k: f[7].at[o, :, :, k], (RING, RING) + tile, i32)]
        outs = exchange('stage_c', 2, items, list(mids),
                        [((2, RING) + block + (w,), bf16) for w in WIDTHS] + [((RING, RING, RING) + small, i32)])
        count_z = outs[3]
        results = expert(outs[:3], w_a, w_b)
        results = [o.reshape((2, RING) + block + (w,)) for o, w in zip(results, WIDTHS)]

        items = [Item(third[r], lambda f, p, h, r=r: f[r].at[(h,) + spot(third[r], 'zyx', p)],
                      lambda f, o, k, r=r: f[4 + r].at[o, k], block + (WIDTHS[r],), bf16) for r in PARTS]
        outs = exchange('stage_c_back', 3, items, [*results, count_z],
                        [((RING, 2) + block + (w,), bf16) for w in WIDTHS] + [(count_z.shape, i32)], partner=(3, 7))
        mids, count_other = outs[:3], outs[3]
        chips = (RING**3,) + small
        gates = pl.pallas_call(functools.partial(weight_kernel, capacity), out_shape=jax.ShapeDtypeStruct(small, f32), name='weight')(
            ids_t, slot, gate_t, count_z.reshape(chips), count_other.reshape(chips))
        items = [Item(second[r], lambda f, p, h, r=r: f[r].at[(slice(None), h) + spot(second[r], ORDERS[r][:2], p)],
                      lambda f, o, k, r=r: f[4 + r].at[o, k], block + (WIDTHS[r],), bf16, True) for r in PARTS]
        items += [Item(first[r], lambda f, p, h: f[3].at[h], lambda f, o, k, r=r: f[7 + r].at[o, k], tile, f32) for r in PARTS]
        outs = exchange('stage_b_back', 4, items, [*mids, gates],
                        [((RING, 2) + block + (w,), bf16) for w in WIDTHS] + [((RING,) + small, f32)] * 3)
        partial = combine(slots, outs[3:], outs[:3], n_tok)

        items = [Item(first[r], lambda f, p, h, r=r: f[r].at[p, pl.ds(h * half_tok, half_tok)],
                      lambda f, o, k, r=r: f[3 + r].at[o, pl.ds(k * half_tok, half_tok)], (half_tok, WIDTHS[r]), f32) for r in PARTS]
        parts = exchange('stage_a_back', 5, items, list(partial), [((RING, n_tok, w), f32) for w in WIDTHS])
        return final(x, parts)

    tok_spec = P(('dp', 'ep2', 'ep'), None)
    w_spec = P(dev_axes, None, None)
    return jax.shard_map(local_step, mesh=mesh, in_specs=(tok_spec, tok_spec, tok_spec, w_spec, w_spec), out_specs=tok_spec, check_vma=False)
```

```python
import functools

import jax
import jax.numpy as jnp
from jax import lax
from jax.experimental import pallas as pl
from jax.experimental.pallas import tpu as pltpu
from jax.sharding import PartitionSpec as P

MESH = pl.DeviceIdType.MESH
LANES = 16
RING = 4
STRIDE = {'x': 1, 'y': RING, 'z': RING * RING}
ORDERS = ('xyz', 'yzx', 'zxy')
STREAMS = range(2)
PARTS = range(3)
WIDTHS = ((640, 640, 768), (768, 640, 640))
STARTS = ((0, 640, 1280), (0, 768, 1408))
SPAN = 768
SPAN_STARTS = (0, 640, 1280)
BOTH = [(q, r) for q in STREAMS for r in PARTS]


class Place:
    def __init__(self):
        self.core, self.chip = lax.axis_index('ep2'), lax.axis_index('ep')
        self.other = 1 - self.core
        self.coord = {axis: lax.rem(self.chip // stride, RING) for axis, stride in STRIDE.items()}

    def pos(self, axis, step):
        return lax.rem(self.coord[axis] + step + RING, RING)

    def at(self, axis, step):
        return self.chip + (self.pos(axis, step) - self.coord[axis]) * STRIDE[axis]

    def greet(self, both_cores):
        barrier = pltpu.get_barrier_semaphore()
        peers = [(self.other, self.chip)]
        for axis in STRIDE:
            for step in (1, -1):
                peers += [(c, self.at(axis, step)) for c in ((self.core, self.other) if both_cores else (self.core,))]
        for c, chip in peers:
            pl.semaphore_signal(barrier, inc=1, device_id=(0, c, chip), device_id_type=MESH)
        pl.semaphore_wait(barrier, len(peers))


class Lane:
    def __init__(self, place, axis, source, target, relay, send, recv, index, switch=False):
        self.place, self.axis, self.source, self.target, self.relay = place, axis, source, target, relay
        self.send, self.recv, self.index, self.switch = send, recv, index, switch
        self.sent = []

    def start(self, src, dst, s, r, core, chip):
        copy = pltpu.make_async_remote_copy(src_ref=src, dst_ref=dst, send_sem=self.send.at[self.index, s], recv_sem=self.recv.at[self.index, r], device_id=(0, core, chip), device_id_type=MESH)
        copy.start()
        self.sent.append(copy)

    def landed(self, dst, r):
        pltpu.make_async_remote_copy(src_ref=dst, dst_ref=dst, send_sem=self.send.at[self.index, 0], recv_sem=self.recv.at[self.index, r], device_id=(0, self.place.core, self.place.chip), device_id_type=MESH).wait_recv()

    def far(self):
        p = self.place
        for h, step in ((0, 1), (1, -1)):
            self.start(self.source(p.pos(self.axis, 2), h), self.relay.at[h], h, h, p.core, p.at(self.axis, step))

    def near(self):
        p = self.place
        me = p.coord[self.axis]
        for d, step in ((0, 1), (1, -1)):
            for h in (0, 1):
                k, c = (p.core, h) if self.switch else (h, p.core)
                self.start(self.source(p.pos(self.axis, step), h), self.target(me, k), 2 + 2 * d + h, 2 + 2 * d + k, c, p.at(self.axis, step))
        if self.switch:
            self.start(self.source(me, p.other), self.target(me, p.core), 8, 8, p.other, p.chip)

    def forward(self):
        p = self.place
        for h, step in ((0, 1), (1, -1)):
            self.landed(self.relay.at[h], h)
            k, c, r = (p.core, h, 6 + p.core) if self.switch else (h, p.core, 6 + h)
            self.start(self.relay.at[h], self.target(p.pos(self.axis, -step), k), 6 + h, r, c, p.at(self.axis, step))

    def arrive(self):
        p = self.place
        for d, step in ((0, -1), (1, 1)):
            for k in (0, 1):
                self.landed(self.target(p.pos(self.axis, step), k), 2 + 2 * d + k)
        for k in (0, 1):
            self.landed(self.target(p.pos(self.axis, 2), k), 6 + k)
        if self.switch:
            self.landed(self.target(p.coord[self.axis], p.other), 8)

    def own(self, local):
        p = self.place
        me = p.coord[self.axis]
        halves = [(p.core, p.core)] if self.switch else [(0, 0), (1, 1)]
        copies = [pltpu.make_async_copy(self.source(me, h), self.target(me, k), local.at[self.index, n]) for n, (h, k) in enumerate(halves)]
        for copy in copies:
            copy.start()
        return copies

    def drain(self):
        for copy in self.sent:
            copy.wait_send()


class Gather(Lane):
    def forward(self):
        p = self.place
        for h, step in ((0, 1), (1, -1)):
            part = self.target(p.pos(self.axis, -step), h)
            self.landed(part, 2 + 2 * h + h)
            self.start(part, part, 6 + h, 6 + h, p.core, p.at(self.axis, step))

    def arrive_near(self):
        p = self.place
        self.landed(self.target(p.pos(self.axis, -1), 1), 3)
        self.landed(self.target(p.pos(self.axis, 1), 0), 4)

    def arrive_far(self):
        for h in (0, 1):
            self.landed(self.target(self.place.pos(self.axis, 2), h), 6 + h)


def run(lanes, *steps):
    for step in steps:
        for lane in lanes:
            getattr(lane, step)()


def take(refs, *counts):
    refs = list(refs)
    for count in counts:
        yield refs[:count]
        del refs[:count]


def spot(axis, order, index):
    return (slice(None),) * [a for a in 'zyx' if a in order].index(axis) + (index,)


def plane_slots(shape, order, place, q):
    row = lax.broadcasted_iota(jnp.int32, shape, 0)
    first, second, third = [STRIDE[axis] for axis in order]
    dev = ((row >> 6) & 1) * RING**3 + (row >> 7) * second + ((row >> 4) & (RING - 1)) * third + place.coord[order[0]] * first
    return dev * (2 * LANES) + q * LANES + (row & (LANES - 1))


def route_kernel(ids_ref, slot_ref, count_ref):
    ids = ids_ref[...]
    n_top, n_tok = ids.shape
    experts = 2 * count_ref.shape[2]
    expert_of = lax.broadcasted_iota(jnp.int32, (experts, n_tok), 0)
    member = jnp.zeros((experts, n_tok), jnp.float32)
    for j in range(n_top):
        member = jnp.where(expert_of == ids[j:j + 1], 1.0, member)
    row = lax.broadcasted_iota(jnp.int32, (n_tok, n_tok), 0)
    col = lax.broadcasted_iota(jnp.int32, (n_tok, n_tok), 1)
    earlier = jnp.where(row < col, 1.0, 0.0).astype(jnp.bfloat16)
    member_lp = member.astype(jnp.bfloat16)
    before = jnp.dot(member_lp, earlier, preferred_element_type=jnp.float32)
    ones = jnp.ones((n_top, n_tok), jnp.bfloat16)
    counts = lax.dot_general(ones, member_lp, (((1,), (1,)), ((), ())), preferred_element_type=jnp.float32).astype(jnp.int32)
    half = n_tok // 2
    for h in (0, 1):
        count_ref[h] = counts[:, h * half:(h + 1) * half]
    for j in range(n_top):
        rank = jnp.sum(jnp.where(expert_of == ids[j:j + 1], before, 0.0), axis=0, keepdims=True)
        slot = ids[j:j + 1] * LANES + rank.astype(jnp.int32)
        for h in (0, 1):
            slot_ref[h, j:j + 1, :] = slot[:, h * half:(h + 1) * half]


def send_kernel(*refs):
    (x, slot, count), mids, (count_y,), tokens, slots, (count_x,), rows, relays, (send, recv, local) = take(refs, 3, 6, 1, 3, 3, 1, 6, 6, 3)
    place = Place()
    n_tok = x.shape[0]
    half = n_tok // 2
    cut = lambda r: pl.ds(SPAN_STARTS[r], SPAN)
    lane = functools.partial(Lane, place, send=send, recv=recv)
    gather = functools.partial(Gather, place, relay=None, send=send, recv=recv)
    first = [gather(axis=ORDERS[r][0], index=r, source=lambda p, h, r=r: x.at[pl.ds(h * half, half), cut(r)],
                    target=lambda o, k, r=r: tokens[r].at[o, pl.ds(k * half, half)]) for r in PARTS]
    small = [gather(axis=ORDERS[r][0], index=3 + r, source=lambda p, h: slot.at[h], target=lambda o, k, r=r: slots[r].at[o, k]) for r in PARTS]
    small.append(gather(axis='x', index=6, source=lambda p, h: count.at[h], target=lambda o, k: count_x.at[o, k]))
    along_y = gather(axis='y', index=7, source=lambda p, h: count_x.at[:, h], target=lambda o, k: count_y.at[o, :, k])
    second = [lane(axis=ORDERS[r][1], index=8 + 3 * q + r, switch=True, relay=relays[3 * q + r],
                   source=lambda p, h, i=3 * q + r: rows[i].at[p, h],
                   target=lambda o, k, i=3 * q + r, r=r: mids[i].at[(slice(None), k) + spot(ORDERS[r][1], ORDERS[r][:2], o)]) for q, r in BOTH]
    kept = [copy for item in small + first for copy in item.own(local)]
    place.greet(True)
    run(small, 'near')
    run(first, 'near')

    def pack(q, r, step):
        a = place.pos(ORDERS[r][0], step)
        n_row = 2 * RING * RING * LANES
        wanted = plane_slots((n_row, half), ORDERS[r], place, q)
        picks = []
        for h in (0, 1):
            pick = jnp.zeros((n_row, half), jnp.float32)
            for j in range(slots[r].shape[2]):
                pick = jnp.where(wanted == slots[r][a, h, j:j + 1], 1.0, pick)
            picks.append(pick.astype(jnp.bfloat16))
        offset = STARTS[q][r] - SPAN_STARTS[r]
        got = jnp.dot(jnp.concatenate(picks, axis=1), tokens[r][a, :, offset:offset + WIDTHS[q][r]], preferred_element_type=jnp.float32)
        rows[3 * q + r][:, :, :, a] = got.astype(jnp.bfloat16).reshape(RING, 2, RING, LANES, WIDTHS[q][r])

    for copy in kept:
        copy.wait()
    for r in PARTS:
        pack(0, r, 0)
    run(small, 'forward')
    run(first, 'forward')
    run(small, 'arrive_near', 'arrive_far')
    run(first, 'arrive_near')
    kept = along_y.own(local)
    run([along_y], 'near')
    for r in PARTS:
        pl.loop(0, 2)(lambda n, r=r: pack(0, r, 1 + 2 * n))
    run(first, 'arrive_far')
    for r in PARTS:
        pack(0, r, 2)
    run(second[:3], 'far', 'near')
    for r in PARTS:
        pl.loop(0, RING)(lambda n, r=r: pack(1, r, n))
    run(second[:3], 'forward')
    run(second[3:], 'far', 'near')
    run([along_y], 'forward')
    for item in second:
        kept += item.own(local)
    run(second[3:], 'forward')
    run([along_y], 'arrive_near', 'arrive_far')
    run(second, 'arrive')
    for copy in kept:
        copy.wait()
    run(small + first + [along_y] + second, 'drain')


def expert_stage_kernel(*refs):
    mids, (w_in, w_out, count_y), backs, (count_z, count_other), rows, relays, back_relays, (w_in_v, w_out_v), (send, recv, local, extra) = take(refs, 6, 3, 6, 2, 6, 6, 6, 2, 4)
    place = Place()
    lane = functools.partial(Lane, place, send=send, recv=recv)
    out = [lane(axis=ORDERS[r][2], index=3 * q + r, relay=relays[3 * q + r], source=lambda p, h, i=3 * q + r: mids[i].at[p, h],
                target=lambda o, k, i=3 * q + r, r=r: rows[i].at[(k,) + spot(ORDERS[r][2], 'zyx', o)]) for q, r in BOTH]
    back = [lane(axis=ORDERS[r][2], index=6 + 3 * q + r, relay=back_relays[3 * q + r], target=lambda o, k, i=3 * q + r: backs[i].at[o, k],
                 source=lambda p, h, i=3 * q + r, r=r: rows[i].at[(h,) + spot(ORDERS[r][2], 'zyx', p)]) for q, r in BOTH]
    along_z = Gather(place, 'z', lambda p, h: count_y.at[:, :, h], lambda o, k: count_z.at[o, :, :, k], None, send, recv, 12)
    loads = [pltpu.make_async_copy(w_in, w_in_v, extra.at[0]), pltpu.make_async_copy(w_out, w_out_v, extra.at[1])]
    own = [out[i].own(local) for i in range(6)] + [along_z.own(local)]
    for copy in loads:
        copy.start()
    place.greet(False)

    def expert(q, step):
        core, z = step // 2, 2 * lax.rem(step, 2)
        n_row = 2 * RING * RING * LANES
        total = None
        for r in PARTS:
            part = rows[3 * q + r][core, pl.ds(z, 2)].reshape(n_row, WIDTHS[q][r])
            term = jnp.dot(part, w_in_v[q, STARTS[q][r]:STARTS[q][r] + WIDTHS[q][r]], preferred_element_type=jnp.float32)
            total = term if total is None else total + term
        hidden = jax.nn.gelu(total, approximate=True).astype(jnp.bfloat16)
        for r in PARTS:
            res = jnp.dot(hidden, w_out_v[q, :, STARTS[q][r]:STARTS[q][r] + WIDTHS[q][r]], preferred_element_type=jnp.float32)
            rows[3 * q + r][core, pl.ds(z, 2)] = res.astype(jnp.bfloat16).reshape(2, RING, RING, LANES, WIDTHS[q][r])

    run(out[:3], 'far', 'near')
    run([along_z], 'near')
    run(out[:3], 'forward')
    run(out[3:], 'far', 'near')
    run([along_z], 'forward', 'arrive_near', 'arrive_far')
    for copy in own[6]:
        copy.wait()
    swap = Lane(place, 'z', None, None, None, send, recv, 13)
    swap.start(count_z, count_other, 0, 0, place.other, place.chip)
    for copy in loads:
        copy.wait()
    kept = []
    for q in STREAMS:
        mine, behind = slice(3 * q, 3 * q + 3), (out[3:], back[:3])[q]
        run(out[mine], 'arrive')
        for copies in own[mine]:
            for copy in copies:
                copy.wait()
        pl.loop(0, 3)(lambda n, q=q: expert(q, n))
        run(behind, 'forward')
        expert(q, 3)
        run(back[mine], 'far', 'near')
        for item in back[mine]:
            kept += item.own(local)
    run(back[3:], 'forward')
    swap.landed(count_other, 0)
    run(back, 'arrive')
    for copy in kept:
        copy.wait()
    run(out + back + [along_z, swap], 'drain')


def weight_kernel(capacity, ids_ref, slot_ref, gate_ref, mine_ref, partner_ref, out_ref):
    place = Place()
    ids, gate = ids_ref[...], gate_ref[...]
    n_top, n_tok = ids.shape
    mine = mine_ref[...]
    ahead = lax.broadcasted_iota(jnp.int32, mine.shape, 0) < place.chip
    off = jnp.sum(jnp.where(ahead, mine, 0), axis=0) + jnp.where(place.core == 1, jnp.sum(partner_ref[...], axis=0), 0)
    off = jnp.concatenate([off[0], off[1]], axis=1)
    high = (off >> 7).astype(jnp.bfloat16)
    low = (off & 127).astype(jnp.bfloat16)
    expert_of = lax.broadcasted_iota(jnp.int32, (off.shape[1], n_tok), 0)
    half = n_tok // 2
    for j in range(n_top):
        choice = jnp.where(expert_of == ids[j:j + 1], 1.0, 0.0).astype(jnp.bfloat16)
        first = 128 * jnp.dot(high, choice, preferred_element_type=jnp.float32) + jnp.dot(low, choice, preferred_element_type=jnp.float32)
        first = first[0:1].astype(jnp.int32)
        for h in (0, 1):
            cut = slice(h * half, (h + 1) * half)
            rank = first[:, cut] + slot_ref[h, j:j + 1] - ids[j:j + 1, cut] * LANES
            out_ref[h, j:j + 1] = jnp.where(rank < capacity, gate[j:j + 1, cut], 0.0)


def return_kernel(*refs):
    mids, (slot, gate, x, y), rows, relays, slots, gates, sums, got, sum_relays, (send, recv, local) = take(refs, 6, 4, 6, 6, 3, 3, 3, 3, 3, 3)
    place = Place()
    n_tok = x.shape[0]
    half = n_tok // 2
    lane = functools.partial(Lane, place, send=send, recv=recv)
    gather = functools.partial(Gather, place, relay=None, send=send, recv=recv)
    small = [gather(axis=ORDERS[r][0], index=r, source=lambda p, h: slot.at[h], target=lambda o, k, r=r: slots[r].at[o, k]) for r in PARTS]
    small += [gather(axis=ORDERS[r][0], index=3 + r, source=lambda p, h: gate.at[h], target=lambda o, k, r=r: gates[r].at[o, k]) for r in PARTS]
    second = [lane(axis=ORDERS[r][1], index=6 + 3 * q + r, switch=True, relay=relays[3 * q + r], target=lambda o, k, i=3 * q + r: rows[i].at[o, k],
                   source=lambda p, h, i=3 * q + r, r=r: mids[i].at[(slice(None), h) + spot(ORDERS[r][1], ORDERS[r][:2], p)]) for q, r in BOTH]
    first = [lane(axis=ORDERS[r][0], index=12 + r, relay=sum_relays[r], source=lambda p, h, r=r: sums[r].at[p, pl.ds(h * half, half)],
                  target=lambda o, k, r=r: got[r].at[o, pl.ds(k * half, half)]) for r in PARTS]
    kept = [copy for item in small + second for copy in item.own(local)]
    place.greet(True)
    run(small, 'near')
    run(second[:3], 'far', 'near')
    for r in PARTS:
        sums[r][...] = jnp.zeros_like(sums[r])
    run(small, 'forward', 'arrive_near', 'arrive_far')
    run(second[:3], 'forward')
    run(second[3:], 'far', 'near')
    for copy in kept:
        copy.wait()

    def combine(q, r, step, h):
        a = place.pos(ORDERS[r][0], step)
        n_row = 2 * RING * RING * LANES
        wanted = plane_slots((n_row, half), ORDERS[r], place, q)
        weight = jnp.zeros((n_row, half), jnp.float32)
        for j in range(slots[r].shape[2]):
            weight = jnp.where(wanted == slots[r][a, h, j:j + 1], gates[r][a, h, j:j + 1], weight)
        high = weight.astype(jnp.bfloat16)
        rest = weight - high.astype(jnp.float32)
        mid = rest.astype(jnp.bfloat16)
        low = (rest - mid.astype(jnp.float32)).astype(jnp.bfloat16)
        weights = jnp.concatenate([high, mid, low], axis=1)
        back = rows[3 * q + r][:, :, :, a].reshape(n_row, WIDTHS[q][r])
        mix = lax.dot_general(weights, back, (((0,), (0,)), ((), ())), preferred_element_type=jnp.float32)
        offset = STARTS[q][r] - SPAN_STARTS[r]
        sums[r][a, pl.ds(pl.multiple_of(h * half, half), half), offset:offset + WIDTHS[q][r]] += mix[:half] + mix[half:2 * half] + mix[2 * half:]

    run(second[:3], 'arrive')
    for r in PARTS:
        pl.loop(0, 2 * RING)(lambda n, r=r: combine(0, r, n // 2, lax.rem(n, 2)))
    run(second[3:], 'forward', 'arrive')
    for r in PARTS:
        pl.loop(0, 2)(lambda h, r=r: combine(1, r, 2, h))
    run(first, 'far')
    for r in PARTS:
        pl.loop(0, 4)(lambda n, r=r: combine(1, r, 1 + 2 * (n // 2), lax.rem(n, 2)))
    run(first, 'near', 'forward')
    for r in PARTS:
        pl.loop(0, 2)(lambda h, r=r: combine(1, r, 0, h))
    run(first, 'arrive')
    for c in range(0, x.shape[1], 128):
        total = x[:, c:c + 128].astype(jnp.float32)
        for r in PARTS:
            if SPAN_STARTS[r] <= c < SPAN_STARTS[r] + SPAN:
                cut = slice(c - SPAN_STARTS[r], c - SPAN_STARTS[r] + 128)
                total += sums[r][place.coord[ORDERS[r][0]], :, cut]
                for step in (1, 2, 3):
                    total += got[r][place.pos(ORDERS[r][0], step), :, cut]
        y[:, c:c + 128] = total.astype(y.dtype)
    run(small + second + first, 'drain')


def solution(mesh):
    dev_axes = ('ep2', 'ep')
    bf16, f32, i32 = jnp.bfloat16, jnp.float32, jnp.int32
    group_size = mesh.shape['ep2'] * mesh.shape['ep']
    anywhere, dma = pl.BlockSpec(memory_space=pl.ANY), pltpu.SemaphoreType.DMA
    block = (RING, RING, LANES)
    vmem = lambda shapes, dtype: [pltpu.VMEM(shape, dtype) for shape in shapes]
    per_part = lambda lead: [lead + (WIDTHS[q][r],) for q, r in BOTH]
    params = lambda n: pltpu.CompilerParams(collective_id=n, has_side_effects=True, vmem_limit_bytes=60 * 2**20)

    def local_step(x, ids, gate, w_a, w_b):
        n_tok, d_model = x.shape
        n_top = ids.shape[1]
        experts = w_a.shape[0] * group_size
        capacity = 8 * ((5 * group_size * n_tok * n_top) // (32 * experts))
        small = (2, n_top, n_tok // 2)
        ids_t, gate_t = ids.T, gate.T
        shape = jax.ShapeDtypeStruct
        slot, counts = pl.pallas_call(route_kernel, out_shape=(shape(small, i32), shape((2, n_top, experts // 2), i32)), name='route')(ids_t)
        *mids, count_y = pl.pallas_call(
            send_kernel,
            in_specs=[anywhere] * 3,
            out_specs=[anywhere] * 7,
            out_shape=[shape(s, bf16) for s in per_part((RING, 2) + block)] + [shape((RING, RING) + small, i32)],
            scratch_shapes=vmem([(RING, n_tok, SPAN)] * 3, bf16) + vmem([(RING,) + small] * 4, i32)
            + vmem(per_part((RING, 2) + block), bf16) + vmem(per_part((2,) + block), bf16) + [dma((14, 9)), dma((14, 9)), dma((14, 2))],
            compiler_params=params(0),
            name='send_stage',
        )(x, slot, counts)
        chips = (RING, RING, RING) + small
        *mids, count_z, count_other = pl.pallas_call(
            expert_stage_kernel,
            in_specs=[anywhere] * 9,
            out_specs=[anywhere] * 8,
            out_shape=[shape(s, bf16) for s in per_part((RING, 2) + block)] + [shape(chips, i32)] * 2,
            scratch_shapes=vmem(per_part((2, RING) + block), bf16) + vmem(per_part((2,) + block), bf16) * 2
            + vmem([w_a.shape, w_b.shape], bf16) + [dma((14, 9)), dma((14, 9)), dma((14, 2)), dma((2,))],
            compiler_params=params(1),
            name='expert_stage',
        )(*mids, w_a, w_b, count_y)
        chips = (RING**3,) + small
        gates = pl.pallas_call(functools.partial(weight_kernel, capacity), out_shape=shape(small, f32), name='weight')(
            ids_t, slot, gate_t, count_z.reshape(chips), count_other.reshape(chips))
        return pl.pallas_call(
            return_kernel,
            in_specs=[anywhere] * 8 + [pl.BlockSpec(memory_space=pltpu.VMEM)],
            out_specs=pl.BlockSpec(memory_space=pltpu.VMEM),
            out_shape=shape(x.shape, x.dtype),
            scratch_shapes=vmem(per_part((RING, 2) + block), bf16) + vmem(per_part((2,) + block), bf16)
            + vmem([(RING,) + small] * 3, i32) + vmem([(RING,) + small] * 3, f32) + vmem([(RING, n_tok, SPAN)] * 6, f32)
            + vmem([(2, n_tok // 2, SPAN)] * 3, f32) + [dma((15, 9)), dma((15, 9)), dma((15, 2))],
            compiler_params=params(2),
            name='return_stage',
        )(*mids, slot, gates, x)

    tok_spec = P(('dp', 'ep2', 'ep'), None)
    w_spec = P(dev_axes, None, None)
    return jax.shard_map(local_step, mesh=mesh, in_specs=(tok_spec, tok_spec, tok_spec, w_spec, w_spec), out_specs=tok_spec, check_vma=False)
```

```python
import functools

import jax
import jax.numpy as jnp
from jax import lax
from jax.experimental import pallas as pl
from jax.experimental.pallas import tpu as pltpu
from jax.sharding import PartitionSpec as P

MESH = pl.DeviceIdType.MESH
LANES = 16
RING = 4
STRIDE = {'x': 1, 'y': RING, 'z': RING * RING}
ORDERS = ('xyz', 'yzx', 'zxy')
STREAMS = range(2)
PARTS = range(3)
WIDTHS = ((640, 640, 768), (768, 640, 640))
STARTS = ((0, 640, 1280), (0, 768, 1408))
SPAN = 768
SPAN_STARTS = (0, 640, 1280)
BOTH = [(q, r) for q in STREAMS for r in PARTS]


class Place:
    def __init__(self):
        self.core, self.chip = lax.axis_index('ep2'), lax.axis_index('ep')
        self.other = 1 - self.core
        self.coord = {axis: lax.rem(self.chip // stride, RING) for axis, stride in STRIDE.items()}

    def pos(self, axis, step):
        return lax.rem(self.coord[axis] + step + RING, RING)

    def at(self, axis, step):
        return self.chip + (self.pos(axis, step) - self.coord[axis]) * STRIDE[axis]

    def greet(self, both_cores):
        barrier = pltpu.get_barrier_semaphore()
        peers = [(self.other, self.chip)]
        for axis in STRIDE:
            for step in (1, -1):
                peers += [(c, self.at(axis, step)) for c in ((self.core, self.other) if both_cores else (self.core,))]
        for c, chip in peers:
            pl.semaphore_signal(barrier, inc=1, device_id=(0, c, chip), device_id_type=MESH)
        pl.semaphore_wait(barrier, len(peers))


class Lane:
    def __init__(self, place, axis, source, target, relay, send, recv, index, switch=False):
        self.place, self.axis, self.source, self.target, self.relay = place, axis, source, target, relay
        self.send, self.recv, self.index, self.switch = send, recv, index, switch
        self.sent = []

    def start(self, src, dst, s, r, core, chip):
        copy = pltpu.make_async_remote_copy(src_ref=src, dst_ref=dst, send_sem=self.send.at[self.index, s], recv_sem=self.recv.at[self.index, r], device_id=(0, core, chip), device_id_type=MESH)
        copy.start()
        self.sent.append(copy)

    def landed(self, dst, r):
        pltpu.make_async_remote_copy(src_ref=dst, dst_ref=dst, send_sem=self.send.at[self.index, 0], recv_sem=self.recv.at[self.index, r], device_id=(0, self.place.core, self.place.chip), device_id_type=MESH).wait_recv()

    def far(self):
        p = self.place
        for h, step in ((0, 1), (1, -1)):
            self.start(self.source(p.pos(self.axis, 2), h), self.relay.at[h], h, h, p.core, p.at(self.axis, step))

    def near(self):
        p = self.place
        me = p.coord[self.axis]
        for d, step in ((0, 1), (1, -1)):
            for h in (0, 1):
                k, c = (p.core, h) if self.switch else (h, p.core)
                self.start(self.source(p.pos(self.axis, step), h), self.target(me, k), 2 + 2 * d + h, 2 + 2 * d + k, c, p.at(self.axis, step))
        if self.switch:
            self.start(self.source(me, p.other), self.target(me, p.core), 8, 8, p.other, p.chip)

    def forward(self):
        p = self.place
        for h, step in ((0, 1), (1, -1)):
            self.landed(self.relay.at[h], h)
            k, c, r = (p.core, h, 6 + p.core) if self.switch else (h, p.core, 6 + h)
            self.start(self.relay.at[h], self.target(p.pos(self.axis, -step), k), 6 + h, r, c, p.at(self.axis, step))

    def arrive(self):
        p = self.place
        for d, step in ((0, -1), (1, 1)):
            for k in (0, 1):
                self.landed(self.target(p.pos(self.axis, step), k), 2 + 2 * d + k)
        for k in (0, 1):
            self.landed(self.target(p.pos(self.axis, 2), k), 6 + k)
        if self.switch:
            self.landed(self.target(p.coord[self.axis], p.other), 8)

    def own(self, local):
        p = self.place
        me = p.coord[self.axis]
        halves = [(p.core, p.core)] if self.switch else [(0, 0), (1, 1)]
        copies = [pltpu.make_async_copy(self.source(me, h), self.target(me, k), local.at[self.index, n]) for n, (h, k) in enumerate(halves)]
        for copy in copies:
            copy.start()
        return copies

    def drain(self):
        for copy in self.sent:
            copy.wait_send()


class Gather(Lane):
    def forward(self):
        p = self.place
        for h, step in ((0, 1), (1, -1)):
            part = self.target(p.pos(self.axis, -step), h)
            self.landed(part, 2 + 2 * h + h)
            self.start(part, part, 6 + h, 6 + h, p.core, p.at(self.axis, step))

    def arrive_near(self):
        p = self.place
        self.landed(self.target(p.pos(self.axis, -1), 1), 3)
        self.landed(self.target(p.pos(self.axis, 1), 0), 4)

    def arrive_far(self):
        for h in (0, 1):
            self.landed(self.target(self.place.pos(self.axis, 2), h), 6 + h)


class Reduce(Lane):
    def near(self):
        p = self.place
        for side, step in ((0, 1), (1, -1)):
            self.start(self.source(p.pos(self.axis, step), 1 - side), self.target(side, 1 - side), 2 + side, 2 + side, p.core, p.at(self.axis, step))

    def add(self):
        for h, step in ((0, 1), (1, -1)):
            self.landed(self.relay.at[h], h)
            self.relay[h] += self.source(self.place.pos(self.axis, step), h)[...]

    def forward(self):
        p = self.place
        for h, step in ((0, 1), (1, -1)):
            self.start(self.relay.at[h], self.target(h, h), 4 + h, 4 + h, p.core, p.at(self.axis, step))

    def arrive(self):
        for side in (0, 1):
            self.landed(self.target(side, 1 - side), 2 + side)
            self.landed(self.target(side, side), 4 + side)


def run(lanes, *steps):
    for step in steps:
        for lane in lanes:
            getattr(lane, step)()


def take(refs, *counts):
    refs = list(refs)
    for count in counts:
        yield refs[:count]
        del refs[:count]


def spot(axis, order, index):
    return (slice(None),) * [a for a in 'zyx' if a in order].index(axis) + (index,)


def plane_slots(shape, order, place, q, base=0):
    row = lax.broadcasted_iota(jnp.int32, shape, 0) + base
    first, second, third = [STRIDE[axis] for axis in order]
    dev = ((row >> 6) & 1) * RING**3 + (row >> 7) * second + ((row >> 4) & (RING - 1)) * third + place.coord[order[0]] * first
    return dev * (2 * LANES) + q * LANES + (row & (LANES - 1))


def route_kernel(ids_ref, slot_ref, count_ref):
    ids = ids_ref[...]
    n_top, n_tok = ids.shape
    experts = 2 * count_ref.shape[2]
    expert_of = lax.broadcasted_iota(jnp.int32, (experts, n_tok), 0)
    member = jnp.zeros((experts, n_tok), jnp.float32)
    for j in range(n_top):
        member = jnp.where(expert_of == ids[j:j + 1], 1.0, member)
    row = lax.broadcasted_iota(jnp.int32, (n_tok, n_tok), 0)
    col = lax.broadcasted_iota(jnp.int32, (n_tok, n_tok), 1)
    earlier = jnp.where(row < col, 1.0, 0.0).astype(jnp.bfloat16)
    member_lp = member.astype(jnp.bfloat16)
    before = jnp.dot(member_lp, earlier, preferred_element_type=jnp.float32)
    ones = jnp.ones((n_top, n_tok), jnp.bfloat16)
    counts = lax.dot_general(ones, member_lp, (((1,), (1,)), ((), ())), preferred_element_type=jnp.float32).astype(jnp.int32)
    half = n_tok // 2
    for h in (0, 1):
        count_ref[h] = counts[:, h * half:(h + 1) * half]
    for j in range(n_top):
        rank = jnp.sum(jnp.where(expert_of == ids[j:j + 1], before, 0.0), axis=0, keepdims=True)
        slot = ids[j:j + 1] * LANES + rank.astype(jnp.int32)
        for h in (0, 1):
            slot_ref[h, j:j + 1, :] = slot[:, h * half:(h + 1) * half]


def layer_kernel(capacity, *refs):
    (x, ids, gate, slot, count), (w_in, w_out), (y,), mids, backs, ends, b_relay, c_relay, cb_relay, bb_relay, refs = take(refs, 5, 2, 1, 6, 6, 6, 6, 6, 6, 6, None)
    tokens, slots, gates, packed, rows, sums, got, sum_relay, (count_x, count_y, count_z, count_other, mine, w_in_v, w_out_v, send, recv, local, extra) = take(refs, 3, 3, 3, 6, 6, 3, 3, 3, None)
    place = Place()
    n_tok, n_top = x.shape[0], slot.shape[1]
    half = n_tok // 2
    n_row = 2 * RING * RING * LANES
    index = iter(range(send.shape[0]))
    lane = lambda kind, axis, source, target, relay=None, switch=False: kind(place, axis, source, target, relay, send, recv, next(index), switch)
    first, second, third = [[ORDERS[r][k] for r in PARTS] for k in PARTS]

    a_small = [lane(Gather, first[r], lambda p, h: slot.at[h], lambda o, k, r=r: slots[r].at[o, k]) for r in PARTS]
    a_small.append(lane(Gather, 'x', lambda p, h: count.at[h], lambda o, k: count_x.at[o, k]))
    a_out = [lane(Gather, first[r], lambda p, h, r=r: x.at[pl.ds(h * half, half), pl.ds(SPAN_STARTS[r], SPAN)],
                  lambda o, k, r=r: tokens[r].at[o, pl.ds(k * half, half)]) for r in PARTS]
    along_y = lane(Gather, 'y', lambda p, h: count_x.at[:, h], lambda o, k: count_y.at[o, :, k])
    along_z = lane(Gather, 'z', lambda p, h: count_y.at[:, :, h], lambda o, k: count_z.at[o, :, :, k])
    swap = lane(Lane, 'z', None, None)
    a_gate = [lane(Gather, first[r], lambda p, h: mine.at[h], lambda o, k, r=r: gates[r].at[o, k]) for r in PARTS]
    b_out = [lane(Lane, second[r], lambda p, h, i=3 * q + r: packed[i].at[p, h],
                  lambda o, k, i=3 * q + r, r=r: mids[i].at[(slice(None), k) + spot(second[r], ORDERS[r][:2], o)], b_relay[3 * q + r], True) for q, r in BOTH]
    c_out = [lane(Lane, third[r], lambda p, h, i=3 * q + r: mids[i].at[p, h],
                  lambda o, k, i=3 * q + r, r=r: rows[i].at[(k,) + spot(third[r], 'zyx', o)], c_relay[3 * q + r]) for q, r in BOTH]
    c_back = [lane(Lane, third[r], lambda p, h, i=3 * q + r, r=r: rows[i].at[(h,) + spot(third[r], 'zyx', p)],
                   lambda o, k, i=3 * q + r: backs[i].at[o, k], cb_relay[3 * q + r]) for q, r in BOTH]
    b_back = [lane(Lane, second[r], lambda p, h, i=3 * q + r, r=r: backs[i].at[(slice(None), h) + spot(second[r], ORDERS[r][:2], p)],
                   lambda o, k, i=3 * q + r: ends[i].at[o, k], bb_relay[3 * q + r], True) for q, r in BOTH]
    a_back = [lane(Reduce, first[r], lambda p, h, r=r: sums[r].at[p, pl.ds(h * half, half)],
                   lambda side, h, r=r: got[r].at[side, pl.ds(h * half, half)], sum_relay[r]) for r in PARTS]
    one, two = slice(0, 3), slice(3, 6)

    def pack(q, r, step):
        a = place.pos(first[r], step)
        offset = STARTS[q][r] - SPAN_STARTS[r]
        for part in (0, 1):
            wanted = plane_slots((n_row // 2, half), ORDERS[r], place, q, part * n_row // 2)
            picks = []
            for h in (0, 1):
                pick = jnp.zeros((n_row // 2, half), jnp.float32)
                for j in range(n_top):
                    pick = jnp.where(wanted == slots[r][a, h, j:j + 1], 1.0, pick)
                picks.append(pick.astype(jnp.bfloat16))
            block = jnp.dot(jnp.concatenate(picks, axis=1), tokens[r][a, :, offset:offset + WIDTHS[q][r]], preferred_element_type=jnp.float32)
            packed[3 * q + r][2 * part:2 * part + 2, :, :, a] = block.astype(jnp.bfloat16).reshape(RING // 2, 2, RING, LANES, WIDTHS[q][r])

    def expert(q, step):
        core, z = step // RING, lax.rem(step, RING)
        total = None
        for r in PARTS:
            part = rows[3 * q + r][core, z].reshape(RING * RING * LANES, WIDTHS[q][r])
            term = jnp.dot(part, w_in_v[STARTS[q][r]:STARTS[q][r] + WIDTHS[q][r]], preferred_element_type=jnp.float32)
            total = term if total is None else total + term
        hidden = jax.nn.gelu(total, approximate=True).astype(jnp.bfloat16)
        for r in PARTS:
            res = jnp.dot(hidden, w_out_v[:, STARTS[q][r]:STARTS[q][r] + WIDTHS[q][r]], preferred_element_type=jnp.float32)
            rows[3 * q + r][core, z] = res.astype(jnp.bfloat16).reshape(RING, RING, LANES, WIDTHS[q][r])

    def weigh():
        counted = lambda ref: ref[...].reshape((RING**3,) + count.shape)
        ahead = lax.broadcasted_iota(jnp.int32, (RING**3,) + count.shape, 0) < place.chip
        off = jnp.sum(jnp.where(ahead, counted(count_z), 0), axis=0) + jnp.where(place.core == 1, jnp.sum(counted(count_other), axis=0), 0)
        off = jnp.concatenate([off[0], off[1]], axis=1)
        high, low = (off >> 7).astype(jnp.bfloat16), (off & 127).astype(jnp.bfloat16)
        expert_of = lax.broadcasted_iota(jnp.int32, (off.shape[1], n_tok), 0)
        for j in range(n_top):
            choice = jnp.where(expert_of == ids[j:j + 1], 1.0, 0.0).astype(jnp.bfloat16)
            before = 128 * jnp.dot(high, choice, preferred_element_type=jnp.float32) + jnp.dot(low, choice, preferred_element_type=jnp.float32)
            before = before[0:1].astype(jnp.int32)
            for h in (0, 1):
                cut = slice(h * half, (h + 1) * half)
                rank = before[:, cut] + slot[h, j:j + 1] - ids[j:j + 1, cut] * LANES
                mine[h, j:j + 1] = jnp.where(rank < capacity, gate[j:j + 1, cut], 0.0)

    def combine(q, r, step, h):
        a = place.pos(first[r], step)
        wanted = plane_slots((n_row, half), ORDERS[r], place, q)
        weight = jnp.zeros((n_row, half), jnp.float32)
        for j in range(n_top):
            weight = jnp.where(wanted == slots[r][a, h, j:j + 1], gates[r][a, h, j:j + 1], weight)
        high = weight.astype(jnp.bfloat16)
        rest = weight - high.astype(jnp.float32)
        mid = rest.astype(jnp.bfloat16)
        low = (rest - mid.astype(jnp.float32)).astype(jnp.bfloat16)
        weights = jnp.concatenate([high, mid, low], axis=1)
        offset = STARTS[q][r] - SPAN_STARTS[r]
        for lo, hi in ((0, 384), (384, WIDTHS[q][r])):
            back = packed[3 * q + r][:, :, :, a, :, lo:hi].reshape(n_row, hi - lo)
            mix = lax.dot_general(weights, back, (((0,), (0,)), ((), ())), preferred_element_type=jnp.float32)
            sums[r][a, pl.ds(pl.multiple_of(h * half, half), half), offset + lo:offset + hi] += mix[:half] + mix[half:2 * half] + mix[2 * half:]

    def wait(copies):
        for copy in copies:
            copy.wait()

    def own(lanes):
        return [copy for item in lanes for copy in item.own(local)]

    def load(src, dst, n):
        copy = pltpu.make_async_copy(src, dst, extra.at[n])
        copy.start()
        return copy

    def own_rows(lanes, i):
        me = [place.coord[item.axis] for item in lanes]
        return [load(item.source(me[r], place.core), packed[i + r].at[me[r], place.core], 4 + i + r) for r, item in enumerate(lanes)]

    def fetch(i):
        axis = second[i % 3]
        pieces = [(place.pos(axis, step),) for step in (1, 2, 3)] + [(place.coord[axis], place.other)]
        return [load(ends[i].at[at], packed[i].at[at], 10 + 4 * i + n) for n, at in enumerate(pieces)]

    kept = own(a_small + a_out)
    weights = [load(w_in.at[0], w_in_v, 0), load(w_out.at[0], w_out_v, 1)]
    place.greet(True)
    run(a_small, 'near')
    run(a_out, 'near')
    wait(kept)
    for r in PARTS:
        pack(0, r, 0)
    run(a_small, 'forward')
    run(a_out, 'forward')
    run(a_small, 'arrive_near', 'arrive_far')
    run(a_out, 'arrive_near')
    for r in PARTS:
        pl.loop(0, 2)(lambda n, r=r: pack(0, r, 1 + 2 * n))
    run(a_out, 'arrive_far')
    for r in PARTS:
        pack(0, r, 2)
    run(b_out[one], 'far', 'near')
    kept_y = own([along_y])
    run([along_y], 'near')
    kept_b = own(b_out[one])
    for r in PARTS:
        pl.loop(0, RING)(lambda n, r=r: pack(1, r, n))
    run(b_out[one], 'forward')
    run(b_out[two], 'far', 'near')
    kept_b += own(b_out[two])
    run([along_y], 'forward', 'arrive_near', 'arrive_far')
    wait(kept_y)
    kept_z = own([along_z])
    run([along_z], 'near')
    wait(kept_b)
    run(b_out[two], 'forward')
    run(b_out[one], 'arrive')
    run(c_out[one], 'far', 'near')
    kept = own(c_out[one])
    run([along_z], 'forward', 'arrive_near', 'arrive_far')
    wait(kept_z)
    swap.start(count_z, count_other, 0, 0, place.other, place.chip)
    run(c_out[one], 'forward')
    run(b_out[two], 'arrive')
    run(c_out[two], 'far', 'near')
    kept_two = own(c_out[two])
    run(c_out[one], 'arrive')
    wait(kept + weights)
    pl.loop(0, 2 * RING)(lambda n: expert(0, n))
    weights = [load(w_in.at[1], w_in_v, 2), load(w_out.at[1], w_out_v, 3)]
    run(c_out[two], 'forward')
    run(c_back[one], 'far', 'near')
    kept = own(c_back[one])
    run(c_out[two], 'arrive')
    wait(kept_two + weights)
    pl.loop(0, 2 * RING)(lambda n: expert(1, n))
    run(c_back[one], 'forward')
    run(c_back[two], 'far', 'near')
    kept_two = own(c_back[two])
    swap.landed(count_other, 0)
    weigh()
    wait(kept)
    run(c_back[two], 'forward')
    run(c_back[one], 'arrive')
    run(b_back[one], 'far', 'near')
    run(b_out, 'drain')
    kept = own_rows(b_back[one], 0)
    kept_gate = own(a_gate)
    run(a_gate, 'near')
    for r in PARTS:
        sums[r][...] = jnp.zeros_like(sums[r])
    run(a_gate, 'forward', 'arrive_near', 'arrive_far')
    wait(kept_gate + kept_two)
    run(b_back[one], 'forward')
    run(c_back[two], 'arrive')
    run(b_back[two], 'far', 'near')
    kept_two = own_rows(b_back[two], 3)
    run(b_back[one], 'arrive')
    wait(kept)
    loads = [fetch(r) for r in PARTS]
    for r in PARTS:
        wait(loads[r])
        pl.loop(0, 2 * RING)(lambda n, r=r: combine(0, r, n // 2, lax.rem(n, 2)))
    run(b_back[two], 'forward', 'arrive')
    wait(kept_two)
    loads = [fetch(3 + r) for r in PARTS]
    for r in PARTS:
        wait(loads[r])
        pl.loop(0, 2)(lambda h, r=r: combine(1, r, 2, h))
    run(a_back, 'far')
    for r in PARTS:
        pl.loop(0, 4)(lambda n, r=r: combine(1, r, 1 + 2 * (n // 2), lax.rem(n, 2)))
    run(a_back, 'near', 'add')
    run(a_back, 'forward')
    for r in PARTS:
        pl.loop(0, 2)(lambda h, r=r: combine(1, r, 0, h))
    run(a_back, 'arrive')
    for c in range(0, x.shape[1], 128):
        total = x[:, c:c + 128].astype(jnp.float32)
        for r in PARTS:
            if SPAN_STARTS[r] <= c < SPAN_STARTS[r] + SPAN:
                cut = slice(c - SPAN_STARTS[r], c - SPAN_STARTS[r] + 128)
                total += sums[r][place.coord[first[r]], :, cut] + got[r][0, :, cut] + got[r][1, :, cut]
        y[:, c:c + 128] = total.astype(y.dtype)
    run(a_small + a_out + [along_y, along_z, swap] + a_gate + c_out + c_back + b_back + a_back, 'drain')


def solution(mesh):
    dev_axes = ('ep2', 'ep')
    bf16, f32, i32 = jnp.bfloat16, jnp.float32, jnp.int32
    group_size = mesh.shape['ep2'] * mesh.shape['ep']
    anywhere, near, dma = pl.BlockSpec(memory_space=pl.ANY), pl.BlockSpec(memory_space=pltpu.VMEM), pltpu.SemaphoreType.DMA
    vmem = lambda shapes, dtype: [pltpu.VMEM(shape, dtype) for shape in shapes]
    per_part = lambda *lead: [lead + (RING, RING, LANES, WIDTHS[q][r]) for q, r in BOTH]

    def local_step(x, ids, gate, w_a, w_b):
        n_tok, d_model = x.shape
        n_top = ids.shape[1]
        experts = w_a.shape[0] * group_size
        capacity = 8 * ((5 * group_size * n_tok * n_top) // (32 * experts))
        small = (2, n_top, n_tok // 2)
        ids_t, gate_t = ids.T, gate.T
        shape = jax.ShapeDtypeStruct
        slot, counts = pl.pallas_call(route_kernel, out_shape=(shape(small, i32), shape((2, n_top, experts // 2), i32)), name='route')(ids_t)
        between = per_part(RING, 2) * 3 + per_part(2) * 4
        lanes = 4 + 3 + 2 + 1 + 3 + 4 * 6 + 3
        return pl.pallas_call(
            functools.partial(layer_kernel, capacity),
            in_specs=[near] * 5 + [anywhere] * 2,
            out_specs=[near] + [anywhere] * len(between),
            out_shape=[shape(x.shape, x.dtype)] + [shape(s, bf16) for s in between],
            scratch_shapes=vmem([(RING, n_tok, SPAN)] * 3, bf16) + vmem([(RING,) + small] * 3, i32) + vmem([(RING,) + small] * 3, f32)
            + vmem(per_part(RING, 2), bf16) + vmem(per_part(2, RING), bf16) + vmem([(RING, n_tok, SPAN)] * 3, f32)
            + vmem([(2, n_tok, SPAN)] * 3, f32) + vmem([(2, n_tok // 2, SPAN)] * 3, f32)
            + vmem([(RING,) + small, (RING, RING) + small] + [(RING, RING, RING) + small] * 2, i32) + vmem([small], f32)
            + vmem([w_a.shape[1:], w_b.shape[1:]], bf16) + [dma((lanes, 9)), dma((lanes, 9)), dma((lanes, 2)), dma((34,))],
            compiler_params=pltpu.CompilerParams(collective_id=0, has_side_effects=True, vmem_limit_bytes=67043328),
            name='layer',
        )(x, ids_t, gate_t, slot, counts, w_a, w_b)[0]

    tok_spec = P(('dp', 'ep2', 'ep'), None)
    w_spec = P(dev_axes, None, None)
    return jax.shard_map(local_step, mesh=mesh, in_specs=(tok_spec, tok_spec, tok_spec, w_spec, w_spec), out_specs=tok_spec, check_vma=False)
```

```python
import functools

import jax
import jax.numpy as jnp
from jax import lax
from jax.experimental import pallas as pl
from jax.experimental.pallas import tpu as pltpu
from jax.sharding import PartitionSpec as P

MESH = pl.DeviceIdType.MESH
LANES = 16
RING = 4
STRIDE = {'x': 1, 'y': RING, 'z': RING * RING}
ORDERS = ('xyz', 'yzx', 'zxy')
STREAMS = range(2)
PARTS = range(3)
WIDTHS = ((640, 640, 768), (768, 640, 640))
STARTS = ((0, 640, 1280), (0, 768, 1408))
SPAN = 768
SPAN_STARTS = (0, 640, 1280)
BOTH = [(q, r) for q in STREAMS for r in PARTS]


class Place:
    def __init__(self):
        self.core, self.chip = lax.axis_index('ep2'), lax.axis_index('ep')
        self.other = 1 - self.core
        self.coord = {axis: lax.rem(self.chip // stride, RING) for axis, stride in STRIDE.items()}

    def pos(self, axis, step):
        return lax.rem(self.coord[axis] + step + RING, RING)

    def at(self, axis, step):
        return self.chip + (self.pos(axis, step) - self.coord[axis]) * STRIDE[axis]

    def greet(self, both_cores):
        barrier = pltpu.get_barrier_semaphore()
        peers = [(self.other, self.chip)]
        for axis in STRIDE:
            for step in (1, -1):
                peers += [(c, self.at(axis, step)) for c in ((self.core, self.other) if both_cores else (self.core,))]
        for c, chip in peers:
            pl.semaphore_signal(barrier, inc=1, device_id=(0, c, chip), device_id_type=MESH)
        pl.semaphore_wait(barrier, len(peers))


class Lane:
    def __init__(self, place, axis, source, target, relay, send, recv, index, switch=False):
        self.place, self.axis, self.source, self.target, self.relay = place, axis, source, target, relay
        self.send, self.recv, self.index, self.switch = send, recv, index, switch
        self.sent = []

    def start(self, src, dst, s, r, core, chip):
        copy = pltpu.make_async_remote_copy(src_ref=src, dst_ref=dst, send_sem=self.send.at[self.index, s], recv_sem=self.recv.at[self.index, r], device_id=(0, core, chip), device_id_type=MESH)
        copy.start()
        self.sent.append(copy)

    def landed(self, dst, r):
        pltpu.make_async_remote_copy(src_ref=dst, dst_ref=dst, send_sem=self.send.at[self.index, 0], recv_sem=self.recv.at[self.index, r], device_id=(0, self.place.core, self.place.chip), device_id_type=MESH).wait_recv()

    def far(self):
        p = self.place
        for h, step in ((0, 1), (1, -1)):
            self.start(self.source(p.pos(self.axis, 2), h), self.relay.at[h], h, h, p.core, p.at(self.axis, step))

    def near(self):
        p = self.place
        me = p.coord[self.axis]
        for d, step in ((0, 1), (1, -1)):
            for h in (0, 1):
                k, c = (p.core, h) if self.switch else (h, p.core)
                self.start(self.source(p.pos(self.axis, step), h), self.target(me, k), 2 + 2 * d + h, 2 + 2 * d + k, c, p.at(self.axis, step))
        if self.switch:
            self.start(self.source(me, p.other), self.target(me, p.core), 8, 8, p.other, p.chip)

    def forward(self):
        p = self.place
        for h, step in ((0, 1), (1, -1)):
            self.landed(self.relay.at[h], h)
            k, c, r = (p.core, h, 6 + p.core) if self.switch else (h, p.core, 6 + h)
            self.start(self.relay.at[h], self.target(p.pos(self.axis, -step), k), 6 + h, r, c, p.at(self.axis, step))

    def arrive_near(self):
        p = self.place
        for d, step in ((0, -1), (1, 1)):
            for k in (0, 1):
                self.landed(self.target(p.pos(self.axis, step), k), 2 + 2 * d + k)
        if self.switch:
            self.landed(self.target(p.coord[self.axis], p.other), 8)

    def arrive_far(self):
        for k in (0, 1):
            self.landed(self.target(self.place.pos(self.axis, 2), k), 6 + k)

    def arrive(self):
        self.arrive_near()
        self.arrive_far()

    def own(self, local):
        p = self.place
        me = p.coord[self.axis]
        halves = [(p.core, p.core)] if self.switch else [(0, 0), (1, 1)]
        copies = [pltpu.make_async_copy(self.source(me, h), self.target(me, k), local.at[self.index, n]) for n, (h, k) in enumerate(halves)]
        for copy in copies:
            copy.start()
        return copies

    def drain(self):
        for copy in self.sent:
            copy.wait_send()


class Gather(Lane):
    def forward(self):
        p = self.place
        for h, step in ((0, 1), (1, -1)):
            part = self.target(p.pos(self.axis, -step), h)
            self.landed(part, 2 + 2 * h + h)
            self.start(part, part, 6 + h, 6 + h, p.core, p.at(self.axis, step))

    def arrive_near(self):
        p = self.place
        self.landed(self.target(p.pos(self.axis, -1), 1), 3)
        self.landed(self.target(p.pos(self.axis, 1), 0), 4)

    def arrive_far(self):
        for h in (0, 1):
            self.landed(self.target(self.place.pos(self.axis, 2), h), 6 + h)


class Reduce(Lane):
    def near(self):
        p = self.place
        for side, step in ((0, 1), (1, -1)):
            self.start(self.source(p.pos(self.axis, step), 1 - side), self.target(side, 1 - side), 2 + side, 2 + side, p.core, p.at(self.axis, step))

    def add(self):
        for h, step in ((0, 1), (1, -1)):
            self.landed(self.relay.at[h], h)
            self.relay[h] += self.source(self.place.pos(self.axis, step), h)[...]

    def forward(self):
        p = self.place
        for h, step in ((0, 1), (1, -1)):
            self.start(self.relay.at[h], self.target(h, h), 4 + h, 4 + h, p.core, p.at(self.axis, step))

    def arrive(self):
        for side in (0, 1):
            self.landed(self.target(side, 1 - side), 2 + side)
            self.landed(self.target(side, side), 4 + side)


def run(lanes, *steps):
    for step in steps:
        for lane in lanes:
            getattr(lane, step)()


def take(refs, *counts):
    refs = list(refs)
    for count in counts:
        yield refs[:count]
        del refs[:count]


def spot(axis, order, index):
    return (slice(None),) * [a for a in 'zyx' if a in order].index(axis) + (index,)


def plane_slots(shape, order, place, q, base=0):
    row = lax.broadcasted_iota(jnp.int32, shape, 0) + base
    first, second, third = [STRIDE[axis] for axis in order]
    dev = ((row >> 6) & 1) * RING**3 + (row >> 7) * second + ((row >> 4) & (RING - 1)) * third + place.coord[order[0]] * first
    return dev * (2 * LANES) + q * LANES + (row & (LANES - 1))


def route(ids_ref, slot_ref, count_ref):
    ids = ids_ref[...]
    n_top, n_tok = ids.shape
    experts = 2 * count_ref.shape[2]
    expert_of = lax.broadcasted_iota(jnp.int32, (experts, n_tok), 0)
    member = jnp.zeros((experts, n_tok), jnp.float32)
    for j in range(n_top):
        member = jnp.where(expert_of == ids[j:j + 1], 1.0, member)
    row = lax.broadcasted_iota(jnp.int32, (n_tok, n_tok), 0)
    col = lax.broadcasted_iota(jnp.int32, (n_tok, n_tok), 1)
    earlier = jnp.where(row < col, 1.0, 0.0).astype(jnp.bfloat16)
    member_lp = member.astype(jnp.bfloat16)
    before = jnp.dot(member_lp, earlier, preferred_element_type=jnp.float32)
    ones = jnp.ones((n_top, n_tok), jnp.bfloat16)
    counts = lax.dot_general(ones, member_lp, (((1,), (1,)), ((), ())), preferred_element_type=jnp.float32).astype(jnp.int32)
    half = n_tok // 2
    for h in (0, 1):
        count_ref[h] = counts[:, h * half:(h + 1) * half]
    for j in range(n_top):
        rank = jnp.sum(jnp.where(expert_of == ids[j:j + 1], before, 0.0), axis=0, keepdims=True)
        slot = ids[j:j + 1] * LANES + rank.astype(jnp.int32)
        for h in (0, 1):
            slot_ref[h, j:j + 1, :] = slot[:, h * half:(h + 1) * half]


def layer_kernel(capacity, *refs):
    (x, ids, gate), (w_in, w_out), (y,), mids, backs, ends, b_relay, c_relay, cb_relay, bb_relay, refs = take(refs, 3, 2, 1, 6, 6, 6, 6, 6, 6, 6, None)
    tokens, slots, gates, packed, rows, sums, got, sum_relay, (slot, count, count_x, count_y, count_z, count_other, mine, w_in_v, w_out_v, send, recv, local, extra) = take(refs, 3, 3, 3, 6, 6, 3, 3, 3, None)
    place = Place()
    n_tok, n_top = x.shape[0], slot.shape[1]
    half = n_tok // 2
    n_row = 2 * RING * RING * LANES
    index = iter(range(send.shape[0]))
    lane = lambda kind, axis, source, target, relay=None, switch=False: kind(place, axis, source, target, relay, send, recv, next(index), switch)
    first, second, third = [[ORDERS[r][k] for r in PARTS] for k in PARTS]

    a_small = [lane(Gather, first[r], lambda p, h: slot.at[h], lambda o, k, r=r: slots[r].at[o, k]) for r in PARTS]
    a_small.append(lane(Gather, 'x', lambda p, h: count.at[h], lambda o, k: count_x.at[o, k]))
    a_out = [lane(Gather, first[r], lambda p, h, r=r: x.at[pl.ds(h * half, half), pl.ds(SPAN_STARTS[r], SPAN)],
                  lambda o, k, r=r: tokens[r].at[o, pl.ds(k * half, half)]) for r in PARTS]
    along_y = lane(Gather, 'y', lambda p, h: count_x.at[:, h], lambda o, k: count_y.at[o, :, k])
    along_z = lane(Gather, 'z', lambda p, h: count_y.at[:, :, h], lambda o, k: count_z.at[o, :, :, k])
    swap = lane(Lane, 'z', None, None)
    a_gate = [lane(Gather, first[r], lambda p, h: mine.at[h], lambda o, k, r=r: gates[r].at[o, k]) for r in PARTS]
    b_out = [lane(Lane, second[r], lambda p, h, i=3 * q + r: packed[i].at[p, h],
                  lambda o, k, i=3 * q + r, r=r: mids[i].at[(slice(None), k) + spot(second[r], ORDERS[r][:2], o)], b_relay[3 * q + r], True) for q, r in BOTH]
    c_out = [lane(Lane, third[r], lambda p, h, i=3 * q + r: mids[i].at[p, h],
                  lambda o, k, i=3 * q + r, r=r: rows[i].at[(k,) + spot(third[r], 'zyx', o)], c_relay[3 * q + r]) for q, r in BOTH]
    c_back = [lane(Lane, third[r], lambda p, h, i=3 * q + r, r=r: rows[i].at[(h,) + spot(third[r], 'zyx', p)],
                   lambda o, k, i=3 * q + r: backs[i].at[o, k], cb_relay[3 * q + r]) for q, r in BOTH]
    b_back = [lane(Lane, second[r], lambda p, h, i=3 * q + r, r=r: backs[i].at[(slice(None), h) + spot(second[r], ORDERS[r][:2], p)],
                   lambda o, k, i=3 * q + r: ends[i].at[o, k], bb_relay[3 * q + r], True) for q, r in BOTH]
    a_back = [lane(Reduce, first[r], lambda p, h, r=r: sums[r].at[p, pl.ds(h * half, half)],
                   lambda side, h, r=r: got[r].at[side, pl.ds(h * half, half)], sum_relay[r]) for r in PARTS]
    one, two = slice(0, 3), slice(3, 6)

    def pack(q, r, step):
        a = place.pos(first[r], step)
        offset = STARTS[q][r] - SPAN_STARTS[r]
        for part in (0, 1):
            wanted = plane_slots((n_row // 2, half), ORDERS[r], place, q, part * n_row // 2)
            picks = []
            for h in (0, 1):
                pick = jnp.zeros((n_row // 2, half), jnp.float32)
                for j in range(n_top):
                    pick = jnp.where(wanted == slots[r][a, h, j:j + 1], 1.0, pick)
                picks.append(pick.astype(jnp.bfloat16))
            block = jnp.dot(jnp.concatenate(picks, axis=1), tokens[r][a, :, offset:offset + WIDTHS[q][r]], preferred_element_type=jnp.float32)
            packed[3 * q + r][2 * part:2 * part + 2, :, :, a] = block.astype(jnp.bfloat16).reshape(RING // 2, 2, RING, LANES, WIDTHS[q][r])

    def expert(q, step):
        core, z = step // RING, lax.rem(step, RING)
        total = None
        for r in PARTS:
            part = rows[3 * q + r][core, z].reshape(RING * RING * LANES, WIDTHS[q][r])
            term = jnp.dot(part, w_in_v[STARTS[q][r]:STARTS[q][r] + WIDTHS[q][r]], preferred_element_type=jnp.float32)
            total = term if total is None else total + term
        hidden = jax.nn.gelu(total, approximate=True).astype(jnp.bfloat16)
        for r in PARTS:
            res = jnp.dot(hidden, w_out_v[:, STARTS[q][r]:STARTS[q][r] + WIDTHS[q][r]], preferred_element_type=jnp.float32)
            rows[3 * q + r][core, z] = res.astype(jnp.bfloat16).reshape(RING, RING, LANES, WIDTHS[q][r])

    def weigh():
        counted = lambda ref: ref[...].reshape((RING**3,) + slot.shape)
        ahead = lax.broadcasted_iota(jnp.int32, (RING**3,) + slot.shape, 0) < place.chip
        off = jnp.sum(jnp.where(ahead, counted(count_z), 0), axis=0) + jnp.where(place.core == 1, jnp.sum(counted(count_other), axis=0), 0)
        off = jnp.concatenate([off[0], off[1]], axis=1)
        high, low = (off >> 7).astype(jnp.bfloat16), (off & 127).astype(jnp.bfloat16)
        expert_of = lax.broadcasted_iota(jnp.int32, (off.shape[1], n_tok), 0)
        for j in range(n_top):
            choice = jnp.where(expert_of == ids[j:j + 1], 1.0, 0.0).astype(jnp.bfloat16)
            before = 128 * jnp.dot(high, choice, preferred_element_type=jnp.float32) + jnp.dot(low, choice, preferred_element_type=jnp.float32)
            before = before[0:1].astype(jnp.int32)
            for h in (0, 1):
                cut = slice(h * half, (h + 1) * half)
                rank = before[:, cut] + slot[h, j:j + 1] - ids[j:j + 1, cut] * LANES
                mine[h, j:j + 1] = jnp.where(rank < capacity, gate[j:j + 1, cut], 0.0)

    def combine(q, r, step, h, b=None):
        a = place.pos(first[r], step)
        lead, n = (slice(None), n_row) if b is None else (pl.ds(b, 1), n_row // RING)
        wanted = plane_slots((n, half), ORDERS[r], place, q, 0 if b is None else b * n)
        weight = jnp.zeros((n, half), jnp.float32)
        for j in range(n_top):
            weight = jnp.where(wanted == slots[r][a, h, j:j + 1], gates[r][a, h, j:j + 1], weight)
        high = weight.astype(jnp.bfloat16)
        rest = weight - high.astype(jnp.float32)
        mid = rest.astype(jnp.bfloat16)
        low = (rest - mid.astype(jnp.float32)).astype(jnp.bfloat16)
        weights = jnp.concatenate([high, mid, low], axis=1)
        offset = STARTS[q][r] - SPAN_STARTS[r]
        for lo, hi in ((0, 384), (384, WIDTHS[q][r])):
            back = packed[3 * q + r][lead, :, :, a, :, lo:hi].reshape(n, hi - lo)
            mix = lax.dot_general(weights, back, (((0,), (0,)), ((), ())), preferred_element_type=jnp.float32)
            sums[r][a, pl.ds(pl.multiple_of(h * half, half), half), offset + lo:offset + hi] += mix[:half] + mix[half:2 * half] + mix[2 * half:]

    def wait(copies):
        for copy in copies:
            copy.wait()

    def own(lanes):
        return [copy for item in lanes for copy in item.own(local)]

    def load(src, dst, n):
        copy = pltpu.make_async_copy(src, dst, extra.at[n])
        copy.start()
        return copy

    def own_rows(lanes, i):
        me = [place.coord[item.axis] for item in lanes]
        return [load(item.source(me[r], place.core), packed[i + r].at[me[r], place.core], 4 + i + r) for r, item in enumerate(lanes)]

    def fetch(i, near):
        axis = second[i % 3]
        pieces = [(place.pos(axis, step),) for step in ((1, 3) if near else (2,))]
        if near:
            pieces.append((place.coord[axis], place.other))
        return [load(ends[i].at[at], packed[i].at[at], 10 + 4 * i + n + (0 if near else 3)) for n, at in enumerate(pieces)]

    kept = own(a_out)
    weights = [load(w_in.at[0], w_in_v, 0), load(w_out.at[0], w_out_v, 1)]
    place.greet(True)
    run(a_out, 'near')
    route(ids, slot, count)
    kept += own(a_small)
    run(a_small, 'near')
    wait(kept)
    for r in PARTS:
        pack(0, r, 0)
    run(a_out, 'forward')
    run(a_small, 'forward', 'arrive_near')
    run(a_out, 'arrive_near')
    for r in PARTS:
        pl.loop(0, 2)(lambda n, r=r: pack(0, r, 1 + 2 * n))
    run(a_small, 'arrive_far')
    run(a_out, 'arrive_far')
    for r in PARTS:
        pack(0, r, 2)
    run(b_out[one], 'far', 'near')
    kept_y = own([along_y])
    run([along_y], 'near')
    kept_b = own(b_out[one])
    for r in PARTS:
        pl.loop(0, RING)(lambda n, r=r: pack(1, r, n))
    run(b_out[one], 'forward')
    run(b_out[two], 'far', 'near')
    kept_b += own(b_out[two])
    run([along_y], 'forward')
    run(b_out[two], 'forward')
    wait(kept_b)
    run(b_out[one], 'arrive')
    run(c_out[one], 'far', 'near')
    kept = own(c_out[one])
    run([along_y], 'arrive_near', 'arrive_far')
    wait(kept_y)
    kept_z = own([along_z])
    run([along_z], 'near')
    run(c_out[one], 'forward')
    run(b_out[two], 'arrive')
    run(c_out[two], 'far', 'near')
    kept_two = own(c_out[two])
    run(c_out[one], 'arrive')
    wait(kept + weights)
    pl.loop(0, 2 * RING)(lambda n: expert(0, n))
    weights = [load(w_in.at[1], w_in_v, 2), load(w_out.at[1], w_out_v, 3)]
    run(c_out[two], 'forward')
    run(c_back[one], 'far', 'near')
    kept = own(c_back[one])
    run([along_z], 'forward')
    run(c_out[two], 'arrive')
    wait(kept_two + weights)
    pl.loop(0, 2 * RING)(lambda n: expert(1, n))
    run(c_back[one], 'forward')
    run(c_back[two], 'far', 'near')
    kept_two = own(c_back[two])
    run([along_z], 'arrive_near', 'arrive_far')
    wait(kept_z)
    swap.start(count_z, count_other, 0, 0, place.other, place.chip)
    swap.landed(count_other, 0)
    weigh()
    kept_gate = own(a_gate)
    run(a_gate, 'near')
    run(c_back[two], 'forward')
    run(c_back[one], 'arrive')
    wait(kept)
    run(b_back[one], 'far', 'near')
    run(b_out, 'drain')
    kept = own_rows(b_back[one], 0)
    for r in PARTS:
        sums[r][...] = jnp.zeros_like(sums[r])
    run(a_gate, 'forward')
    run(b_back[one], 'forward')
    run(c_back[two], 'arrive')
    wait(kept_two)
    run(b_back[two], 'far', 'near')
    kept_two = own_rows(b_back[two], 3)
    run(b_back[one], 'arrive')
    wait(kept)
    loads = [fetch(r, True) + fetch(r, False) for r in PARTS]
    run(a_gate, 'arrive_near', 'arrive_far')
    wait(kept_gate)
    for r in PARTS:
        wait(loads[r])
        pl.loop(0, 2 * RING)(lambda n, r=r: combine(0, r, n // 2, lax.rem(n, 2)))
    run(b_back[two], 'forward', 'arrive_near')
    loads = [fetch(3 + r, True) for r in PARTS]
    wait(kept_two)
    for r in PARTS:
        wait(loads[r])
        pl.loop(0, 6 * RING)(lambda n, r=r: combine(1, r, n // 6, lax.rem(n, 2), place.pos(second[r], 3 + lax.rem(n, 6) // 2)))
    run(b_back[two], 'arrive_far')
    loads = [fetch(3 + r, False) for r in PARTS]
    for r in PARTS:
        wait(loads[r])
        pl.loop(0, 2)(lambda h, r=r: combine(1, r, 2, h, place.pos(second[r], 2)))
    run(a_back, 'far')
    for r in PARTS:
        pl.loop(0, 4)(lambda n, r=r: combine(1, r, 1 + 2 * (n // 2), lax.rem(n, 2), place.pos(second[r], 2)))
    run(a_back, 'near', 'add')
    run(a_back, 'forward')
    for r in PARTS:
        pl.loop(0, 2)(lambda h, r=r: combine(1, r, 0, h, place.pos(second[r], 2)))
        sums[r][place.coord[first[r]], :, :SPAN_STARTS[1]] += x[:, SPAN_STARTS[r]:SPAN_STARTS[r] + SPAN_STARTS[1]].astype(jnp.float32)
    sums[2][place.coord[first[2]], :, SPAN_STARTS[1]:] += x[:, SPAN_STARTS[2] + SPAN_STARTS[1]:].astype(jnp.float32)
    run(a_back, 'arrive')
    for c in range(0, x.shape[1], 128):
        total = None
        for r in PARTS:
            if SPAN_STARTS[r] <= c < SPAN_STARTS[r] + SPAN:
                cut = slice(c - SPAN_STARTS[r], c - SPAN_STARTS[r] + 128)
                part = sums[r][place.coord[first[r]], :, cut] + got[r][0, :, cut] + got[r][1, :, cut]
                total = part if total is None else total + part
        y[:, c:c + 128] = total.astype(y.dtype)
    run(a_small + a_out + [along_y, along_z, swap] + a_gate + c_out + c_back + b_back + a_back, 'drain')


def solution(mesh):
    dev_axes = ('ep2', 'ep')
    bf16, f32, i32 = jnp.bfloat16, jnp.float32, jnp.int32
    group_size = mesh.shape['ep2'] * mesh.shape['ep']
    anywhere, near, dma = pl.BlockSpec(memory_space=pl.ANY), pl.BlockSpec(memory_space=pltpu.VMEM), pltpu.SemaphoreType.DMA
    vmem = lambda shapes, dtype: [pltpu.VMEM(shape, dtype) for shape in shapes]
    per_part = lambda *lead: [lead + (RING, RING, LANES, WIDTHS[q][r]) for q, r in BOTH]

    def local_step(x, ids, gate, w_a, w_b):
        n_tok, d_model = x.shape
        n_top = ids.shape[1]
        experts = w_a.shape[0] * group_size
        capacity = 8 * ((5 * group_size * n_tok * n_top) // (32 * experts))
        small = (2, n_top, n_tok // 2)
        ids_t, gate_t = ids.T, gate.T
        shape = jax.ShapeDtypeStruct
        between = per_part(RING, 2) * 3 + per_part(2) * 4
        lanes = 4 + 3 + 2 + 1 + 3 + 4 * 6 + 3
        return pl.pallas_call(
            functools.partial(layer_kernel, capacity),
            in_specs=[near] * 3 + [anywhere] * 2,
            out_specs=[near] + [anywhere] * len(between),
            out_shape=[shape(x.shape, x.dtype)] + [shape(s, bf16) for s in between],
            scratch_shapes=vmem([(RING, n_tok, SPAN)] * 3, bf16) + vmem([(RING,) + small] * 3, i32) + vmem([(RING,) + small] * 3, f32)
            + vmem(per_part(RING, 2), bf16) + vmem(per_part(2, RING), bf16) + vmem([(RING, n_tok, SPAN)] * 3, f32)
            + vmem([(2, n_tok, SPAN)] * 3, f32) + vmem([(2, n_tok // 2, SPAN)] * 3, f32)
            + vmem([small, (2, n_top, experts // 2), (RING,) + small, (RING, RING) + small] + [(RING, RING, RING) + small] * 2, i32) + vmem([small], f32)
            + vmem([w_a.shape[1:], w_b.shape[1:]], bf16) + [dma((lanes, 9)), dma((lanes, 9)), dma((lanes, 2)), dma((34,))],
            compiler_params=pltpu.CompilerParams(collective_id=0, has_side_effects=True, vmem_limit_bytes=67043328),
            name='layer',
        )(x, ids_t, gate_t, w_a, w_b)[0]

    tok_spec = P(('dp', 'ep2', 'ep'), None)
    w_spec = P(dev_axes, None, None)
    return jax.shard_map(local_step, mesh=mesh, in_specs=(tok_spec, tok_spec, tok_spec, w_spec, w_spec), out_specs=tok_spec, check_vma=False)
```

```python
import functools

import jax
import jax.numpy as jnp
from jax import lax
from jax.experimental import pallas as pl
from jax.experimental.pallas import tpu as pltpu
from jax.sharding import PartitionSpec as P

MESH = pl.DeviceIdType.MESH
LANES = 16
RING = 4
STRIDE = {'x': 1, 'y': RING, 'z': RING * RING}
ORDERS = ('xyz', 'yzx', 'zxy')
STREAMS = range(2)
PARTS = range(3)
WIDTHS = ((640, 640, 768), (768, 640, 640))
STARTS = ((0, 640, 1280), (0, 768, 1408))
SPAN = 768
SPAN_STARTS = (0, 640, 1280)
BOTH = [(q, r) for q in STREAMS for r in PARTS]


class Place:
    def __init__(self):
        self.core, self.chip = lax.axis_index('ep2'), lax.axis_index('ep')
        self.other = 1 - self.core
        self.coord = {axis: lax.rem(self.chip // stride, RING) for axis, stride in STRIDE.items()}

    def pos(self, axis, step):
        return lax.rem(self.coord[axis] + step + RING, RING)

    def at(self, axis, step):
        return self.chip + (self.pos(axis, step) - self.coord[axis]) * STRIDE[axis]

    def greet(self, both_cores):
        barrier = pltpu.get_barrier_semaphore()
        peers = [(self.other, self.chip)]
        for axis in STRIDE:
            for step in (1, -1):
                peers += [(c, self.at(axis, step)) for c in ((self.core, self.other) if both_cores else (self.core,))]
        for c, chip in peers:
            pl.semaphore_signal(barrier, inc=1, device_id=(0, c, chip), device_id_type=MESH)
        pl.semaphore_wait(barrier, len(peers))


class Lane:
    def __init__(self, place, axis, source, target, relay, send, recv, index, switch=False):
        self.place, self.axis, self.source, self.target, self.relay = place, axis, source, target, relay
        self.send, self.recv, self.index, self.switch = send, recv, index, switch
        self.sent = []

    def start(self, src, dst, s, r, core, chip):
        copy = pltpu.make_async_remote_copy(src_ref=src, dst_ref=dst, send_sem=self.send.at[self.index, s], recv_sem=self.recv.at[self.index, r], device_id=(0, core, chip), device_id_type=MESH)
        copy.start()
        self.sent.append(copy)

    def landed(self, dst, r):
        pltpu.make_async_remote_copy(src_ref=dst, dst_ref=dst, send_sem=self.send.at[self.index, 0], recv_sem=self.recv.at[self.index, r], device_id=(0, self.place.core, self.place.chip), device_id_type=MESH).wait_recv()

    def far(self):
        p = self.place
        for h, step in ((0, 1), (1, -1)):
            self.start(self.source(p.pos(self.axis, 2), h), self.relay.at[h], h, h, p.core, p.at(self.axis, step))

    def near(self):
        p = self.place
        me = p.coord[self.axis]
        for d, step in ((0, 1), (1, -1)):
            for h in (0, 1):
                k, c = (p.core, h) if self.switch else (h, p.core)
                self.start(self.source(p.pos(self.axis, step), h), self.target(me, k), 2 + 2 * d + h, 2 + 2 * d + k, c, p.at(self.axis, step))
        if self.switch:
            self.start(self.source(me, p.other), self.target(me, p.core), 8, 8, p.other, p.chip)

    def forward(self):
        p = self.place
        for h, step in ((0, 1), (1, -1)):
            self.landed(self.relay.at[h], h)
            k, c, r = (p.core, h, 6 + p.core) if self.switch else (h, p.core, 6 + h)
            self.start(self.relay.at[h], self.target(p.pos(self.axis, -step), k), 6 + h, r, c, p.at(self.axis, step))

    def arrive_near(self):
        p = self.place
        for d, step in ((0, -1), (1, 1)):
            for k in (0, 1):
                self.landed(self.target(p.pos(self.axis, step), k), 2 + 2 * d + k)
        if self.switch:
            self.landed(self.target(p.coord[self.axis], p.other), 8)

    def arrive_far(self):
        for k in (0, 1):
            self.landed(self.target(self.place.pos(self.axis, 2), k), 6 + k)

    def arrive(self):
        self.arrive_near()
        self.arrive_far()

    def own(self, local):
        p = self.place
        me = p.coord[self.axis]
        halves = [(p.core, p.core)] if self.switch else [(0, 0), (1, 1)]
        copies = [pltpu.make_async_copy(self.source(me, h), self.target(me, k), local.at[self.index, n]) for n, (h, k) in enumerate(halves)]
        for copy in copies:
            copy.start()
        return copies

    def drain(self):
        for copy in self.sent:
            copy.wait_send()


class Gather(Lane):
    def forward(self):
        p = self.place
        for h, step in ((0, 1), (1, -1)):
            part = self.target(p.pos(self.axis, -step), h)
            self.landed(part, 2 + 2 * h + h)
            self.start(part, part, 6 + h, 6 + h, p.core, p.at(self.axis, step))

    def arrive_near(self):
        p = self.place
        self.landed(self.target(p.pos(self.axis, -1), 1), 3)
        self.landed(self.target(p.pos(self.axis, 1), 0), 4)

    def arrive_far(self):
        for h in (0, 1):
            self.landed(self.target(self.place.pos(self.axis, 2), h), 6 + h)


class Reduce(Lane):
    def near(self):
        p = self.place
        for side, step in ((0, 1), (1, -1)):
            self.start(self.source(p.pos(self.axis, step), 1 - side), self.target(side, 1 - side), 2 + side, 2 + side, p.core, p.at(self.axis, step))

    def add(self):
        for h, step in ((0, 1), (1, -1)):
            self.landed(self.relay.at[h], h)
            self.relay[h] += self.source(self.place.pos(self.axis, step), h)[...]

    def forward(self):
        p = self.place
        for h, step in ((0, 1), (1, -1)):
            self.start(self.relay.at[h], self.target(h, h), 4 + h, 4 + h, p.core, p.at(self.axis, step))

    def arrive(self):
        for side in (0, 1):
            self.landed(self.target(side, 1 - side), 2 + side)
            self.landed(self.target(side, side), 4 + side)


def run(lanes, *steps):
    for step in steps:
        for lane in lanes:
            getattr(lane, step)()


def take(refs, *counts):
    refs = list(refs)
    for count in counts:
        yield refs[:count]
        del refs[:count]


def spot(axis, order, index):
    return (slice(None),) * [a for a in 'zyx' if a in order].index(axis) + (index,)


def plane_slots(shape, order, place, q, base=0):
    row = lax.broadcasted_iota(jnp.int32, shape, 0) + base
    first, second, third = [STRIDE[axis] for axis in order]
    dev = ((row >> 6) & 1) * RING**3 + (row >> 7) * second + ((row >> 4) & (RING - 1)) * third + place.coord[order[0]] * first
    return dev * (2 * LANES) + q * LANES + (row & (LANES - 1))


def route(ids_ref, slot_ref, count_ref):
    ids = ids_ref[...]
    n_top, n_tok = ids.shape
    experts = 2 * count_ref.shape[2]
    expert_of = lax.broadcasted_iota(jnp.int32, (experts, n_tok), 0)
    member = jnp.zeros((experts, n_tok), jnp.float32)
    for j in range(n_top):
        member = jnp.where(expert_of == ids[j:j + 1], 1.0, member)
    row = lax.broadcasted_iota(jnp.int32, (n_tok, n_tok), 0)
    col = lax.broadcasted_iota(jnp.int32, (n_tok, n_tok), 1)
    earlier = jnp.where(row < col, 1.0, 0.0).astype(jnp.bfloat16)
    member_lp = member.astype(jnp.bfloat16)
    before = jnp.dot(member_lp, earlier, preferred_element_type=jnp.float32)
    ones = jnp.ones((n_top, n_tok), jnp.bfloat16)
    counts = lax.dot_general(ones, member_lp, (((1,), (1,)), ((), ())), preferred_element_type=jnp.float32).astype(jnp.int32)
    half = n_tok // 2
    for h in (0, 1):
        count_ref[h] = counts[:, h * half:(h + 1) * half]
    for j in range(n_top):
        rank = jnp.sum(jnp.where(expert_of == ids[j:j + 1], before, 0.0), axis=0, keepdims=True)
        slot = ids[j:j + 1] * LANES + rank.astype(jnp.int32)
        for h in (0, 1):
            slot_ref[h, j:j + 1, :] = slot[:, h * half:(h + 1) * half]


def layer_kernel(capacity, *refs):
    (x, ids, gate), (w_in, w_out), (y,), mids, backs, ends, b_relay, c_relay, cb_relay, bb_relay, refs = take(refs, 3, 2, 1, 6, 6, 6, 6, 6, 6, 6, None)
    tokens, slots, gates, packed, rows, sums, got, sum_relay, (slot, count, count_x, count_y, count_z, count_other, mine, w_in_v, w_out_v, send, recv, local, extra) = take(refs, 3, 3, 3, 6, 6, 3, 3, 3, None)
    place = Place()
    n_tok, n_top = x.shape[0], slot.shape[1]
    half = n_tok // 2
    n_row = 2 * RING * RING * LANES
    index = iter(range(send.shape[0]))
    lane = lambda kind, axis, source, target, relay=None, switch=False: kind(place, axis, source, target, relay, send, recv, next(index), switch)
    first, second, third = [[ORDERS[r][k] for r in PARTS] for k in PARTS]

    a_small = [lane(Gather, first[r], lambda p, h: slot.at[h], lambda o, k, r=r: slots[r].at[o, k]) for r in PARTS]
    a_small.append(lane(Gather, 'x', lambda p, h: count.at[h], lambda o, k: count_x.at[o, k]))
    a_out = [lane(Gather, first[r], lambda p, h, r=r: x.at[pl.ds(h * half, half), pl.ds(SPAN_STARTS[r], SPAN)],
                  lambda o, k, r=r: tokens[r].at[o, pl.ds(k * half, half)]) for r in PARTS]
    along_y = lane(Gather, 'y', lambda p, h: count_x.at[:, h], lambda o, k: count_y.at[o, :, k])
    along_z = lane(Gather, 'z', lambda p, h: count_y.at[:, :, h], lambda o, k: count_z.at[o, :, :, k])
    swap = lane(Lane, 'z', None, None)
    a_gate = [lane(Gather, first[r], lambda p, h: mine.at[h], lambda o, k, r=r: gates[r].at[o, k]) for r in PARTS]
    b_out = [lane(Lane, second[r], lambda p, h, i=3 * q + r: packed[i].at[p, h],
                  lambda o, k, i=3 * q + r, r=r: mids[i].at[(slice(None), k) + spot(second[r], ORDERS[r][:2], o)], b_relay[3 * q + r], True) for q, r in BOTH]
    c_out = [lane(Lane, third[r], lambda p, h, i=3 * q + r: mids[i].at[p, h],
                  lambda o, k, i=3 * q + r, r=r: rows[i].at[(k,) + spot(third[r], 'zyx', o)], c_relay[3 * q + r]) for q, r in BOTH]
    c_back = [lane(Lane, third[r], lambda p, h, i=3 * q + r, r=r: rows[i].at[(h,) + spot(third[r], 'zyx', p)],
                   lambda o, k, i=3 * q + r: backs[i].at[o, k], cb_relay[3 * q + r]) for q, r in BOTH]
    b_back = [lane(Lane, second[r], lambda p, h, i=3 * q + r, r=r: backs[i].at[(slice(None), h) + spot(second[r], ORDERS[r][:2], p)],
                   lambda o, k, i=3 * q + r: ends[i].at[o, k], bb_relay[3 * q + r], True) for q, r in BOTH]
    a_back = [lane(Reduce, first[r], lambda p, h, r=r: sums[r].at[p, pl.ds(h * half, half)],
                   lambda side, h, r=r: got[r].at[side, pl.ds(h * half, half)], sum_relay[r]) for r in PARTS]
    one, two = slice(0, 3), slice(3, 6)

    def pack(q, r, step):
        a = place.pos(first[r], step)
        offset = STARTS[q][r] - SPAN_STARTS[r]
        for part in (0, 1):
            wanted = plane_slots((n_row // 2, half), ORDERS[r], place, q, part * n_row // 2)
            picks = []
            for h in (0, 1):
                pick = jnp.zeros((n_row // 2, half), jnp.float32)
                for j in range(n_top):
                    pick = jnp.where(wanted == slots[r][a, h, j:j + 1], 1.0, pick)
                picks.append(pick.astype(jnp.bfloat16))
            block = jnp.dot(jnp.concatenate(picks, axis=1), tokens[r][a, :, offset:offset + WIDTHS[q][r]], preferred_element_type=jnp.float32)
            packed[3 * q + r][2 * part:2 * part + 2, :, :, a] = block.astype(jnp.bfloat16).reshape(RING // 2, 2, RING, LANES, WIDTHS[q][r])

    def expert(q, step):
        core, z = step // RING, lax.rem(step, RING)
        total = None
        for r in PARTS:
            part = rows[3 * q + r][core, z].reshape(RING * RING * LANES, WIDTHS[q][r])
            term = jnp.dot(part, w_in_v[STARTS[q][r]:STARTS[q][r] + WIDTHS[q][r]], preferred_element_type=jnp.float32)
            total = term if total is None else total + term
        hidden = jax.nn.gelu(total, approximate=True).astype(jnp.bfloat16)
        for r in PARTS:
            res = jnp.dot(hidden, w_out_v[:, STARTS[q][r]:STARTS[q][r] + WIDTHS[q][r]], preferred_element_type=jnp.float32)
            rows[3 * q + r][core, z] = res.astype(jnp.bfloat16).reshape(RING, RING, LANES, WIDTHS[q][r])

    def weigh():
        counted = lambda ref: ref[...].reshape((RING**3,) + slot.shape)
        ahead = lax.broadcasted_iota(jnp.int32, (RING**3,) + slot.shape, 0) < place.chip
        off = jnp.sum(jnp.where(ahead, counted(count_z), 0), axis=0) + jnp.where(place.core == 1, jnp.sum(counted(count_other), axis=0), 0)
        off = jnp.concatenate([off[0], off[1]], axis=1)
        high, low = (off >> 7).astype(jnp.bfloat16), (off & 127).astype(jnp.bfloat16)
        expert_of = lax.broadcasted_iota(jnp.int32, (off.shape[1], n_tok), 0)
        for j in range(n_top):
            choice = jnp.where(expert_of == ids[j:j + 1], 1.0, 0.0).astype(jnp.bfloat16)
            before = 128 * jnp.dot(high, choice, preferred_element_type=jnp.float32) + jnp.dot(low, choice, preferred_element_type=jnp.float32)
            before = before[0:1].astype(jnp.int32)
            for h in (0, 1):
                cut = slice(h * half, (h + 1) * half)
                rank = before[:, cut] + slot[h, j:j + 1] - ids[j:j + 1, cut] * LANES
                mine[h, j:j + 1] = jnp.where(rank < capacity, gate[j:j + 1, cut], 0.0)

    def combine(q, r, step, h):
        a = place.pos(first[r], step)
        wanted = plane_slots((n_row, half), ORDERS[r], place, q)
        weight = jnp.zeros((n_row, half), jnp.float32)
        for j in range(n_top):
            weight = jnp.where(wanted == slots[r][a, h, j:j + 1], gates[r][a, h, j:j + 1], weight)
        high = weight.astype(jnp.bfloat16)
        rest = weight - high.astype(jnp.float32)
        mid = rest.astype(jnp.bfloat16)
        low = (rest - mid.astype(jnp.float32)).astype(jnp.bfloat16)
        weights = jnp.concatenate([high, mid, low], axis=1)
        offset = STARTS[q][r] - SPAN_STARTS[r]
        for lo, hi in ((0, 384), (384, WIDTHS[q][r])):
            back = packed[3 * q + r][:, :, :, a, :, lo:hi].reshape(n_row, hi - lo)
            mix = lax.dot_general(weights, back, (((0,), (0,)), ((), ())), preferred_element_type=jnp.float32)
            sums[r][a, pl.ds(pl.multiple_of(h * half, half), half), offset + lo:offset + hi] += mix[:half] + mix[half:2 * half] + mix[2 * half:]

    def wait(copies):
        for copy in copies:
            copy.wait()

    def own(lanes):
        return [copy for item in lanes for copy in item.own(local)]

    def load(src, dst, n):
        copy = pltpu.make_async_copy(src, dst, extra.at[n])
        copy.start()
        return copy

    def own_rows(lanes, i):
        me = [place.coord[item.axis] for item in lanes]
        return [load(item.source(me[r], place.core), packed[i + r].at[me[r], place.core], 4 + i + r) for r, item in enumerate(lanes)]

    def fetch(i, near):
        axis = second[i % 3]
        pieces = [(place.pos(axis, step),) for step in ((1, 3) if near else (2,))]
        if near:
            pieces.append((place.coord[axis], place.other))
        return [load(ends[i].at[at], packed[i].at[at], 10 + 4 * i + n + (0 if near else 3)) for n, at in enumerate(pieces)]

    kept = own(a_out)
    weights = [load(w_in.at[0], w_in_v, 0), load(w_out.at[0], w_out_v, 1)]
    place.greet(True)
    run(a_out, 'near')
    route(ids, slot, count)
    kept += own(a_small)
    run(a_small, 'near')
    wait(kept)
    for r in PARTS:
        pack(0, r, 0)
    run(a_out, 'forward')
    run(a_small, 'forward', 'arrive_near')
    run(a_out, 'arrive_near')
    for r in PARTS:
        pl.loop(0, 2)(lambda n, r=r: pack(0, r, 1 + 2 * n))
    run(a_small, 'arrive_far')
    run(a_out, 'arrive_far')
    for r in PARTS:
        pack(0, r, 2)
    run(b_out[one], 'far', 'near')
    kept_y = own([along_y])
    run([along_y], 'near')
    kept_b = own(b_out[one])
    for r in PARTS:
        pl.loop(0, RING)(lambda n, r=r: pack(1, r, n))
    run(b_out[one], 'forward')
    run(b_out[two], 'far', 'near')
    kept_b += own(b_out[two])
    run([along_y], 'forward')
    run(b_out[two], 'forward')
    wait(kept_b)
    run(b_out[one], 'arrive')
    run(c_out[one], 'far', 'near')
    kept = own(c_out[one])
    run([along_y], 'arrive_near', 'arrive_far')
    wait(kept_y)
    kept_z = own([along_z])
    run([along_z], 'near')
    run(c_out[one], 'forward')
    run(b_out[two], 'arrive')
    run(c_out[two], 'far', 'near')
    kept_two = own(c_out[two])
    run(c_out[one], 'arrive')
    wait(kept + weights)
    pl.loop(0, 2 * RING)(lambda n: expert(0, n))
    weights = [load(w_in.at[1], w_in_v, 2), load(w_out.at[1], w_out_v, 3)]
    run(c_out[two], 'forward')
    run(c_back[one], 'far', 'near')
    kept = own(c_back[one])
    run([along_z], 'forward')
    run(c_out[two], 'arrive')
    wait(kept_two + weights)
    pl.loop(0, 2 * RING)(lambda n: expert(1, n))
    run(c_back[one], 'forward')
    run(c_back[two], 'far', 'near')
    kept_two = own(c_back[two])
    run([along_z], 'arrive_near', 'arrive_far')
    wait(kept_z)
    swap.start(count_z, count_other, 0, 0, place.other, place.chip)
    swap.landed(count_other, 0)
    weigh()
    kept_gate = own(a_gate)
    run(a_gate, 'near')
    run(c_back[two], 'forward')
    run(c_back[one], 'arrive')
    wait(kept)
    run(b_back[one], 'far', 'near')
    run(b_out, 'drain')
    kept = own_rows(b_back[one], 0)
    for r in PARTS:
        sums[r][...] = jnp.zeros_like(sums[r])
    run(a_gate, 'forward')
    run(b_back[one], 'forward')
    run(c_back[two], 'arrive')
    wait(kept_two)
    run(b_back[two], 'far', 'near')
    kept_two = own_rows(b_back[two], 3)
    run(b_back[one], 'arrive')
    wait(kept)
    loads = [fetch(r, True) + fetch(r, False) for r in PARTS]
    run(a_gate, 'arrive_near', 'arrive_far')
    wait(kept_gate)
    for r in PARTS:
        wait(loads[r])
        pl.loop(0, 2 * RING)(lambda n, r=r: combine(0, r, n // 2, lax.rem(n, 2)))
    run(b_back[two], 'forward', 'arrive_near')
    loads = [fetch(3 + r, True) for r in PARTS]
    wait(kept_two)
    run(b_back[two], 'arrive_far')
    loads = [loads[r] + fetch(3 + r, False) for r in PARTS]
    for r in PARTS:
        wait(loads[r])
        pl.loop(0, 2)(lambda h, r=r: combine(1, r, 2, h))
    run(a_back, 'far')
    for r in PARTS:
        pl.loop(0, 4)(lambda n, r=r: combine(1, r, 1 + 2 * (n // 2), lax.rem(n, 2)))
    run(a_back, 'near', 'add')
    run(a_back, 'forward')
    for r in PARTS:
        pl.loop(0, 2)(lambda h, r=r: combine(1, r, 0, h))
        sums[r][place.coord[first[r]], :, :SPAN_STARTS[1]] += x[:, SPAN_STARTS[r]:SPAN_STARTS[r] + SPAN_STARTS[1]].astype(jnp.float32)
    sums[2][place.coord[first[2]], :, SPAN_STARTS[1]:] += x[:, SPAN_STARTS[2] + SPAN_STARTS[1]:].astype(jnp.float32)
    run(a_back, 'arrive')
    for c in range(0, x.shape[1], 128):
        total = None
        for r in PARTS:
            if SPAN_STARTS[r] <= c < SPAN_STARTS[r] + SPAN:
                cut = slice(c - SPAN_STARTS[r], c - SPAN_STARTS[r] + 128)
                part = sums[r][place.coord[first[r]], :, cut] + got[r][0, :, cut] + got[r][1, :, cut]
                total = part if total is None else total + part
        y[:, c:c + 128] = total.astype(y.dtype)
    run(a_small + a_out + [along_y, along_z, swap] + a_gate + c_out + c_back + b_back + a_back, 'drain')


def solution(mesh):
    dev_axes = ('ep2', 'ep')
    bf16, f32, i32 = jnp.bfloat16, jnp.float32, jnp.int32
    group_size = mesh.shape['ep2'] * mesh.shape['ep']
    anywhere, near, dma = pl.BlockSpec(memory_space=pl.ANY), pl.BlockSpec(memory_space=pltpu.VMEM), pltpu.SemaphoreType.DMA
    vmem = lambda shapes, dtype: [pltpu.VMEM(shape, dtype) for shape in shapes]
    per_part = lambda *lead: [lead + (RING, RING, LANES, WIDTHS[q][r]) for q, r in BOTH]

    def local_step(x, ids, gate, w_a, w_b):
        n_tok, d_model = x.shape
        n_top = ids.shape[1]
        experts = w_a.shape[0] * group_size
        capacity = 8 * ((5 * group_size * n_tok * n_top) // (32 * experts))
        small = (2, n_top, n_tok // 2)
        ids_t, gate_t = ids.T, gate.T
        shape = jax.ShapeDtypeStruct
        between = per_part(RING, 2) * 3 + per_part(2) * 4
        lanes = 4 + 3 + 2 + 1 + 3 + 4 * 6 + 3
        return pl.pallas_call(
            functools.partial(layer_kernel, capacity),
            in_specs=[near] * 3 + [anywhere] * 2,
            out_specs=[near] + [anywhere] * len(between),
            out_shape=[shape(x.shape, x.dtype)] + [shape(s, bf16) for s in between],
            scratch_shapes=vmem([(RING, n_tok, SPAN)] * 3, bf16) + vmem([(RING,) + small] * 3, i32) + vmem([(RING,) + small] * 3, f32)
            + vmem(per_part(RING, 2), bf16) + vmem(per_part(2, RING), bf16) + vmem([(RING, n_tok, SPAN)] * 3, f32)
            + vmem([(2, n_tok, SPAN)] * 3, f32) + vmem([(2, n_tok // 2, SPAN)] * 3, f32)
            + vmem([small, (2, n_top, experts // 2), (RING,) + small, (RING, RING) + small] + [(RING, RING, RING) + small] * 2, i32) + vmem([small], f32)
            + vmem([w_a.shape[1:], w_b.shape[1:]], bf16) + [dma((lanes, 9)), dma((lanes, 9)), dma((lanes, 2)), dma((34,))],
            compiler_params=pltpu.CompilerParams(collective_id=0, has_side_effects=True, vmem_limit_bytes=67043328),
            name='layer',
        )(x, ids_t, gate_t, w_a, w_b)[0]

    tok_spec = P(('dp', 'ep2', 'ep'), None)
    w_spec = P(dev_axes, None, None)
    return jax.shard_map(local_step, mesh=mesh, in_specs=(tok_spec, tok_spec, tok_spec, w_spec, w_spec), out_specs=tok_spec, check_vma=False)
```

```python
import functools

import jax
import jax.numpy as jnp
from jax import lax
from jax.experimental import pallas as pl
from jax.experimental.pallas import tpu as pltpu
from jax.sharding import PartitionSpec as P

MESH = pl.DeviceIdType.MESH
LANES = 16
RING = 4
STRIDE = {'x': 1, 'y': RING, 'z': RING * RING}
ORDERS = ('xyz', 'yzx', 'zxy')
STREAMS = range(2)
PARTS = range(3)
WIDTHS = ((640, 640, 768), (768, 640, 640))
STARTS = ((0, 640, 1280), (0, 768, 1408))
SPAN = 768
SPAN_STARTS = (0, 640, 1280)
BOTH = [(q, r) for q in STREAMS for r in PARTS]


class Place:
    def __init__(self):
        self.core, self.chip = lax.axis_index('ep2'), lax.axis_index('ep')
        self.other = 1 - self.core
        self.coord = {axis: lax.rem(self.chip // stride, RING) for axis, stride in STRIDE.items()}

    def pos(self, axis, step):
        return lax.rem(self.coord[axis] + step + RING, RING)

    def at(self, axis, step):
        return self.chip + (self.pos(axis, step) - self.coord[axis]) * STRIDE[axis]

    def greet(self, both_cores):
        barrier = pltpu.get_barrier_semaphore()
        peers = [(self.other, self.chip)]
        for axis in STRIDE:
            for step in (1, -1):
                peers += [(c, self.at(axis, step)) for c in ((self.core, self.other) if both_cores else (self.core,))]
        for c, chip in peers:
            pl.semaphore_signal(barrier, inc=1, device_id=(0, c, chip), device_id_type=MESH)
        pl.semaphore_wait(barrier, len(peers))


class Lane:
    def __init__(self, place, axis, source, target, relay, send, recv, index, switch=False):
        self.place, self.axis, self.source, self.target, self.relay = place, axis, source, target, relay
        self.send, self.recv, self.index, self.switch = send, recv, index, switch
        self.sent = []

    def start(self, src, dst, s, r, core, chip):
        copy = pltpu.make_async_remote_copy(src_ref=src, dst_ref=dst, send_sem=self.send.at[self.index, s], recv_sem=self.recv.at[self.index, r], device_id=(0, core, chip), device_id_type=MESH)
        copy.start()
        self.sent.append(copy)

    def landed(self, dst, r):
        pltpu.make_async_remote_copy(src_ref=dst, dst_ref=dst, send_sem=self.send.at[self.index, 0], recv_sem=self.recv.at[self.index, r], device_id=(0, self.place.core, self.place.chip), device_id_type=MESH).wait_recv()

    def far(self):
        p = self.place
        for h, step in ((0, 1), (1, -1)):
            self.start(self.source(p.pos(self.axis, 2), h), self.relay.at[h], h, h, p.core, p.at(self.axis, step))

    def near(self):
        p = self.place
        me = p.coord[self.axis]
        for d, step in ((0, 1), (1, -1)):
            for h in (0, 1):
                k, c = (p.core, h) if self.switch else (h, p.core)
                self.start(self.source(p.pos(self.axis, step), h), self.target(me, k), 2 + 2 * d + h, 2 + 2 * d + k, c, p.at(self.axis, step))
        if self.switch:
            self.start(self.source(me, p.other), self.target(me, p.core), 8, 8, p.other, p.chip)

    def forward(self):
        p = self.place
        for h, step in ((0, 1), (1, -1)):
            self.landed(self.relay.at[h], h)
            k, c, r = (p.core, h, 6 + p.core) if self.switch else (h, p.core, 6 + h)
            self.start(self.relay.at[h], self.target(p.pos(self.axis, -step), k), 6 + h, r, c, p.at(self.axis, step))

    def arrive_near(self):
        p = self.place
        for d, step in ((0, -1), (1, 1)):
            for k in (0, 1):
                self.landed(self.target(p.pos(self.axis, step), k), 2 + 2 * d + k)
        if self.switch:
            self.landed(self.target(p.coord[self.axis], p.other), 8)

    def arrive_far(self):
        for k in (0, 1):
            self.landed(self.target(self.place.pos(self.axis, 2), k), 6 + k)

    def arrive(self):
        self.arrive_near()
        self.arrive_far()

    def own(self, local):
        p = self.place
        me = p.coord[self.axis]
        halves = [(p.core, p.core)] if self.switch else [(0, 0), (1, 1)]
        copies = [pltpu.make_async_copy(self.source(me, h), self.target(me, k), local.at[self.index, n]) for n, (h, k) in enumerate(halves)]
        for copy in copies:
            copy.start()
        return copies

    def drain(self):
        for copy in self.sent:
            copy.wait_send()


class Gather(Lane):
    def near(self):
        p = self.place
        me = p.coord[self.axis]
        for d, step, halves in ((0, 1, (0, 1)), (1, -1, (1, 0))):
            for h in halves:
                self.start(self.source(me, h), self.target(me, h), 2 + 2 * d + h, 2 + 2 * d + h, p.core, p.at(self.axis, step))

    def forward(self):
        p = self.place
        for h, step in ((0, 1), (1, -1)):
            part = self.target(p.pos(self.axis, -step), h)
            self.landed(part, 2 + 2 * h + h)
            self.start(part, part, 6 + h, 6 + h, p.core, p.at(self.axis, step))

    def arrive_near(self):
        p = self.place
        self.landed(self.target(p.pos(self.axis, -1), 1), 3)
        self.landed(self.target(p.pos(self.axis, 1), 0), 4)

    def arrive_far(self):
        for h in (0, 1):
            self.landed(self.target(self.place.pos(self.axis, 2), h), 6 + h)


class Reduce(Lane):
    def near(self):
        p = self.place
        for side, step in ((0, 1), (1, -1)):
            self.start(self.source(p.pos(self.axis, step), 1 - side), self.target(side, 1 - side), 2 + side, 2 + side, p.core, p.at(self.axis, step))

    def add(self):
        for h, step in ((0, 1), (1, -1)):
            self.landed(self.relay.at[h], h)
            self.relay[h] += self.source(self.place.pos(self.axis, step), h)[...]

    def forward(self):
        p = self.place
        for h, step in ((0, 1), (1, -1)):
            self.start(self.relay.at[h], self.target(h, h), 4 + h, 4 + h, p.core, p.at(self.axis, step))

    def arrive(self):
        for side in (0, 1):
            self.landed(self.target(side, 1 - side), 2 + side)
            self.landed(self.target(side, side), 4 + side)


def run(lanes, *steps):
    for step in steps:
        for lane in lanes:
            getattr(lane, step)()


def take(refs, *counts):
    refs = list(refs)
    for count in counts:
        yield refs[:count]
        del refs[:count]


def spot(axis, order, index):
    return (slice(None),) * [a for a in 'zyx' if a in order].index(axis) + (index,)


def plane_slots(shape, order, place, q, base=0):
    row = lax.broadcasted_iota(jnp.int32, shape, 0) + base
    first, second, third = [STRIDE[axis] for axis in order]
    dev = ((row >> 6) & 1) * RING**3 + (row >> 7) * second + ((row >> 4) & (RING - 1)) * third + place.coord[order[0]] * first
    return dev * (2 * LANES) + q * LANES + (row & (LANES - 1))


def line_slots(shape, order, place, q):
    row = lax.broadcasted_iota(jnp.int32, shape, 0)
    first, second, third = [STRIDE[axis] for axis in order]
    dev = ((row >> 4) & 1) * RING**3 + (row >> 5) * third + place.coord[order[0]] * first + place.coord[order[1]] * second
    return dev * (2 * LANES) + q * LANES + (row & (LANES - 1))


def route(ids_ref, slot_ref, count_ref):
    ids = ids_ref[...]
    n_top, n_tok = ids.shape
    experts = 2 * count_ref.shape[2]
    expert_of = lax.broadcasted_iota(jnp.int32, (experts, n_tok), 0)
    member = jnp.zeros((experts, n_tok), jnp.float32)
    for j in range(n_top):
        member = jnp.where(expert_of == ids[j:j + 1], 1.0, member)
    row = lax.broadcasted_iota(jnp.int32, (n_tok, n_tok), 0)
    col = lax.broadcasted_iota(jnp.int32, (n_tok, n_tok), 1)
    earlier = jnp.where(row < col, 1.0, 0.0).astype(jnp.bfloat16)
    member_lp = member.astype(jnp.bfloat16)
    before = jnp.dot(member_lp, earlier, preferred_element_type=jnp.float32)
    ones = jnp.ones((n_top, n_tok), jnp.bfloat16)
    counts = lax.dot_general(ones, member_lp, (((1,), (1,)), ((), ())), preferred_element_type=jnp.float32).astype(jnp.int32)
    half = n_tok // 2
    for h in (0, 1):
        count_ref[h] = counts[:, h * half:(h + 1) * half]
    for j in range(n_top):
        rank = jnp.sum(jnp.where(expert_of == ids[j:j + 1], before, 0.0), axis=0, keepdims=True)
        slot = ids[j:j + 1] * LANES + rank.astype(jnp.int32)
        for h in (0, 1):
            slot_ref[h, j:j + 1, :] = slot[:, h * half:(h + 1) * half]


def layer_kernel(capacity, *refs):
    (x, ids, gate), (w_in, w_out), (y,), wide, backs, ends, c_relay, cb_relay, bb_relay, refs = take(refs, 3, 2, 1, 3, 6, 6, 6, 6, 6, None)
    tokens, slots, wide_slots, gates, packed, rows, sums, got, sum_relay, (slot, count, count_x, count_y, count_z, count_other, mine, w_in_v, w_out_v, send, recv, local, extra) = take(refs, 3, 3, 3, 3, 6, 6, 3, 3, 3, None)
    place = Place()
    n_tok, n_top = x.shape[0], slot.shape[1]
    half = n_tok // 2
    n_row = 2 * RING * RING * LANES
    index = iter(range(send.shape[0]))
    lane = lambda kind, axis, source, target, relay=None, switch=False: kind(place, axis, source, target, relay, send, recv, next(index), switch)
    first, second, third = [[ORDERS[r][k] for r in PARTS] for k in PARTS]

    a_small = [lane(Gather, first[r], lambda p, h: slot.at[h], lambda o, k, r=r: slots[r].at[o, k]) for r in PARTS]
    a_small.append(lane(Gather, 'x', lambda p, h: count.at[h], lambda o, k: count_x.at[o, k]))
    a_out = [lane(Gather, first[r], lambda p, h, r=r: x.at[pl.ds(h * half, half), pl.ds(SPAN_STARTS[r], SPAN)],
                  lambda o, k, r=r: tokens[r].at[o, pl.ds(k * half, half)]) for r in PARTS]
    along_y = lane(Gather, 'y', lambda p, h: count_x.at[:, h], lambda o, k: count_y.at[o, :, k])
    along_z = lane(Gather, 'z', lambda p, h: count_y.at[:, :, h], lambda o, k: count_z.at[o, :, :, k])
    swap = lane(Lane, 'z', None, None)
    a_gate = [lane(Gather, first[r], lambda p, h: mine.at[h], lambda o, k, r=r: gates[r].at[o, k]) for r in PARTS]
    b_small = [lane(Gather, second[r], lambda p, h, r=r: slots[r].at[pl.ds(2 * h, 2)], lambda o, k, r=r: wide_slots[r].at[o, pl.ds(2 * k, 2)]) for r in PARTS]
    b_out = [lane(Gather, second[r], lambda p, h, r=r: tokens[r].at[pl.ds(2 * h, 2)], lambda o, k, r=r: wide[r].at[o, pl.ds(2 * k, 2)]) for r in PARTS]
    c_out = [lane(Lane, third[r], lambda p, h, i=3 * q + r: packed[i].at[p, h],
                  lambda o, k, i=3 * q + r, r=r: rows[i].at[(k,) + spot(third[r], 'zyx', o)], c_relay[3 * q + r], True) for q, r in BOTH]
    c_back = [lane(Lane, third[r], lambda p, h, i=3 * q + r, r=r: rows[i].at[(h,) + spot(third[r], 'zyx', p)],
                   lambda o, k, i=3 * q + r: backs[i].at[o, k], cb_relay[3 * q + r]) for q, r in BOTH]
    b_back = [lane(Lane, second[r], lambda p, h, i=3 * q + r, r=r: backs[i].at[(slice(None), h) + spot(second[r], ORDERS[r][:2], p)],
                   lambda o, k, i=3 * q + r: ends[i].at[o, k], bb_relay[3 * q + r], True) for q, r in BOTH]
    a_back = [lane(Reduce, first[r], lambda p, h, r=r: sums[r].at[p, pl.ds(h * half, half)],
                   lambda side, h, r=r: got[r].at[side, pl.ds(h * half, half)], sum_relay[r]) for r in PARTS]
    one, two = slice(0, 3), slice(3, 6)

    def pack(q, r, step, a):
        b = place.pos(second[r], step)
        n = 2 * RING * LANES
        wanted = line_slots((n, half), ORDERS[r], place, q)
        picks = []
        for h in (0, 1):
            pick = jnp.zeros((n, half), jnp.float32)
            for j in range(n_top):
                pick = jnp.where(wanted == wide_slots[r][b, a, h, j:j + 1], 1.0, pick)
            picks.append(pick.astype(jnp.bfloat16))
        offset = STARTS[q][r] - SPAN_STARTS[r]
        block = jnp.dot(jnp.concatenate(picks, axis=1), tokens[r][a, :, offset:offset + WIDTHS[q][r]], preferred_element_type=jnp.float32)
        spots = (b, a) if 'zyx'.index(second[r]) < 'zyx'.index(first[r]) else (a, b)
        packed[3 * q + r][(slice(None), slice(None)) + spots] = block.astype(jnp.bfloat16).reshape(RING, 2, LANES, WIDTHS[q][r])

    def expert(q, step):
        core, z = step // RING, lax.rem(step, RING)
        total = None
        for r in PARTS:
            part = rows[3 * q + r][core, z].reshape(RING * RING * LANES, WIDTHS[q][r])
            term = jnp.dot(part, w_in_v[STARTS[q][r]:STARTS[q][r] + WIDTHS[q][r]], preferred_element_type=jnp.float32)
            total = term if total is None else total + term
        hidden = jax.nn.gelu(total, approximate=True).astype(jnp.bfloat16)
        for r in PARTS:
            res = jnp.dot(hidden, w_out_v[:, STARTS[q][r]:STARTS[q][r] + WIDTHS[q][r]], preferred_element_type=jnp.float32)
            rows[3 * q + r][core, z] = res.astype(jnp.bfloat16).reshape(RING, RING, LANES, WIDTHS[q][r])

    def weigh():
        counted = lambda ref: ref[...].reshape((RING**3,) + slot.shape)
        ahead = lax.broadcasted_iota(jnp.int32, (RING**3,) + slot.shape, 0) < place.chip
        off = jnp.sum(jnp.where(ahead, counted(count_z), 0), axis=0) + jnp.where(place.core == 1, jnp.sum(counted(count_other), axis=0), 0)
        off = jnp.concatenate([off[0], off[1]], axis=1)
        high, low = (off >> 7).astype(jnp.bfloat16), (off & 127).astype(jnp.bfloat16)
        expert_of = lax.broadcasted_iota(jnp.int32, (off.shape[1], n_tok), 0)
        for j in range(n_top):
            choice = jnp.where(expert_of == ids[j:j + 1], 1.0, 0.0).astype(jnp.bfloat16)
            before = 128 * jnp.dot(high, choice, preferred_element_type=jnp.float32) + jnp.dot(low, choice, preferred_element_type=jnp.float32)
            before = before[0:1].astype(jnp.int32)
            for h in (0, 1):
                cut = slice(h * half, (h + 1) * half)
                rank = before[:, cut] + slot[h, j:j + 1] - ids[j:j + 1, cut] * LANES
                mine[h, j:j + 1] = jnp.where(rank < capacity, gate[j:j + 1, cut], 0.0)

    def combine(q, r, step, h):
        a = place.pos(first[r], step)
        wanted = plane_slots((n_row, half), ORDERS[r], place, q)
        weight = jnp.zeros((n_row, half), jnp.float32)
        for j in range(n_top):
            weight = jnp.where(wanted == slots[r][a, h, j:j + 1], gates[r][a, h, j:j + 1], weight)
        high = weight.astype(jnp.bfloat16)
        rest = weight - high.astype(jnp.float32)
        mid = rest.astype(jnp.bfloat16)
        low = (rest - mid.astype(jnp.float32)).astype(jnp.bfloat16)
        weights = jnp.concatenate([high, mid, low], axis=1)
        offset = STARTS[q][r] - SPAN_STARTS[r]
        for lo, hi in ((0, 384), (384, WIDTHS[q][r])):
            back = packed[3 * q + r][:, :, :, a, :, lo:hi].reshape(n_row, hi - lo)
            mix = lax.dot_general(weights, back, (((0,), (0,)), ((), ())), preferred_element_type=jnp.float32)
            sums[r][a, pl.ds(pl.multiple_of(h * half, half), half), offset + lo:offset + hi] += mix[:half] + mix[half:2 * half] + mix[2 * half:]

    def wait(copies):
        for copy in copies:
            copy.wait()

    def wait_sent(item, count):
        for copy in item.sent[:count]:
            copy.wait_send()
        del item.sent[:count]

    def own(lanes):
        return [copy for item in lanes for copy in item.own(local)]

    def load(src, dst, n):
        copy = pltpu.make_async_copy(src, dst, extra.at[n])
        copy.start()
        return copy

    def own_rows(lanes, i):
        me = [place.coord[item.axis] for item in lanes]
        return [load(item.source(me[r], place.core), packed[i + r].at[me[r], place.core], 4 + i + r) for r, item in enumerate(lanes)]

    def fetch(i, near):
        axis = second[i % 3]
        pieces = [(place.pos(axis, step),) for step in ((1, 3) if near else (2,))]
        if near:
            pieces.append((place.coord[axis], place.other))
        return [load(ends[i].at[at], packed[i].at[at], 10 + 4 * i + n + (0 if near else 3)) for n, at in enumerate(pieces)]

    def slabs(step):
        return [load(wide[r].at[place.pos(second[r], step)], tokens[r], 4 + r) for r in PARTS]

    kept = own(a_out)
    weights = [load(w_in.at[0], w_in_v, 0), load(w_out.at[0], w_out_v, 1)]
    place.greet(True)
    run(a_out, 'near')
    route(ids, slot, count)
    kept += own(a_small)
    run(a_small, 'near')
    wait(kept)
    run(a_out, 'forward')
    run(a_small, 'forward', 'arrive_near', 'arrive_far')
    kept = own(b_small + [along_y])
    run(b_small + [along_y], 'near')
    run(a_out, 'arrive_near', 'arrive_far')
    run(b_out, 'near')
    run(b_small + [along_y], 'forward')
    wait(kept)
    for r in PARTS:
        pl.loop(0, RING)(lambda a, r=r: [pack(q, r, 0, a) for q in STREAMS] and None)
    run(b_out, 'forward')
    run(b_small, 'arrive_near')
    run(b_out, 'arrive_near')
    run(a_out, 'drain')
    for item in b_out:
        wait_sent(item, 4)

    @pl.loop(0, 2)
    def _(n):
        loads = slabs(1 + 2 * n)
        for r in PARTS:
            loads[r].wait()
            pl.loop(0, RING)(lambda a, r=r: [pack(q, r, 1 + 2 * n, a) for q in STREAMS] and None)

    run(b_small + [along_y], 'arrive_far')
    run([along_y], 'arrive_near')
    kept_z = own([along_z])
    run([along_z], 'near')
    run(b_out, 'arrive_far')
    loads = slabs(2)
    for r in PARTS:
        loads[r].wait()
        pl.loop(0, RING)(lambda a, r=r: pack(0, r, 2, a))
    run(c_out[one], 'far', 'near')
    kept = own(c_out[one])
    for r in PARTS:
        pl.loop(0, RING)(lambda a, r=r: pack(1, r, 2, a))
    run(c_out[one], 'forward')
    run(c_out[two], 'far', 'near')
    kept_two = own(c_out[two])
    run([along_z], 'forward')
    run(c_out[one], 'arrive')
    wait(kept + weights)
    pl.loop(0, 2 * RING)(lambda n: expert(0, n))
    weights = [load(w_in.at[1], w_in_v, 2), load(w_out.at[1], w_out_v, 3)]
    run(c_out[two], 'forward')
    run(c_back[one], 'far', 'near')
    kept = own(c_back[one])
    run(c_out[two], 'arrive')
    wait(kept_two + weights)
    pl.loop(0, 2 * RING)(lambda n: expert(1, n))
    run(c_back[one], 'forward')
    run(c_back[two], 'far', 'near')
    kept_two = own(c_back[two])
    run([along_z], 'arrive_near', 'arrive_far')
    wait(kept_z)
    swap.start(count_z, count_other, 0, 0, place.other, place.chip)
    swap.landed(count_other, 0)
    weigh()
    kept_gate = own(a_gate)
    run(a_gate, 'near')
    run(c_back[two], 'forward')
    run(c_back[one], 'arrive')
    wait(kept)
    run(b_back[one], 'far', 'near')
    run(c_out, 'drain')
    kept = own_rows(b_back[one], 0)
    for r in PARTS:
        sums[r][...] = jnp.zeros_like(sums[r])
    run(a_gate, 'forward')
    run(b_back[one], 'forward')
    run(c_back[two], 'arrive')
    wait(kept_two)
    run(b_back[two], 'far', 'near')
    kept_two = own_rows(b_back[two], 3)
    run(b_back[one], 'arrive')
    wait(kept)
    loads = [fetch(r, True) + fetch(r, False) for r in PARTS]
    run(a_gate, 'arrive_near', 'arrive_far')
    wait(kept_gate)
    for r in PARTS:
        wait(loads[r])
        pl.loop(0, 2 * RING)(lambda n, r=r: combine(0, r, n // 2, lax.rem(n, 2)))
    run(b_back[two], 'forward', 'arrive_near')
    loads = [fetch(3 + r, True) for r in PARTS]
    wait(kept_two)
    run(b_back[two], 'arrive_far')
    loads = [loads[r] + fetch(3 + r, False) for r in PARTS]
    for r in PARTS:
        wait(loads[r])
        pl.loop(0, 2)(lambda h, r=r: combine(1, r, 2, h))
    run(a_back, 'far')
    for r in PARTS:
        pl.loop(0, 4)(lambda n, r=r: combine(1, r, 1 + 2 * (n // 2), lax.rem(n, 2)))
    run(a_back, 'near', 'add')
    run(a_back, 'forward')
    for r in PARTS:
        pl.loop(0, 2)(lambda h, r=r: combine(1, r, 0, h))
        sums[r][place.coord[first[r]], :, :SPAN_STARTS[1]] += x[:, SPAN_STARTS[r]:SPAN_STARTS[r] + SPAN_STARTS[1]].astype(jnp.float32)
    sums[2][place.coord[first[2]], :, SPAN_STARTS[1]:] += x[:, SPAN_STARTS[2] + SPAN_STARTS[1]:].astype(jnp.float32)
    run(a_back, 'arrive')
    for c in range(0, x.shape[1], 128):
        total = None
        for r in PARTS:
            if SPAN_STARTS[r] <= c < SPAN_STARTS[r] + SPAN:
                cut = slice(c - SPAN_STARTS[r], c - SPAN_STARTS[r] + 128)
                part = sums[r][place.coord[first[r]], :, cut] + got[r][0, :, cut] + got[r][1, :, cut]
                total = part if total is None else total + part
        y[:, c:c + 128] = total.astype(y.dtype)
    run(a_small + b_small + b_out + [along_y, along_z, swap] + a_gate + c_back + b_back + a_back, 'drain')


def solution(mesh):
    dev_axes = ('ep2', 'ep')
    bf16, f32, i32 = jnp.bfloat16, jnp.float32, jnp.int32
    group_size = mesh.shape['ep2'] * mesh.shape['ep']
    anywhere, near, dma = pl.BlockSpec(memory_space=pl.ANY), pl.BlockSpec(memory_space=pltpu.VMEM), pltpu.SemaphoreType.DMA
    vmem = lambda shapes, dtype: [pltpu.VMEM(shape, dtype) for shape in shapes]
    per_part = lambda *lead: [lead + (RING, RING, LANES, WIDTHS[q][r]) for q, r in BOTH]

    def local_step(x, ids, gate, w_a, w_b):
        n_tok, d_model = x.shape
        n_top = ids.shape[1]
        experts = w_a.shape[0] * group_size
        capacity = 8 * ((5 * group_size * n_tok * n_top) // (32 * experts))
        small = (2, n_top, n_tok // 2)
        ids_t, gate_t = ids.T, gate.T
        shape = jax.ShapeDtypeStruct
        between = [(RING, RING, n_tok, SPAN)] * 3 + per_part(RING, 2) * 2 + per_part(2) * 3
        lanes = 4 + 3 + 2 + 1 + 3 + 3 + 3 + 3 * 6 + 3
        return pl.pallas_call(
            functools.partial(layer_kernel, capacity),
            in_specs=[near] * 3 + [anywhere] * 2,
            out_specs=[near] + [anywhere] * len(between),
            out_shape=[shape(x.shape, x.dtype)] + [shape(s, bf16) for s in between],
            scratch_shapes=vmem([(RING, n_tok, SPAN)] * 3, bf16) + vmem([(RING,) + small] * 3 + [(RING, RING) + small] * 3, i32) + vmem([(RING,) + small] * 3, f32)
            + vmem(per_part(RING, 2), bf16) + vmem(per_part(2, RING), bf16) + vmem([(RING, n_tok, SPAN)] * 3, f32)
            + vmem([(2, n_tok, SPAN)] * 3, f32) + vmem([(2, n_tok // 2, SPAN)] * 3, f32)
            + vmem([small, (2, n_top, experts // 2), (RING,) + small, (RING, RING) + small] + [(RING, RING, RING) + small] * 2, i32) + vmem([small], f32)
            + vmem([w_a.shape[1:], w_b.shape[1:]], bf16) + [dma((lanes, 9)), dma((lanes, 9)), dma((lanes, 2)), dma((34,))],
            compiler_params=pltpu.CompilerParams(collective_id=0, has_side_effects=True, vmem_limit_bytes=67043328),
            name='layer',
        )(x, ids_t, gate_t, w_a, w_b)[0]

    tok_spec = P(('dp', 'ep2', 'ep'), None)
    w_spec = P(dev_axes, None, None)
    return jax.shard_map(local_step, mesh=mesh, in_specs=(tok_spec, tok_spec, tok_spec, w_spec, w_spec), out_specs=tok_spec, check_vma=False)
```

```python
import functools

import jax
import jax.numpy as jnp
from jax import lax
from jax.experimental import pallas as pl
from jax.experimental.pallas import tpu as pltpu
from jax.sharding import PartitionSpec as P

MESH = pl.DeviceIdType.MESH
LANES = 16
RING = 4
STRIDE = {'x': 1, 'y': RING, 'z': RING * RING}
ORDERS = ('xyz', 'yzx', 'zxy')
STREAMS = range(2)
PARTS = range(3)
WIDTHS = ((640, 640, 768), (768, 640, 640))
STARTS = ((0, 640, 1280), (0, 768, 1408))
SPAN = 768
SPAN_STARTS = (0, 640, 1280)
BOTH = [(q, r) for q in STREAMS for r in PARTS]


class Place:
    def __init__(self):
        self.core, self.chip = lax.axis_index('ep2'), lax.axis_index('ep')
        self.other = 1 - self.core
        self.coord = {axis: lax.rem(self.chip // stride, RING) for axis, stride in STRIDE.items()}

    def pos(self, axis, step):
        return lax.rem(self.coord[axis] + step + RING, RING)

    def at(self, axis, step):
        return self.chip + (self.pos(axis, step) - self.coord[axis]) * STRIDE[axis]

    def greet(self, both_cores):
        barrier = pltpu.get_barrier_semaphore()
        peers = [(self.other, self.chip)]
        for axis in STRIDE:
            for step in (1, -1):
                peers += [(c, self.at(axis, step)) for c in ((self.core, self.other) if both_cores else (self.core,))]
        for c, chip in peers:
            pl.semaphore_signal(barrier, inc=1, device_id=(0, c, chip), device_id_type=MESH)
        pl.semaphore_wait(barrier, len(peers))


class Lane:
    def __init__(self, place, axis, source, target, relay, send, recv, index, switch=False):
        self.place, self.axis, self.source, self.target, self.relay = place, axis, source, target, relay
        self.send, self.recv, self.index, self.switch = send, recv, index, switch
        self.sent = []

    def start(self, src, dst, s, r, core, chip):
        copy = pltpu.make_async_remote_copy(src_ref=src, dst_ref=dst, send_sem=self.send.at[self.index, s], recv_sem=self.recv.at[self.index, r], device_id=(0, core, chip), device_id_type=MESH)
        copy.start()
        self.sent.append(copy)

    def landed(self, dst, r):
        pltpu.make_async_remote_copy(src_ref=dst, dst_ref=dst, send_sem=self.send.at[self.index, 0], recv_sem=self.recv.at[self.index, r], device_id=(0, self.place.core, self.place.chip), device_id_type=MESH).wait_recv()

    def far(self):
        p = self.place
        for h, step in ((0, 1), (1, -1)):
            self.start(self.source(p.pos(self.axis, 2), h), self.relay.at[h], h, h, p.core, p.at(self.axis, step))

    def near(self):
        p = self.place
        me = p.coord[self.axis]
        for d, step in ((0, 1), (1, -1)):
            for h in (0, 1):
                k, c = (p.core, h) if self.switch else (h, p.core)
                self.start(self.source(p.pos(self.axis, step), h), self.target(me, k), 2 + 2 * d + h, 2 + 2 * d + k, c, p.at(self.axis, step))
        if self.switch:
            self.start(self.source(me, p.other), self.target(me, p.core), 8, 8, p.other, p.chip)

    def forward(self):
        p = self.place
        for h, step in ((0, 1), (1, -1)):
            self.landed(self.relay.at[h], h)
            k, c, r = (p.core, h, 6 + p.core) if self.switch else (h, p.core, 6 + h)
            self.start(self.relay.at[h], self.target(p.pos(self.axis, -step), k), 6 + h, r, c, p.at(self.axis, step))

    def arrive_near(self):
        p = self.place
        for d, step in ((0, -1), (1, 1)):
            for k in (0, 1):
                self.landed(self.target(p.pos(self.axis, step), k), 2 + 2 * d + k)
        if self.switch:
            self.landed(self.target(p.coord[self.axis], p.other), 8)

    def arrive_far(self):
        for k in (0, 1):
            self.landed(self.target(self.place.pos(self.axis, 2), k), 6 + k)

    def arrive(self):
        self.arrive_near()
        self.arrive_far()

    def own(self, local):
        p = self.place
        me = p.coord[self.axis]
        halves = [(p.core, p.core)] if self.switch else [(0, 0), (1, 1)]
        copies = [pltpu.make_async_copy(self.source(me, h), self.target(me, k), local.at[self.index, n]) for n, (h, k) in enumerate(halves)]
        for copy in copies:
            copy.start()
        return copies

    def drain(self):
        for copy in self.sent:
            copy.wait_send()


class Gather(Lane):
    def near(self):
        p = self.place
        me = p.coord[self.axis]
        for d, step, halves in ((0, 1, (0, 1)), (1, -1, (1, 0))):
            for h in halves:
                self.start(self.source(me, h), self.target(me, h), 2 + 2 * d + h, 2 + 2 * d + h, p.core, p.at(self.axis, step))

    def forward(self):
        p = self.place
        for h, step in ((0, 1), (1, -1)):
            part = self.target(p.pos(self.axis, -step), h)
            self.landed(part, 2 + 2 * h + h)
            self.start(part, part, 6 + h, 6 + h, p.core, p.at(self.axis, step))

    def arrive_near(self):
        p = self.place
        self.landed(self.target(p.pos(self.axis, -1), 1), 3)
        self.landed(self.target(p.pos(self.axis, 1), 0), 4)

    def arrive_far(self):
        for h in (0, 1):
            self.landed(self.target(self.place.pos(self.axis, 2), h), 6 + h)


class Reduce(Lane):
    def near(self):
        p = self.place
        for side, step in ((0, 1), (1, -1)):
            self.start(self.source(p.pos(self.axis, step), 1 - side), self.target(side, 1 - side), 2 + side, 2 + side, p.core, p.at(self.axis, step))

    def add(self):
        for h, step in ((0, 1), (1, -1)):
            self.landed(self.relay.at[h], h)
            self.relay[h] += self.source(self.place.pos(self.axis, step), h)[...]

    def forward(self):
        p = self.place
        for h, step in ((0, 1), (1, -1)):
            self.start(self.relay.at[h], self.target(h, h), 4 + h, 4 + h, p.core, p.at(self.axis, step))

    def arrive(self):
        for side in (0, 1):
            self.landed(self.target(side, 1 - side), 2 + side)
            self.landed(self.target(side, side), 4 + side)


def run(lanes, *steps):
    for step in steps:
        for lane in lanes:
            getattr(lane, step)()


def take(refs, *counts):
    refs = list(refs)
    for count in counts:
        yield refs[:count]
        del refs[:count]


def spot(axis, order, index):
    return (slice(None),) * [a for a in 'zyx' if a in order].index(axis) + (index,)


def plane_slots(shape, order, place, q, base=0):
    row = lax.broadcasted_iota(jnp.int32, shape, 0) + base
    first, second, third = [STRIDE[axis] for axis in order]
    dev = ((row >> 6) & 1) * RING**3 + (row >> 7) * second + ((row >> 4) & (RING - 1)) * third + place.coord[order[0]] * first
    return dev * (2 * LANES) + q * LANES + (row & (LANES - 1))


def line_slots(shape, order, place, q):
    row = lax.broadcasted_iota(jnp.int32, shape, 0)
    first, second, third = [STRIDE[axis] for axis in order]
    dev = ((row >> 4) & 1) * RING**3 + (row >> 5) * third + place.coord[order[0]] * first + place.coord[order[1]] * second
    return dev * (2 * LANES) + q * LANES + (row & (LANES - 1))


def route(ids_ref, slot_ref, count_ref):
    ids = ids_ref[...]
    n_top, n_tok = ids.shape
    experts = 2 * count_ref.shape[2]
    expert_of = lax.broadcasted_iota(jnp.int32, (experts, n_tok), 0)
    member = jnp.zeros((experts, n_tok), jnp.float32)
    for j in range(n_top):
        member = jnp.where(expert_of == ids[j:j + 1], 1.0, member)
    row = lax.broadcasted_iota(jnp.int32, (n_tok, n_tok), 0)
    col = lax.broadcasted_iota(jnp.int32, (n_tok, n_tok), 1)
    earlier = jnp.where(row < col, 1.0, 0.0).astype(jnp.bfloat16)
    member_lp = member.astype(jnp.bfloat16)
    before = jnp.dot(member_lp, earlier, preferred_element_type=jnp.float32)
    ones = jnp.ones((n_top, n_tok), jnp.bfloat16)
    counts = lax.dot_general(ones, member_lp, (((1,), (1,)), ((), ())), preferred_element_type=jnp.float32).astype(jnp.int32)
    half = n_tok // 2
    for h in (0, 1):
        count_ref[h] = counts[:, h * half:(h + 1) * half]
    for j in range(n_top):
        rank = jnp.sum(jnp.where(expert_of == ids[j:j + 1], before, 0.0), axis=0, keepdims=True)
        slot = ids[j:j + 1] * LANES + rank.astype(jnp.int32)
        for h in (0, 1):
            slot_ref[h, j:j + 1, :] = slot[:, h * half:(h + 1) * half]


def layer_kernel(capacity, *refs):
    (x, ids, gate), (w_in, w_out), (y,), wide, backs, ends, c_relay, cb_relay, bb_relay, refs = take(refs, 3, 2, 1, 3, 6, 6, 6, 6, 6, None)
    tokens, slots, wide_slots, gates, packed, rows, sums, got, sum_relay, (slot, count, count_x, count_y, count_z, count_other, mine, w_in_v, w_out_v, send, recv, local, extra) = take(refs, 3, 3, 3, 3, 6, 6, 3, 3, 3, None)
    place = Place()
    n_tok, n_top = x.shape[0], slot.shape[1]
    half = n_tok // 2
    n_row = 2 * RING * RING * LANES
    index = iter(range(send.shape[0]))
    lane = lambda kind, axis, source, target, relay=None, switch=False: kind(place, axis, source, target, relay, send, recv, next(index), switch)
    first, second, third = [[ORDERS[r][k] for r in PARTS] for k in PARTS]

    a_small = [lane(Gather, first[r], lambda p, h: slot.at[h], lambda o, k, r=r: slots[r].at[o, k]) for r in PARTS]
    a_small.append(lane(Gather, 'x', lambda p, h: count.at[h], lambda o, k: count_x.at[o, k]))
    a_out = [lane(Gather, first[r], lambda p, h, r=r: x.at[pl.ds(h * half, half), pl.ds(SPAN_STARTS[r], SPAN)],
                  lambda o, k, r=r: tokens[r].at[o, pl.ds(k * half, half)]) for r in PARTS]
    along_y = lane(Gather, 'y', lambda p, h: count_x.at[:, h], lambda o, k: count_y.at[o, :, k])
    along_z = lane(Gather, 'z', lambda p, h: count_y.at[:, :, h], lambda o, k: count_z.at[o, :, :, k])
    swap = lane(Lane, 'z', None, None)
    a_gate = [lane(Gather, first[r], lambda p, h: mine.at[h], lambda o, k, r=r: gates[r].at[o, k]) for r in PARTS]
    b_small = [lane(Gather, second[r], lambda p, h, r=r: slots[r].at[pl.ds(2 * h, 2)], lambda o, k, r=r: wide_slots[r].at[o, pl.ds(2 * k, 2)]) for r in PARTS]
    b_out = [lane(Gather, second[r], lambda p, h, r=r, step=step: tokens[r].at[place.pos(first[r], step), pl.ds(h * half, half)],
                  lambda o, k, r=r, step=step: wide[r].at[o, place.pos(first[r], step), pl.ds(k * half, half)]) for step in (0, 1, 3, 2) for r in PARTS]
    b_own, b_near, b_far = b_out[:3], b_out[3:9], b_out[9:]
    c_out = [lane(Lane, third[r], lambda p, h, i=3 * q + r: packed[i].at[p, h],
                  lambda o, k, i=3 * q + r, r=r: rows[i].at[(k,) + spot(third[r], 'zyx', o)], c_relay[3 * q + r], True) for q, r in BOTH]
    c_back = [lane(Lane, third[r], lambda p, h, i=3 * q + r, r=r: rows[i].at[(h,) + spot(third[r], 'zyx', p)],
                   lambda o, k, i=3 * q + r: backs[i].at[o, k], cb_relay[3 * q + r]) for q, r in BOTH]
    b_back = [lane(Lane, second[r], lambda p, h, i=3 * q + r, r=r: backs[i].at[(slice(None), h) + spot(second[r], ORDERS[r][:2], p)],
                   lambda o, k, i=3 * q + r: ends[i].at[o, k], bb_relay[3 * q + r], True) for q, r in BOTH]
    a_back = [lane(Reduce, first[r], lambda p, h, r=r: sums[r].at[p, pl.ds(h * half, half)],
                   lambda side, h, r=r: got[r].at[side, pl.ds(h * half, half)], sum_relay[r]) for r in PARTS]
    one, two = slice(0, 3), slice(3, 6)

    def pack(q, r, step, a):
        b = place.pos(second[r], step)
        n = 2 * RING * LANES
        wanted = line_slots((n, half), ORDERS[r], place, q)
        picks = []
        for h in (0, 1):
            pick = jnp.zeros((n, half), jnp.float32)
            for j in range(n_top):
                pick = jnp.where(wanted == wide_slots[r][b, a, h, j:j + 1], 1.0, pick)
            picks.append(pick.astype(jnp.bfloat16))
        offset = STARTS[q][r] - SPAN_STARTS[r]
        block = jnp.dot(jnp.concatenate(picks, axis=1), tokens[r][a, :, offset:offset + WIDTHS[q][r]], preferred_element_type=jnp.float32)
        spots = (b, a) if 'zyx'.index(second[r]) < 'zyx'.index(first[r]) else (a, b)
        packed[3 * q + r][(slice(None), slice(None)) + spots] = block.astype(jnp.bfloat16).reshape(RING, 2, LANES, WIDTHS[q][r])

    def expert(q, step):
        core, z = step // RING, lax.rem(step, RING)
        total = None
        for r in PARTS:
            part = rows[3 * q + r][core, z].reshape(RING * RING * LANES, WIDTHS[q][r])
            term = jnp.dot(part, w_in_v[STARTS[q][r]:STARTS[q][r] + WIDTHS[q][r]], preferred_element_type=jnp.float32)
            total = term if total is None else total + term
        hidden = jax.nn.gelu(total, approximate=True).astype(jnp.bfloat16)
        for r in PARTS:
            res = jnp.dot(hidden, w_out_v[:, STARTS[q][r]:STARTS[q][r] + WIDTHS[q][r]], preferred_element_type=jnp.float32)
            rows[3 * q + r][core, z] = res.astype(jnp.bfloat16).reshape(RING, RING, LANES, WIDTHS[q][r])

    def weigh():
        counted = lambda ref: ref[...].reshape((RING**3,) + slot.shape)
        ahead = lax.broadcasted_iota(jnp.int32, (RING**3,) + slot.shape, 0) < place.chip
        off = jnp.sum(jnp.where(ahead, counted(count_z), 0), axis=0) + jnp.where(place.core == 1, jnp.sum(counted(count_other), axis=0), 0)
        off = jnp.concatenate([off[0], off[1]], axis=1)
        high, low = (off >> 7).astype(jnp.bfloat16), (off & 127).astype(jnp.bfloat16)
        expert_of = lax.broadcasted_iota(jnp.int32, (off.shape[1], n_tok), 0)
        for j in range(n_top):
            choice = jnp.where(expert_of == ids[j:j + 1], 1.0, 0.0).astype(jnp.bfloat16)
            before = 128 * jnp.dot(high, choice, preferred_element_type=jnp.float32) + jnp.dot(low, choice, preferred_element_type=jnp.float32)
            before = before[0:1].astype(jnp.int32)
            for h in (0, 1):
                cut = slice(h * half, (h + 1) * half)
                rank = before[:, cut] + slot[h, j:j + 1] - ids[j:j + 1, cut] * LANES
                mine[h, j:j + 1] = jnp.where(rank < capacity, gate[j:j + 1, cut], 0.0)

    def combine(q, r, step, h):
        a = place.pos(first[r], step)
        wanted = plane_slots((n_row, half), ORDERS[r], place, q)
        weight = jnp.zeros((n_row, half), jnp.float32)
        for j in range(n_top):
            weight = jnp.where(wanted == slots[r][a, h, j:j + 1], gates[r][a, h, j:j + 1], weight)
        high = weight.astype(jnp.bfloat16)
        rest = weight - high.astype(jnp.float32)
        mid = rest.astype(jnp.bfloat16)
        low = (rest - mid.astype(jnp.float32)).astype(jnp.bfloat16)
        weights = jnp.concatenate([high, mid, low], axis=1)
        offset = STARTS[q][r] - SPAN_STARTS[r]
        for lo, hi in ((0, 384), (384, WIDTHS[q][r])):
            back = packed[3 * q + r][:, :, :, a, :, lo:hi].reshape(n_row, hi - lo)
            mix = lax.dot_general(weights, back, (((0,), (0,)), ((), ())), preferred_element_type=jnp.float32)
            sums[r][a, pl.ds(pl.multiple_of(h * half, half), half), offset + lo:offset + hi] += mix[:half] + mix[half:2 * half] + mix[2 * half:]

    def wait(copies):
        for copy in copies:
            copy.wait()

    def wait_sent(item, count):
        for copy in item.sent[:count]:
            copy.wait_send()
        del item.sent[:count]

    def own(lanes):
        return [copy for item in lanes for copy in item.own(local)]

    def load(src, dst, n):
        copy = pltpu.make_async_copy(src, dst, extra.at[n])
        copy.start()
        return copy

    def own_rows(lanes, i):
        me = [place.coord[item.axis] for item in lanes]
        return [load(item.source(me[r], place.core), packed[i + r].at[me[r], place.core], 4 + i + r) for r, item in enumerate(lanes)]

    def fetch(i, near):
        axis = second[i % 3]
        pieces = [(place.pos(axis, step),) for step in ((1, 3) if near else (2,))]
        if near:
            pieces.append((place.coord[axis], place.other))
        return [load(ends[i].at[at], packed[i].at[at], 10 + 4 * i + n + (0 if near else 3)) for n, at in enumerate(pieces)]

    def slabs(step):
        return [load(wide[r].at[place.pos(second[r], step)], tokens[r], 4 + r) for r in PARTS]

    kept = own(a_out)
    weights = [load(w_in.at[0], w_in_v, 0), load(w_out.at[0], w_out_v, 1)]
    route(ids, slot, count)
    kept += own(a_small)
    place.greet(True)
    run(a_small, 'near')
    run(a_out, 'near')
    run(a_small, 'forward')
    wait(kept)
    run(b_own, 'near')
    run(a_out, 'forward')
    run(a_small, 'arrive_near', 'arrive_far')
    kept = own(b_small + [along_y])
    run(b_small + [along_y], 'near')
    run(a_out, 'arrive_near')
    run(b_near, 'near')
    run(b_own, 'forward')
    run(a_out, 'arrive_far')
    run(b_far, 'near')
    run(b_small + [along_y], 'forward')
    wait(kept)
    for r in PARTS:
        pl.loop(0, RING)(lambda a, r=r: [pack(q, r, 0, a) for q in STREAMS] and None)
    run(b_near, 'forward')
    run(b_small, 'arrive_near')
    run(b_far, 'forward')
    run(b_out, 'arrive_near')
    run(a_out, 'drain')
    for item in b_out:
        wait_sent(item, 4)

    @pl.loop(0, 2)
    def _(n):
        loads = slabs(1 + 2 * n)
        for r in PARTS:
            loads[r].wait()
            pl.loop(0, RING)(lambda a, r=r: [pack(q, r, 1 + 2 * n, a) for q in STREAMS] and None)

    run(b_small + [along_y], 'arrive_far')
    run([along_y], 'arrive_near')
    kept_z = own([along_z])
    run([along_z], 'near')
    run(b_out, 'arrive_far')
    loads = slabs(2)
    for r in PARTS:
        loads[r].wait()
        pl.loop(0, RING)(lambda a, r=r: pack(0, r, 2, a))
    run(c_out[one], 'far', 'near')
    kept = own(c_out[one])
    for r in PARTS:
        pl.loop(0, RING)(lambda a, r=r: pack(1, r, 2, a))
    run(c_out[one], 'forward')
    run(c_out[two], 'far', 'near')
    kept_two = own(c_out[two])
    run([along_z], 'forward')
    run(c_out[one], 'arrive')
    wait(kept + weights)
    pl.loop(0, 2 * RING)(lambda n: expert(0, n))
    weights = [load(w_in.at[1], w_in_v, 2), load(w_out.at[1], w_out_v, 3)]
    run(c_out[two], 'forward')
    run(c_back[one], 'far', 'near')
    kept = own(c_back[one])
    run(c_out[two], 'arrive')
    wait(kept_two + weights)
    pl.loop(0, 2 * RING)(lambda n: expert(1, n))
    run(c_back[one], 'forward')
    run(c_back[two], 'far', 'near')
    kept_two = own(c_back[two])
    run([along_z], 'arrive_near', 'arrive_far')
    wait(kept_z)
    swap.start(count_z, count_other, 0, 0, place.other, place.chip)
    swap.landed(count_other, 0)
    weigh()
    kept_gate = own(a_gate)
    run(a_gate, 'near')
    run(c_back[two], 'forward')
    run(c_back[one], 'arrive')
    wait(kept)
    run(b_back[one], 'far', 'near')
    run(c_out, 'drain')
    kept = own_rows(b_back[one], 0)
    for r in PARTS:
        sums[r][...] = jnp.zeros_like(sums[r])
    run(a_gate, 'forward')
    run(b_back[one], 'forward')
    run(c_back[two], 'arrive')
    wait(kept_two)
    run(b_back[two], 'far', 'near')
    kept_two = own_rows(b_back[two], 3)
    run(b_back[one], 'arrive')
    wait(kept)
    loads = [fetch(r, True) + fetch(r, False) for r in PARTS]
    run(a_gate, 'arrive_near', 'arrive_far')
    wait(kept_gate)
    for r in PARTS:
        wait(loads[r])
        pl.loop(0, 2 * RING)(lambda n, r=r: combine(0, r, n // 2, lax.rem(n, 2)))
    run(b_back[two], 'forward', 'arrive_near')
    loads = [fetch(3 + r, True) for r in PARTS]
    wait(kept_two)
    run(b_back[two], 'arrive_far')
    loads = [loads[r] + fetch(3 + r, False) for r in PARTS]
    for r in PARTS:
        wait(loads[r])
        pl.loop(0, 2)(lambda h, r=r: combine(1, r, 2, h))
    run(a_back, 'far')
    for r in PARTS:
        pl.loop(0, 4)(lambda n, r=r: combine(1, r, 1 + 2 * (n // 2), lax.rem(n, 2)))
    run(a_back, 'near', 'add')
    run(a_back, 'forward')
    for r in PARTS:
        pl.loop(0, 2)(lambda h, r=r: combine(1, r, 0, h))
        sums[r][place.coord[first[r]], :, :SPAN_STARTS[1]] += x[:, SPAN_STARTS[r]:SPAN_STARTS[r] + SPAN_STARTS[1]].astype(jnp.float32)
    sums[2][place.coord[first[2]], :, SPAN_STARTS[1]:] += x[:, SPAN_STARTS[2] + SPAN_STARTS[1]:].astype(jnp.float32)
    run(a_back, 'arrive')
    for c in range(0, x.shape[1], 128):
        total = None
        for r in PARTS:
            if SPAN_STARTS[r] <= c < SPAN_STARTS[r] + SPAN:
                cut = slice(c - SPAN_STARTS[r], c - SPAN_STARTS[r] + 128)
                part = sums[r][place.coord[first[r]], :, cut] + got[r][0, :, cut] + got[r][1, :, cut]
                total = part if total is None else total + part
        y[:, c:c + 128] = total.astype(y.dtype)
    run(a_small + b_small + b_out + [along_y, along_z, swap] + a_gate + c_back + b_back + a_back, 'drain')


def solution(mesh):
    dev_axes = ('ep2', 'ep')
    bf16, f32, i32 = jnp.bfloat16, jnp.float32, jnp.int32
    group_size = mesh.shape['ep2'] * mesh.shape['ep']
    anywhere, near, dma = pl.BlockSpec(memory_space=pl.ANY), pl.BlockSpec(memory_space=pltpu.VMEM), pltpu.SemaphoreType.DMA
    vmem = lambda shapes, dtype: [pltpu.VMEM(shape, dtype) for shape in shapes]
    per_part = lambda *lead: [lead + (RING, RING, LANES, WIDTHS[q][r]) for q, r in BOTH]

    def local_step(x, ids, gate, w_a, w_b):
        n_tok, d_model = x.shape
        n_top = ids.shape[1]
        experts = w_a.shape[0] * group_size
        capacity = 8 * ((5 * group_size * n_tok * n_top) // (32 * experts))
        small = (2, n_top, n_tok // 2)
        ids_t, gate_t = ids.T, gate.T
        shape = jax.ShapeDtypeStruct
        between = [(RING, RING, n_tok, SPAN)] * 3 + per_part(RING, 2) * 2 + per_part(2) * 3
        lanes = 4 + 3 + 2 + 1 + 3 + 3 + 12 + 3 * 6 + 3
        return pl.pallas_call(
            functools.partial(layer_kernel, capacity),
            in_specs=[near] * 3 + [anywhere] * 2,
            out_specs=[near] + [anywhere] * len(between),
            out_shape=[shape(x.shape, x.dtype)] + [shape(s, bf16) for s in between],
            scratch_shapes=vmem([(RING, n_tok, SPAN)] * 3, bf16) + vmem([(RING,) + small] * 3 + [(RING, RING) + small] * 3, i32) + vmem([(RING,) + small] * 3, f32)
            + vmem(per_part(RING, 2), bf16) + vmem(per_part(2, RING), bf16) + vmem([(RING, n_tok, SPAN)] * 3, f32)
            + vmem([(2, n_tok, SPAN)] * 3, f32) + vmem([(2, n_tok // 2, SPAN)] * 3, f32)
            + vmem([small, (2, n_top, experts // 2), (RING,) + small, (RING, RING) + small] + [(RING, RING, RING) + small] * 2, i32) + vmem([small], f32)
            + vmem([w_a.shape[1:], w_b.shape[1:]], bf16) + [dma((lanes, 9)), dma((lanes, 9)), dma((lanes, 2)), dma((34,))],
            compiler_params=pltpu.CompilerParams(collective_id=0, has_side_effects=True, vmem_limit_bytes=67043328),
            name='layer',
        )(x, ids_t, gate_t, w_a, w_b)[0]

    tok_spec = P(('dp', 'ep2', 'ep'), None)
    w_spec = P(dev_axes, None, None)
    return jax.shard_map(local_step, mesh=mesh, in_specs=(tok_spec, tok_spec, tok_spec, w_spec, w_spec), out_specs=tok_spec, check_vma=False)
```

```python
import functools

import jax
import jax.numpy as jnp
from jax import lax
from jax.experimental import pallas as pl
from jax.experimental.pallas import tpu as pltpu
from jax.sharding import PartitionSpec as P

MESH = pl.DeviceIdType.MESH
LANES = 16
RING = 4
STRIDE = {'x': 1, 'y': RING, 'z': RING * RING}
ORDERS = ('xyz', 'yzx', 'zxy')
STREAMS = range(2)
PARTS = range(3)
WIDTHS = ((640, 640, 768), (768, 640, 640))
STARTS = ((0, 640, 1280), (0, 768, 1408))
SPAN = 768
SPAN_STARTS = (0, 640, 1280)
BOTH = [(q, r) for q in STREAMS for r in PARTS]


class Place:
    def __init__(self):
        self.core, self.chip = lax.axis_index('ep2'), lax.axis_index('ep')
        self.other = 1 - self.core
        self.coord = {axis: lax.rem(self.chip // stride, RING) for axis, stride in STRIDE.items()}

    def pos(self, axis, step):
        return lax.rem(self.coord[axis] + step + RING, RING)

    def at(self, axis, step):
        return self.chip + (self.pos(axis, step) - self.coord[axis]) * STRIDE[axis]

    def greet(self, both_cores):
        barrier = pltpu.get_barrier_semaphore()
        peers = [(self.other, self.chip)]
        for axis in STRIDE:
            for step in (1, -1):
                peers += [(c, self.at(axis, step)) for c in ((self.core, self.other) if both_cores else (self.core,))]
        for c, chip in peers:
            pl.semaphore_signal(barrier, inc=1, device_id=(0, c, chip), device_id_type=MESH)
        pl.semaphore_wait(barrier, len(peers))


class Lane:
    def __init__(self, place, axis, source, target, relay, send, recv, index, switch=False):
        self.place, self.axis, self.source, self.target, self.relay = place, axis, source, target, relay
        self.send, self.recv, self.index, self.switch = send, recv, index, switch
        self.sent = []

    def start(self, src, dst, s, r, core, chip):
        copy = pltpu.make_async_remote_copy(src_ref=src, dst_ref=dst, send_sem=self.send.at[self.index, s], recv_sem=self.recv.at[self.index, r], device_id=(0, core, chip), device_id_type=MESH)
        copy.start()
        self.sent.append(copy)

    def landed(self, dst, r):
        pltpu.make_async_remote_copy(src_ref=dst, dst_ref=dst, send_sem=self.send.at[self.index, 0], recv_sem=self.recv.at[self.index, r], device_id=(0, self.place.core, self.place.chip), device_id_type=MESH).wait_recv()

    def far(self):
        p = self.place
        for h, step in ((0, 1), (1, -1)):
            self.start(self.source(p.pos(self.axis, 2), h), self.relay(h), h, h, p.core, p.at(self.axis, step))

    def near(self):
        p = self.place
        me = p.coord[self.axis]
        for d, step in ((0, 1), (1, -1)):
            for h in (0, 1):
                k, c = (p.core, h) if self.switch else (h, p.core)
                self.start(self.source(p.pos(self.axis, step), h), self.target(me, k), 2 + 2 * d + h, 2 + 2 * d + k, c, p.at(self.axis, step))
        if self.switch:
            self.start(self.source(me, p.other), self.target(me, p.core), 8, 8, p.other, p.chip)

    def forward(self):
        p = self.place
        for h, step in ((0, 1), (1, -1)):
            self.landed(self.relay(h), h)
            k, c, r = (p.core, h, 6 + p.core) if self.switch else (h, p.core, 6 + h)
            self.start(self.relay(h), self.target(p.pos(self.axis, -step), k), 6 + h, r, c, p.at(self.axis, step))

    def arrive_near(self):
        p = self.place
        for d, step in ((0, -1), (1, 1)):
            for k in (0, 1):
                self.landed(self.target(p.pos(self.axis, step), k), 2 + 2 * d + k)
        if self.switch:
            self.landed(self.target(p.coord[self.axis], p.other), 8)

    def arrive_far(self):
        for k in (0, 1):
            self.landed(self.target(self.place.pos(self.axis, 2), k), 6 + k)

    def arrive(self):
        self.arrive_near()
        self.arrive_far()

    def own(self, local):
        p = self.place
        me = p.coord[self.axis]
        halves = [(p.core, p.core)] if self.switch else [(0, 0), (1, 1)]
        copies = [pltpu.make_async_copy(self.source(me, h), self.target(me, k), local.at[self.index, n]) for n, (h, k) in enumerate(halves)]
        for copy in copies:
            copy.start()
        return copies

    def drain(self):
        for copy in self.sent:
            copy.wait_send()


class Gather(Lane):
    def near(self):
        p = self.place
        me = p.coord[self.axis]
        for d, step, halves in ((0, 1, (0, 1)), (1, -1, (1, 0))):
            for h in halves:
                self.start(self.source(me, h), self.target(me, h), 2 + 2 * d + h, 2 + 2 * d + h, p.core, p.at(self.axis, step))

    def forward(self):
        p = self.place
        for h, step in ((0, 1), (1, -1)):
            part = self.target(p.pos(self.axis, -step), h)
            self.landed(part, 2 + 2 * h + h)
            self.start(part, part, 6 + h, 6 + h, p.core, p.at(self.axis, step))

    def arrive_near(self):
        p = self.place
        self.landed(self.target(p.pos(self.axis, -1), 1), 3)
        self.landed(self.target(p.pos(self.axis, 1), 0), 4)

    def arrive_far(self):
        for h in (0, 1):
            self.landed(self.target(self.place.pos(self.axis, 2), h), 6 + h)


class Reduce(Lane):
    def near(self):
        p = self.place
        for side, step in ((0, 1), (1, -1)):
            self.start(self.source(p.pos(self.axis, step), 1 - side), self.target(side, 1 - side), 2 + side, 2 + side, p.core, p.at(self.axis, step))

    def add(self):
        for h, step in ((0, 1), (1, -1)):
            self.landed(self.relay(h), h)
            self.relay(h)[...] += self.source(self.place.pos(self.axis, step), h)[...]

    def forward(self):
        p = self.place
        for h, step in ((0, 1), (1, -1)):
            self.start(self.relay(h), self.target(h, h), 4 + h, 4 + h, p.core, p.at(self.axis, step))

    def arrive(self):
        for side in (0, 1):
            self.landed(self.target(side, 1 - side), 2 + side)
            self.landed(self.target(side, side), 4 + side)


def run(lanes, *steps):
    for step in steps:
        for lane in lanes:
            getattr(lane, step)()


def take(refs, *counts):
    refs = list(refs)
    for count in counts:
        yield refs[:count]
        del refs[:count]


def spot(axis, order, index):
    return (slice(None),) * [a for a in 'zyx' if a in order].index(axis) + (index,)


def plane_slots(shape, order, place, q, base=0):
    row = lax.broadcasted_iota(jnp.int32, shape, 0) + base
    first, second, third = [STRIDE[axis] for axis in order]
    dev = ((row >> 6) & 1) * RING**3 + (row >> 7) * second + ((row >> 4) & (RING - 1)) * third + place.coord[order[0]] * first
    return dev * (2 * LANES) + q * LANES + (row & (LANES - 1))


def line_slots(shape, order, place, q):
    row = lax.broadcasted_iota(jnp.int32, shape, 0)
    first, second, third = [STRIDE[axis] for axis in order]
    dev = ((row >> 4) & 1) * RING**3 + (row >> 5) * third + place.coord[order[0]] * first + place.coord[order[1]] * second
    return dev * (2 * LANES) + q * LANES + (row & (LANES - 1))


def route(ids_ref, slot_ref, count_ref):
    ids = ids_ref[...]
    n_top, n_tok = ids.shape
    experts = 2 * count_ref.shape[2]
    expert_of = lax.broadcasted_iota(jnp.int32, (experts, n_tok), 0)
    member = jnp.zeros((experts, n_tok), jnp.float32)
    for j in range(n_top):
        member = jnp.where(expert_of == ids[j:j + 1], 1.0, member)
    row = lax.broadcasted_iota(jnp.int32, (n_tok, n_tok), 0)
    col = lax.broadcasted_iota(jnp.int32, (n_tok, n_tok), 1)
    earlier = jnp.where(row < col, 1.0, 0.0).astype(jnp.bfloat16)
    member_lp = member.astype(jnp.bfloat16)
    before = jnp.dot(member_lp, earlier, preferred_element_type=jnp.float32)
    ones = jnp.ones((n_top, n_tok), jnp.bfloat16)
    counts = lax.dot_general(ones, member_lp, (((1,), (1,)), ((), ())), preferred_element_type=jnp.float32).astype(jnp.int32)
    half = n_tok // 2
    for h in (0, 1):
        count_ref[h] = counts[:, h * half:(h + 1) * half]
    for j in range(n_top):
        rank = jnp.sum(jnp.where(expert_of == ids[j:j + 1], before, 0.0), axis=0, keepdims=True)
        slot = ids[j:j + 1] * LANES + rank.astype(jnp.int32)
        for h in (0, 1):
            slot_ref[h, j:j + 1, :] = slot[:, h * half:(h + 1) * half]


def layer_kernel(capacity, *refs):
    (x, ids, gate), (w_in, w_out), (y,), wide, backs, ends, c_relay, cb_relay, bb_relay, refs = take(refs, 3, 2, 1, 3, 6, 6, 6, 6, 6, None)
    tokens, slots, wide_slots, gates, packed, rows, sums, got, sum_relay, (slot, count, count_x, count_y, count_z, count_other, mine, w_in_v, w_out_v, send, recv, local, extra) = take(refs, 3, 3, 3, 3, 6, 6, 3, 3, 3, None)
    place = Place()
    n_tok, n_top = x.shape[0], slot.shape[1]
    half = n_tok // 2
    n_row = 2 * RING * RING * LANES
    index = iter(range(send.shape[0]))
    lane = lambda kind, axis, source, target, relay=None, switch=False: kind(place, axis, source, target, relay, send, recv, next(index), switch)
    first, second, third = [[ORDERS[r][k] for r in PARTS] for k in PARTS]

    a_small = [lane(Gather, first[r], lambda p, h: slot.at[h], lambda o, k, r=r: slots[r].at[o, k]) for r in PARTS]
    a_small.append(lane(Gather, 'x', lambda p, h: count.at[h], lambda o, k: count_x.at[o, k]))
    a_out = [lane(Gather, first[r], lambda p, h, r=r: x.at[pl.ds(h * half, half), pl.ds(SPAN_STARTS[r], SPAN)],
                  lambda o, k, r=r: tokens[r].at[o, pl.ds(k * half, half)]) for r in PARTS]
    along_y = lane(Gather, 'y', lambda p, h: count_x.at[:, h], lambda o, k: count_y.at[o, :, k])
    along_z = lane(Gather, 'z', lambda p, h: count_y.at[:, :, h], lambda o, k: count_z.at[o, :, :, k])
    swap = lane(Lane, 'z', None, None)
    a_gate = [lane(Gather, first[r], lambda p, h: mine.at[h], lambda o, k, r=r: gates[r].at[o, k]) for r in PARTS]
    b_small = [lane(Gather, second[r], lambda p, h, r=r: slots[r].at[pl.ds(2 * h, 2)], lambda o, k, r=r: wide_slots[r].at[o, pl.ds(2 * k, 2)]) for r in PARTS]
    b_out = [lane(Gather, second[r], lambda p, h, r=r, step=step: tokens[r].at[place.pos(first[r], step), pl.ds(h * half, half)],
                  lambda o, k, r=r, step=step: wide[r].at[o, place.pos(first[r], step), pl.ds(k * half, half)]) for step in (0, 1, 3, 2) for r in PARTS]
    b_own, b_near, b_far = b_out[:3], b_out[3:9], b_out[9:]
    def along(axes, **index):
        return tuple(index.get(axis, slice(None)) for axis in 'zyx' if axis in axes)

    def c_piece(r, step):
        b = place.pos(second[r], step)
        return lane(Lane, third[r], lambda p, h: packed[r].at[(p, h) + along(ORDERS[r][:2], **{second[r]: b})],
                    lambda o, k: rows[r].at[(k,) + along('zyx', **{second[r]: b, third[r]: o})], lambda h: c_relay[r].at[h, step], True)

    c_own, c_near, c_far = [[c_piece(r, step) for step in steps for r in PARTS] for steps in ((0,), (1, 3), (2,))]
    c_first = c_own + c_near + c_far
    c_second = [lane(Lane, third[r], lambda p, h, r=r: packed[3 + r].at[p, h],
                     lambda o, k, r=r: rows[3 + r].at[(k,) + spot(third[r], 'zyx', o)], lambda h, r=r: c_relay[3 + r].at[h], True) for r in PARTS]
    c_back = [lane(Lane, third[r], lambda p, h, i=3 * q + r, r=r: rows[i].at[(h,) + spot(third[r], 'zyx', p)],
                   lambda o, k, i=3 * q + r: backs[i].at[o, k], lambda h, i=3 * q + r: cb_relay[i].at[h]) for q, r in BOTH]
    b_back = [lane(Lane, second[r], lambda p, h, i=3 * q + r, r=r: backs[i].at[(slice(None), h) + spot(second[r], ORDERS[r][:2], p)],
                   lambda o, k, i=3 * q + r: ends[i].at[o, k], lambda h, i=3 * q + r: bb_relay[i].at[h], True) for q, r in BOTH]
    a_back = [lane(Reduce, first[r], lambda p, h, r=r: sums[r].at[p, pl.ds(h * half, half)],
                   lambda side, h, r=r: got[r].at[side, pl.ds(h * half, half)], lambda h, r=r: sum_relay[r].at[h]) for r in PARTS]
    one, two = slice(0, 3), slice(3, 6)

    def pack(q, r, step, a):
        b = place.pos(second[r], step)
        n = 2 * RING * LANES
        wanted = line_slots((n, half), ORDERS[r], place, q)
        picks = []
        for h in (0, 1):
            pick = jnp.zeros((n, half), jnp.float32)
            for j in range(n_top):
                pick = jnp.where(wanted == wide_slots[r][b, a, h, j:j + 1], 1.0, pick)
            picks.append(pick.astype(jnp.bfloat16))
        offset = STARTS[q][r] - SPAN_STARTS[r]
        block = jnp.dot(jnp.concatenate(picks, axis=1), tokens[r][a, :, offset:offset + WIDTHS[q][r]], preferred_element_type=jnp.float32)
        spots = (b, a) if 'zyx'.index(second[r]) < 'zyx'.index(first[r]) else (a, b)
        packed[3 * q + r][(slice(None), slice(None)) + spots] = block.astype(jnp.bfloat16).reshape(RING, 2, LANES, WIDTHS[q][r])

    def expert(q, step):
        core, z = step // RING, lax.rem(step, RING)
        total = None
        for r in PARTS:
            part = rows[3 * q + r][core, z].reshape(RING * RING * LANES, WIDTHS[q][r])
            term = jnp.dot(part, w_in_v[STARTS[q][r]:STARTS[q][r] + WIDTHS[q][r]], preferred_element_type=jnp.float32)
            total = term if total is None else total + term
        hidden = jax.nn.gelu(total, approximate=True).astype(jnp.bfloat16)
        for r in PARTS:
            res = jnp.dot(hidden, w_out_v[:, STARTS[q][r]:STARTS[q][r] + WIDTHS[q][r]], preferred_element_type=jnp.float32)
            rows[3 * q + r][core, z] = res.astype(jnp.bfloat16).reshape(RING, RING, LANES, WIDTHS[q][r])

    def weigh():
        counted = lambda ref: ref[...].reshape((RING**3,) + slot.shape)
        ahead = lax.broadcasted_iota(jnp.int32, (RING**3,) + slot.shape, 0) < place.chip
        off = jnp.sum(jnp.where(ahead, counted(count_z), 0), axis=0) + jnp.where(place.core == 1, jnp.sum(counted(count_other), axis=0), 0)
        off = jnp.concatenate([off[0], off[1]], axis=1)
        high, low = (off >> 7).astype(jnp.bfloat16), (off & 127).astype(jnp.bfloat16)
        expert_of = lax.broadcasted_iota(jnp.int32, (off.shape[1], n_tok), 0)
        for j in range(n_top):
            choice = jnp.where(expert_of == ids[j:j + 1], 1.0, 0.0).astype(jnp.bfloat16)
            before = 128 * jnp.dot(high, choice, preferred_element_type=jnp.float32) + jnp.dot(low, choice, preferred_element_type=jnp.float32)
            before = before[0:1].astype(jnp.int32)
            for h in (0, 1):
                cut = slice(h * half, (h + 1) * half)
                rank = before[:, cut] + slot[h, j:j + 1] - ids[j:j + 1, cut] * LANES
                mine[h, j:j + 1] = jnp.where(rank < capacity, gate[j:j + 1, cut], 0.0)

    def combine(q, r, step, h):
        a = place.pos(first[r], step)
        wanted = plane_slots((n_row, half), ORDERS[r], place, q)
        weight = jnp.zeros((n_row, half), jnp.float32)
        for j in range(n_top):
            weight = jnp.where(wanted == slots[r][a, h, j:j + 1], gates[r][a, h, j:j + 1], weight)
        high = weight.astype(jnp.bfloat16)
        rest = weight - high.astype(jnp.float32)
        mid = rest.astype(jnp.bfloat16)
        low = (rest - mid.astype(jnp.float32)).astype(jnp.bfloat16)
        weights = jnp.concatenate([high, mid, low], axis=1)
        offset = STARTS[q][r] - SPAN_STARTS[r]
        for lo, hi in ((0, 384), (384, WIDTHS[q][r])):
            back = packed[3 * q + r][:, :, :, a, :, lo:hi].reshape(n_row, hi - lo)
            mix = lax.dot_general(weights, back, (((0,), (0,)), ((), ())), preferred_element_type=jnp.float32)
            sums[r][a, pl.ds(pl.multiple_of(h * half, half), half), offset + lo:offset + hi] += mix[:half] + mix[half:2 * half] + mix[2 * half:]

    def wait(copies):
        for copy in copies:
            copy.wait()

    def wait_sent(item, count):
        for copy in item.sent[:count]:
            copy.wait_send()
        del item.sent[:count]

    def own(lanes):
        return [copy for item in lanes for copy in item.own(local)]

    def load(src, dst, n):
        copy = pltpu.make_async_copy(src, dst, extra.at[n])
        copy.start()
        return copy

    def own_rows(lanes, i):
        me = [place.coord[item.axis] for item in lanes]
        return [load(item.source(me[r], place.core), packed[i + r].at[me[r], place.core], 4 + i + r) for r, item in enumerate(lanes)]

    def fetch(i, near):
        axis = second[i % 3]
        pieces = [(place.pos(axis, step),) for step in ((1, 3) if near else (2,))]
        if near:
            pieces.append((place.coord[axis], place.other))
        return [load(ends[i].at[at], packed[i].at[at], 10 + 4 * i + n + (0 if near else 3)) for n, at in enumerate(pieces)]

    def slabs(step):
        return [load(wide[r].at[place.pos(second[r], step)], tokens[r], 4 + r) for r in PARTS]

    kept = own(a_out)
    weights = [load(w_in.at[0], w_in_v, 0), load(w_out.at[0], w_out_v, 1)]
    route(ids, slot, count)
    kept += own(a_small)
    place.greet(True)
    run(a_small, 'near')
    run(a_out, 'near')
    run(a_small, 'forward')
    wait(kept)
    run(b_own, 'near')
    run(a_out, 'forward')
    run(a_small, 'arrive_near', 'arrive_far')
    kept = own(b_small + [along_y])
    run(b_small + [along_y], 'near')
    run(a_out, 'arrive_near')
    run(b_near, 'near')
    run(b_own, 'forward')
    run(a_out, 'arrive_far')
    run(b_far, 'near')
    run(b_small + [along_y], 'forward')
    wait(kept)
    for r in PARTS:
        pl.loop(0, RING)(lambda a, r=r: [pack(q, r, 0, a) for q in STREAMS] and None)
    run(b_near, 'forward')
    run(b_small, 'arrive_near')
    run(b_far, 'forward')
    run(c_own, 'far', 'near')
    kept = own(c_own)
    run(b_out, 'arrive_near')
    run(a_out, 'drain')
    for item in b_out:
        wait_sent(item, 4)

    @pl.loop(0, 2)
    def _(n):
        loads = slabs(1 + 2 * n)
        for r in PARTS:
            loads[r].wait()
            pl.loop(0, RING)(lambda a, r=r: [pack(q, r, 1 + 2 * n, a) for q in STREAMS] and None)

    run(c_near, 'far', 'near')
    kept += own(c_near)
    run(c_own, 'forward')
    run(b_small + [along_y], 'arrive_far')
    run([along_y], 'arrive_near')
    kept_z = own([along_z])
    run(b_out, 'arrive_far')
    loads = slabs(2)
    for r in PARTS:
        loads[r].wait()
        pl.loop(0, RING)(lambda a, r=r: pack(0, r, 2, a))
    run([along_z], 'near')
    run(c_far, 'far', 'near')
    kept += own(c_far)
    for r in PARTS:
        pl.loop(0, RING)(lambda a, r=r: pack(1, r, 2, a))
    run(c_near, 'forward')
    run(c_far, 'forward')
    run(c_second, 'far', 'near')
    kept_two = own(c_second)
    run([along_z], 'forward')
    run(c_first, 'arrive')
    wait(kept + weights)
    pl.loop(0, 2 * RING)(lambda n: expert(0, n))
    weights = [load(w_in.at[1], w_in_v, 2), load(w_out.at[1], w_out_v, 3)]
    run(c_second, 'forward')
    run(c_back[one], 'far', 'near')
    kept = own(c_back[one])
    run(c_second, 'arrive')
    wait(kept_two + weights)
    pl.loop(0, 2 * RING)(lambda n: expert(1, n))
    run(c_back[one], 'forward')
    run(c_back[two], 'far', 'near')
    kept_two = own(c_back[two])
    run([along_z], 'arrive_near', 'arrive_far')
    wait(kept_z)
    swap.start(count_z, count_other, 0, 0, place.other, place.chip)
    swap.landed(count_other, 0)
    weigh()
    kept_gate = own(a_gate)
    run(a_gate, 'near')
    run(c_back[two], 'forward')
    run(c_back[one], 'arrive')
    wait(kept)
    run(b_back[one], 'far', 'near')
    run(c_first + c_second, 'drain')
    kept = own_rows(b_back[one], 0)
    for r in PARTS:
        sums[r][...] = jnp.zeros_like(sums[r])
    run(a_gate, 'forward')
    run(b_back[one], 'forward')
    run(c_back[two], 'arrive')
    wait(kept_two)
    run(b_back[two], 'far', 'near')
    kept_two = own_rows(b_back[two], 3)
    run(b_back[one], 'arrive')
    wait(kept)
    loads = [fetch(r, True) + fetch(r, False) for r in PARTS]
    run(a_gate, 'arrive_near', 'arrive_far')
    wait(kept_gate)
    for r in PARTS:
        wait(loads[r])
        pl.loop(0, 2 * RING)(lambda n, r=r: combine(0, r, n // 2, lax.rem(n, 2)))
    run(b_back[two], 'forward', 'arrive_near')
    loads = [fetch(3 + r, True) for r in PARTS]
    wait(kept_two)
    run(b_back[two], 'arrive_far')
    loads = [loads[r] + fetch(3 + r, False) for r in PARTS]
    for r in PARTS:
        wait(loads[r])
        pl.loop(0, 2)(lambda h, r=r: combine(1, r, 2, h))
    run(a_back, 'far')
    for r in PARTS:
        pl.loop(0, 4)(lambda n, r=r: combine(1, r, 1 + 2 * (n // 2), lax.rem(n, 2)))
    run(a_back, 'near', 'add')
    run(a_back, 'forward')
    for r in PARTS:
        pl.loop(0, 2)(lambda h, r=r: combine(1, r, 0, h))
        sums[r][place.coord[first[r]], :, :SPAN_STARTS[1]] += x[:, SPAN_STARTS[r]:SPAN_STARTS[r] + SPAN_STARTS[1]].astype(jnp.float32)
    sums[2][place.coord[first[2]], :, SPAN_STARTS[1]:] += x[:, SPAN_STARTS[2] + SPAN_STARTS[1]:].astype(jnp.float32)
    run(a_back, 'arrive')
    for c in range(0, x.shape[1], 128):
        total = None
        for r in PARTS:
            if SPAN_STARTS[r] <= c < SPAN_STARTS[r] + SPAN:
                cut = slice(c - SPAN_STARTS[r], c - SPAN_STARTS[r] + 128)
                part = sums[r][place.coord[first[r]], :, cut] + got[r][0, :, cut] + got[r][1, :, cut]
                total = part if total is None else total + part
        y[:, c:c + 128] = total.astype(y.dtype)
    run(a_small + b_small + b_out + [along_y, along_z, swap] + a_gate + c_back + b_back + a_back, 'drain')


def solution(mesh):
    dev_axes = ('ep2', 'ep')
    bf16, f32, i32 = jnp.bfloat16, jnp.float32, jnp.int32
    group_size = mesh.shape['ep2'] * mesh.shape['ep']
    anywhere, near, dma = pl.BlockSpec(memory_space=pl.ANY), pl.BlockSpec(memory_space=pltpu.VMEM), pltpu.SemaphoreType.DMA
    vmem = lambda shapes, dtype: [pltpu.VMEM(shape, dtype) for shape in shapes]
    per_part = lambda *lead: [lead + (RING, RING, LANES, WIDTHS[q][r]) for q, r in BOTH]

    def local_step(x, ids, gate, w_a, w_b):
        n_tok, d_model = x.shape
        n_top = ids.shape[1]
        experts = w_a.shape[0] * group_size
        capacity = 8 * ((5 * group_size * n_tok * n_top) // (32 * experts))
        small = (2, n_top, n_tok // 2)
        ids_t, gate_t = ids.T, gate.T
        shape = jax.ShapeDtypeStruct
        between = [(RING, RING, n_tok, SPAN)] * 3 + per_part(RING, 2) * 2 + per_part(2) * 3
        lanes = 4 + 3 + 2 + 1 + 3 + 3 + 12 + 12 + 3 + 2 * 6 + 3
        return pl.pallas_call(
            functools.partial(layer_kernel, capacity),
            in_specs=[near] * 3 + [anywhere] * 2,
            out_specs=[near] + [anywhere] * len(between),
            out_shape=[shape(x.shape, x.dtype)] + [shape(s, bf16) for s in between],
            scratch_shapes=vmem([(RING, n_tok, SPAN)] * 3, bf16) + vmem([(RING,) + small] * 3 + [(RING, RING) + small] * 3, i32) + vmem([(RING,) + small] * 3, f32)
            + vmem(per_part(RING, 2), bf16) + vmem(per_part(2, RING), bf16) + vmem([(RING, n_tok, SPAN)] * 3, f32)
            + vmem([(2, n_tok, SPAN)] * 3, f32) + vmem([(2, n_tok // 2, SPAN)] * 3, f32)
            + vmem([small, (2, n_top, experts // 2), (RING,) + small, (RING, RING) + small] + [(RING, RING, RING) + small] * 2, i32) + vmem([small], f32)
            + vmem([w_a.shape[1:], w_b.shape[1:]], bf16) + [dma((lanes, 9)), dma((lanes, 9)), dma((lanes, 2)), dma((34,))],
            compiler_params=pltpu.CompilerParams(collective_id=0, has_side_effects=True, vmem_limit_bytes=67043328),
            name='layer',
        )(x, ids_t, gate_t, w_a, w_b)[0]

    tok_spec = P(('dp', 'ep2', 'ep'), None)
    w_spec = P(dev_axes, None, None)
    return jax.shard_map(local_step, mesh=mesh, in_specs=(tok_spec, tok_spec, tok_spec, w_spec, w_spec), out_specs=tok_spec, check_vma=False)
```
